32 devices in a mesh: tok: 4 (over z), out: 4 (over x, core), grp: 2 (over y).
Axes of the slice: x: 2, y: 2, z: 4, core: 2. Of those that a mesh axis runs over, the one named last changes fastest.
Arguments:
- activations: bfloat16 [1024, 2, 2048], P(('tok', 'grp'), None, 'out'), may hold values from -16 to 16
- out_grads: bfloat16 [1024, 2, 2048], P(('tok', 'grp'), None, 'out'), may hold values from -16 to 16
- weight: bfloat16 [2, 2048, 4096], P(None, 'out'), may hold values from -0.09375 to 0.09375
Outputs:
- update: bfloat16 [4096, 2, 2048], P(('tok', 'grp'), None, 'out')
- input_grad: bfloat16 [1024, 2, 2048], P(('tok', 'grp'), None, 'out')
The draws below stay inside these ranges and needn't reach their ends.
All inputs are finite; a program needn't handle non-finite values.
Results may differ from the reference program's by a relative error of at most 0.0092.
Values may be sent and summed in bfloat16 or wider, within the bound.
A program may use at most 64 MiB of HBM per device.

```python
import math
import jax
import jax.numpy as jnp
from jax import lax

BLOCK = 2048
NBLOCKS = 2
POWER = 3
D = 4096
TOKENS = 1024


def shaped_sides(key):
    noise_key, level_key, reach_key, sign_key, turn_key, weight_key, factor_key = jax.random.split(key, 7)
    array_shape = (TOKENS, NBLOCKS, BLOCK)
    bulk_noise = jnp.clip(jax.random.normal(noise_key, array_shape, jnp.float32), -4.0, 4.0)
    strength = jax.random.uniform(factor_key, (NBLOCKS,), jnp.float32, 1.8, 3.0)
    levels = jnp.exp(jax.random.uniform(level_key, (NBLOCKS, BLOCK), jnp.float32, -1.2, 1.2))
    block_reach = jax.random.uniform(reach_key, (NBLOCKS,), jnp.float32, 0.35, 0.7)
    parity = jnp.where(jnp.arange(NBLOCKS) % 2 == 0, 1.0, -1.0)
    block_sign = jnp.where(jax.random.bernoulli(sign_key, 0.5), 1.0, -1.0)
    magnitude = jnp.exp(block_reach * parity * block_sign)
    squares = levels * levels
    orthonormal = []
    for column_vec in (jnp.ones_like(squares), squares, squares * squares):
        for member in orthonormal:
            column_vec = column_vec - jnp.sum(column_vec * member, axis=1, keepdims=True) * member
        orthonormal.append(column_vec / jnp.sqrt(jnp.sum(column_vec * column_vec, axis=1, keepdims=True)))
    direction = jax.random.normal(turn_key, (NBLOCKS, BLOCK), jnp.float32)
    for member in orthonormal:
        direction = direction - jnp.sum(direction * member, axis=1, keepdims=True) * member
    direction = direction / jnp.sqrt(jnp.sum(direction * direction, axis=1, keepdims=True))
    amplitude = jnp.sqrt(strength * 3.0 * jnp.max(squares, axis=1))
    weights = jax.random.normal(weight_key, (TOKENS, NBLOCKS), jnp.float32)
    shaped = magnitude[None, :, None] * (levels[None] * bulk_noise + amplitude[None, :, None] * weights[:, :, None] * direction[None])
    return jnp.clip(shaped, -16.0, 16.0)


def draw_activations(key, part):
    return shaped_sides(jax.random.fold_in(key, 11)).astype(jnp.bfloat16)


def draw_out_grads(key, part):
    return shaped_sides(jax.random.fold_in(key, 23)).astype(jnp.bfloat16)


def shard_levels(rng, extent, shards, low, largest):
    def one(axis_at, blocks):
        steps = jax.random.uniform(jax.random.fold_in(jax.random.fold_in(rng, 6), axis_at), (blocks,), jnp.float32, low / len(shards), largest / len(shards))
        return jnp.repeat(jnp.exp(steps), extent[axis_at] // blocks).reshape((-1,) + (1,) * (len(extent) - axis_at - 1))

    factor_of = one(*shards[0])
    for cut in shards[1:]:
        factor_of = factor_of * one(*cut)
    return factor_of


def gaussian(key, shape, width, limit, cuts=(), kind=jnp.bfloat16):
    result = width * jax.random.normal(key, shape, jnp.float32)
    if cuts:
        result = result * shard_levels(key, shape, cuts, -0.22, 0.18)
    return jnp.clip(result, -limit, limit).astype(kind)


def setup_inputs(seed: int = 0) -> dict:
    seeds = jax.random.split(jax.random.key(seed), 4)
    activations = draw_activations(jax.random.fold_in(seeds[3], 71), 0)
    out_grads = draw_out_grads(jax.random.fold_in(seeds[3], 71), 0)
    weight = gaussian(seeds[2], (NBLOCKS, BLOCK, D), D ** -0.5, 0.09375, ((1, 4),))
    return dict(activations=activations, out_grads=out_grads, weight=weight)


DAMPING = 0.1
HIGH = lax.Precision.HIGHEST

def lowered(value):
    return lax.optimization_barrier(value.astype(jnp.bfloat16))

def batched(left, right):
    return jnp.einsum('kij,kjl->kil', left.astype(jnp.float32), right.astype(jnp.float32), precision=HIGH)

def reference(activations, out_grads, weight):
    sides = jnp.concatenate([activations, out_grads], axis=1)
    wide = sides.astype(jnp.float32)
    tokens = sides.shape[0]
    count = sides.shape[1]
    block = sides.shape[2]
    half = count // 2
    identity = jnp.eye(block, dtype=jnp.float32)[None]
    factor = jnp.einsum('tki,tkj->kij', wide, wide, precision=HIGH) / tokens + DAMPING * identity
    vector = jnp.ones((count, block), jnp.float32)
    image = vector
    for step in range(POWER):
        image = jnp.einsum('kij,kj->ki', factor, vector, precision=HIGH)
        if step + 1 < POWER:
            vector = image / jnp.sqrt(lax.optimization_barrier(jnp.sum(image * image, axis=1, keepdims=True)))
    scale = lax.optimization_barrier(jnp.sum(vector * image, axis=1)) / lax.optimization_barrier(jnp.sum(vector * vector, axis=1))
    start = factor / scale[:, None, None]
    start_low = lowered(start)
    first_low = lowered((3.0 * identity - start) / 2.0)
    square_low = lowered(batched(first_low, first_low))
    moved = batched(square_low, start_low)
    second_low = lowered((3.0 * identity - moved) / 2.0)
    roots = lowered(batched(first_low, second_low) / jnp.sqrt(scale)[:, None, None])
    whitened = lowered(jnp.einsum('tkj,kjc->tkc', wide, roots.astype(jnp.float32), precision=HIGH))
    acts_flat = whitened[:, :half, :].reshape(tokens, half * block).astype(jnp.float32)
    grads_low = whitened[:, half:, :].astype(jnp.float32)
    update = jnp.einsum('ta,tbc->abc', acts_flat, grads_low, precision=HIGH) / math.sqrt(tokens)
    grads_flat = out_grads.reshape(tokens, half * block).astype(jnp.float32)
    input_grad = jnp.einsum('tj,bcj->tbc', grads_flat, weight.astype(jnp.float32), precision=HIGH)
    return (update.astype(jnp.bfloat16), input_grad.astype(jnp.bfloat16))
```

```python
import math

import jax
import jax.numpy as jnp
from jax import lax
from jax.experimental import pallas as pl
from jax.experimental.pallas import tpu as pltpu
from jax.sharding import PartitionSpec as P

POWER = 3


DAMPING = 0.1
HIGH = lax.Precision.HIGHEST


def spread(piece):
    return lax.all_gather(piece, "out", axis=2, tiled=True)


def token_sums(maker, rows):
    return lax.psum_scatter(
        maker(jnp.int32(0), rows * lax.axis_size(("tok", "grp"))),
        ("tok", "grp"),
        scatter_dimension=0,
        tiled=True,
    )


def shared_rows(piece):
    return lax.all_gather(piece, ("tok", "grp"), axis=0, tiled=True)


def shared_total(vector):
    return lax.psum(vector, ("tok", "out", "grp"))


def diagonal_mask(rows, width, row_start, col_start):
    row_ids = row_start + lax.broadcasted_iota(jnp.int32, (rows, 1, width), 0)
    col_ids = col_start + lax.broadcasted_iota(jnp.int32, (rows, 1, width), 2)
    return jnp.where(row_ids == col_ids, 1.0, 0.0).astype(jnp.float32)


def multiply(left, right, gather_columns):
    row_band = spread(left)
    column_band = gather_columns(right)
    return jnp.einsum("rkj,jkc->rkc", row_band, column_band, preferred_element_type=jnp.float32)


def inverse_roots(tile, row_start, col_start, gather_columns, total):
    rows, count, width = tile.shape
    block = width * lax.axis_size("out")
    mask = diagonal_mask(rows, width, row_start, col_start)
    vector = jnp.ones((count, block), jnp.float32)
    image = vector
    for step in range(POWER):
        columns = lax.dynamic_slice_in_dim(vector, col_start, width, 1)
        part = jnp.einsum("rkc,kc->kr", tile, columns, precision=HIGH)
        placed = lax.dynamic_update_slice_in_dim(
            jnp.zeros((count, block), jnp.float32), part, row_start, 1
        )
        image = total(placed)
        if step + 1 < POWER:
            vector = image / jnp.sqrt(jnp.sum(image * image, axis=1, keepdims=True))
    scale = jnp.sum(vector * image, axis=1) / jnp.sum(vector * vector, axis=1)
    start = tile / scale[None, :, None]
    start_low = start.astype(jnp.bfloat16)
    first_low = ((3.0 * mask - start) / 2.0).astype(jnp.bfloat16)
    square_low = multiply(first_low, first_low, gather_columns).astype(jnp.bfloat16)
    moved = multiply(square_low, start_low, gather_columns)
    second_low = ((3.0 * mask - moved) / 2.0).astype(jnp.bfloat16)
    roots = multiply(first_low, second_low, gather_columns) / jnp.sqrt(scale)[None, :, None]
    return roots.astype(jnp.bfloat16)


def local(activations, out_grads, weight):
    tok_dev, blocks, width = activations.shape
    block = width * lax.axis_size("out")
    token_count = tok_dev * lax.axis_size("tok") * lax.axis_size("grp")
    col_start = lax.axis_index("out") * width
    local_sides = jnp.concatenate([activations, out_grads], axis=1)
    whole_sides = spread(local_sides)
    grads_whole = whole_sides[:, blocks:, :]
    weight_rows = weight.reshape(blocks, width, blocks, block)
    input_grad = jnp.einsum(
        "tjq,bcjq->tbc", grads_whole, weight_rows, preferred_element_type=jnp.float32
    ).astype(jnp.bfloat16)
    rows = block // (lax.axis_size("tok") * lax.axis_size("grp"))
    row_start = lax.axis_index(("tok", "grp")) * rows

    def shared_terms(start, span):
        return jnp.einsum(
            "tkr,tkc->rkc", whole_sides, local_sides, preferred_element_type=jnp.float32
        )

    sums = token_sums(shared_terms, rows)
    tile = sums / token_count + DAMPING * diagonal_mask(rows, width, row_start, col_start)
    roots = inverse_roots(tile, row_start, col_start, shared_rows, shared_total)
    bands = shared_rows(roots)
    whitened = jnp.einsum(
        "tkj,jkc->tkc", whole_sides, bands, preferred_element_type=jnp.float32
    ).astype(jnp.bfloat16)
    acts_whole = spread(whitened[:, :blocks, :]).reshape(tok_dev, blocks * block)
    grads_low = whitened[:, blocks:, :]
    owned_acts = lax.all_to_all(acts_whole, ("tok", "grp"), split_axis=1, concat_axis=0, tiled=True)
    update = jnp.einsum(
        "ta,tbc->abc",
        owned_acts,
        lax.all_gather(grads_low, ("tok", "grp"), axis=0, tiled=True),
        preferred_element_type=jnp.float32,
    )
    update = (update / math.sqrt(token_count)).astype(jnp.bfloat16)
    return (update, input_grad)


MESH = pl.DeviceIdType.MESH
CHUNKS = 8
PARTS = 4
LATE = 4
BEHIND = 2
LAG = 3


def greet(peers):
    barrier = pltpu.get_barrier_semaphore()
    for peer in peers:
        pl.semaphore_signal(barrier, inc=1, device_id=peer, device_id_type=MESH)
    pl.semaphore_wait(barrier, len(peers))


def remote(src, dst, send, recv, peer):
    return pltpu.make_async_remote_copy(
        src_ref=src, dst_ref=dst, send_sem=send, recv_sem=recv, device_id=peer, device_id_type=MESH
    )


def held(z):
    return z + 2 - 3 * ((z + 2) // 3) + z // 3


def neighbours():
    z, o, y = lax.axis_index("tok"), lax.axis_index("out"), lax.axis_index("grp")
    ox = lax.rem(o + 2, 4)
    oc = o + 1 - 2 * lax.rem(o, 2)
    at = lambda a, b, c: {"tok": a, "out": b, "grp": c}
    zs = [lax.rem(z + j, 4) for j in range(4)]
    peers = [at(zs[j], o, y) for j in (1, 2, 3)]
    return z, o, y, ox, oc, zs, peers, at(z, o, 1 - y), at(z, ox, y), at(z, oc, y)


def hops(z):
    return (z, z + 1 - 2 * lax.rem(z, 2), 2 - z // 2, 3 - 3 * (z // 2))


def gather_kernel(
    pieces, out, sides, low, head, left, right, tail, rays,
    z_send, send, recv, c_send, c_recv, local,
):
    z, o, y, ox, oc, zs, z_peers, y_peer, x_peer, c_peer = neighbours()
    oxc = lax.rem(oc + 2, 4)
    width = pieces.shape[2]
    rows = pieces.shape[1] // PARTS
    group = rows * 8
    tokens, block = sides.shape
    part = out.shape[1]
    near = hops(z)
    across = (((1,), (1,)), ((), ()))
    sent = []

    def columns(oi):
        return pl.ds(pl.multiple_of(oi * width, width), width)

    def tile(oi, yi, zi, s):
        start = pl.multiple_of(((s * 2 + yi) * 4 + zi) * rows, rows)
        return sides.at[pl.ds(start, rows), columns(oi)]

    def piece(zi, s):
        return pieces.at[held(zi), pl.ds(s * rows, rows), :]

    def sem_of(oi, yi, zi, s):
        return recv.at[((oi // 2) * 8 + yi * 4 + zi) * PARTS + s]

    def push(src, where, peer):
        copy = remote(src, tile(*where), send.at[len(sent)], sem_of(*where), peer)
        copy.start()
        sent.append(copy)

    def arrived(*where):
        ref = tile(*where)
        remote(ref, ref, send.at[0], sem_of(*where), c_peer).wait_recv()
        return ref

    def band(oi, s):
        return sides.at[pl.ds(s * group, group), columns(oi)]

    def over_core(oi, s, place):
        n = s * 2 + place
        return remote(band(oi, s), band(oi, s), c_send.at[n], c_recv.at[n], c_peer)

    greet(z_peers + [y_peer, x_peer, c_peer])
    z_sent = []
    for s in range(PARTS):
        for j in (3, 2, 1):
            copy = remote(
                piece(near[j], s), tile(o, y, z, s), z_send.at[len(z_sent)], sem_of(o, y, z, s),
                {"tok": near[j], "out": o, "grp": y},
            )
            copy.start()
            z_sent.append(copy)
        push(piece(z, s), (o, y, z, s), y_peer)
        push(piece(z, s), (o, y, z, s), x_peer)
    owns = []
    for s in range(PARTS):
        owns.append(pltpu.make_async_copy(piece(z, s), tile(o, y, z, s), local.at[s]))
        owns[-1].start()

    ones = jnp.ones((16, block), sides.dtype)

    def gram_group(s):
        here = pl.ds(s * group, group)
        sums = lax.dot_general(ones, sides[here, :], across, preferred_element_type=jnp.float32)
        rays[0:8, here] = sums[0:8]

        def step(i, carry):
            there = pl.ds(pl.multiple_of(i * group, group), group)
            product = lax.dot_general(
                sides[here, :], sides[there, :], across, preferred_element_type=jnp.float32
            )
            low[here, there] = (product * (1.0 / tokens)).astype(low.dtype)
            return carry

        lax.fori_loop(0, s + 1, step, 0)

        def mirror(i, carry):
            there = pl.ds(pl.multiple_of(i * group, group), group)
            product = lax.dot_general(
                sides[there, :], sides[here, :], across, preferred_element_type=jnp.float32
            )
            low[there, here] = (product * (1.0 / tokens)).astype(low.dtype)
            return carry

        if s:
            lax.fori_loop(0, s, mirror, 0)

    order = [(0, s) for s in range(PARTS)]
    order += [(j, s) for s in range(PARTS) for j in (1, 2, 3)]
    last = {s: order.index((3, s)) for s in range(PARTS)}
    for step in range(len(order) + LATE + BEHIND + 1):
        if step < len(order) and order[step][0]:
            j, s = order[step]
            where = (o, y, near[j], s)
            ref = arrived(*where)
            push(ref, where, y_peer)
            push(ref, where, x_peer)
        if LATE <= step < LATE + len(order):
            j, s = order[step - LATE]
            even = (j + s) % 2 == 0
            where = (o, 1 - y, near[j], s)
            ref = arrived(*where)
            if even:
                push(ref, where, x_peer)
            where = (ox, y, near[j], s)
            ref = arrived(*where)
            if not even:
                push(ref, where, y_peer)
            if step - LATE == last[s]:
                owns[s].wait()
                over_core(o, s, 0).start()
        for s in range(PARTS):
            if step == last[s] + LATE + BEHIND:
                for j in range(4):
                    arrived(ox, 1 - y, near[j], s)
                over_core(ox, s, 1).start()
            if step == last[s] + LATE + BEHIND + 1:
                over_core(oc, s, 0).wait_recv()
                over_core(oxc, s, 1).wait_recv()
                gram_group(s)

    def pair(a, b):
        return jnp.sum(a * b, axis=1, keepdims=True)

    def advance(ray):
        high = ray.astype(low.dtype)
        rest = ray - high.astype(jnp.float32)
        middle = rest.astype(low.dtype)
        least = (rest - middle.astype(jnp.float32)).astype(low.dtype)
        zero = jnp.zeros((13, tokens), low.dtype)
        stack = jnp.concatenate([high, middle, least, zero], axis=0)
        image = jnp.dot(stack, low[...], preferred_element_type=jnp.float32)
        return image[0:1] + image[1:2] + image[2:3] + DAMPING * ray

    ray_0 = rays[0:1, :]
    ray_1 = advance(ray_0)
    ray_2 = advance(ray_1)
    dots = [
        pair(ray_0, ray_0),
        pair(ray_0, ray_1),
        pair(ray_1, ray_1),
        pair(ray_1, ray_2),
        pair(ray_2, ray_2),
    ]

    def moment(power):
        total = jnp.full((1, 1), DAMPING**power * block, jnp.float32)
        for i in range(power):
            total = total + DAMPING ** (power - 1 - i) * dots[i] / tokens
        return total

    scale = moment(2 * POWER - 1) / moment(2 * POWER - 2)
    inverse = 1.0 / scale
    root = 1.0 / jnp.sqrt(scale)
    act_start = 2 * (lax.rem(o, 2) * 2 + y) + o // 2
    is_grad = (z // 3) + (3 - z) // 3
    start = (is_grad * (2 * o + y) + (1 - is_grad) * act_start) * part
    cols = pl.ds(pl.multiple_of(start, part), part)
    tall = min(512, tokens)
    steps = tokens // tall

    def span(i):
        return pl.ds(pl.multiple_of(i * tall, tall), tall)

    def apply(i, source, value):
        image = jnp.dot(low[span(i), :], source[...], preferred_element_type=jnp.float32)
        return (image + DAMPING * value) * inverse

    left[...] = sides[:, cols]

    @pl.loop(0, steps)
    def _(i):
        value = left[span(i), :].astype(jnp.float32)
        value = 1.5 * value - 0.5 * apply(i, left, value)
        head[span(i), :] = value
        right[span(i), :] = value.astype(right.dtype)

    @pl.loop(0, steps)
    def _(i):
        value = apply(i, right, head[span(i), :])
        tail[span(i), :] = value
        left[span(i), :] = value.astype(left.dtype)

    @pl.loop(0, steps)
    def _(i):
        value = tail[span(i), :]
        value = 1.5 * value - 0.5 * apply(i, left, value)
        tail[span(i), :] = value
        right[span(i), :] = value.astype(right.dtype)

    @pl.loop(0, steps)
    def _(i):
        value = tail[span(i), :]
        value = 1.5 * value - 0.5 * apply(i, right, value)
        out[span(i), :] = ((1.5 * head[span(i), :] - 0.5 * value) * root).astype(out.dtype)

    for copy in z_sent:
        copy.wait_send()
    for copy in sent:
        copy.wait_send()
    for s in range(PARTS):
        over_core(o, s, 0).wait_send()
        over_core(ox, s, 1).wait_send()


def gather(pieces, part):
    _, rows, width = pieces.shape
    tokens, block = rows * 8, width * 4
    dma = pltpu.SemaphoreType.DMA
    vmem = pl.BlockSpec(memory_space=pltpu.VMEM)
    sends = (2 * 4 + 2 * 4) * PARTS
    return pl.pallas_call(
        gather_kernel,
        out_shape=jax.ShapeDtypeStruct((tokens, part), pieces.dtype),
        in_specs=[vmem],
        out_specs=vmem,
        scratch_shapes=[
            pltpu.VMEM((tokens, block), pieces.dtype),
            pltpu.VMEM((tokens, tokens), pieces.dtype),
            pltpu.VMEM((tokens, part), jnp.float32),
            pltpu.VMEM((tokens, part), pieces.dtype),
            pltpu.VMEM((tokens, part), pieces.dtype),
            pltpu.VMEM((tokens, part), jnp.float32),
            pltpu.VMEM((8, tokens), jnp.float32),
            dma((3 * PARTS,)),
            dma((sends,)),
            dma((16 * PARTS,)),
            dma((2 * PARTS,)),
            dma((2 * PARTS,)),
            dma((PARTS,)),
        ],
        compiler_params=pltpu.CompilerParams(collective_id=0, has_side_effects=True),
        name="gather",
    )(pieces)


def deliver_kernel(
    low, pieces, weight, grads, acts, product,
    raw, held_weight, w_sem, r_send, r_recv, g_send, y_send, g_recv, y_recv,
    a_send, a_recv, x_send, x_recv, c_send, c_recv, local,
):
    z, o, y, ox, oc, zs, z_peers, y_peer, x_peer, c_peer = neighbours()
    tokens, part = low.shape
    rows = tokens // CHUNKS
    width = pieces.shape[2]
    block = raw.shape[2]
    strip = width // 2
    is_grad = (z == 0) | (z == 3)
    is_act = jnp.logical_not(is_grad)
    mine = z // 3
    h = o // 2
    goal_z = (z // 2) * 2 + lax.rem(o, 2)
    stays = goal_z == z
    goal = {"tok": goal_z, "out": o, "grp": y}
    near, far = z // 2, 1 - z // 2
    is_hub = lax.rem(o, 2) == lax.rem(z, 2)
    here = is_act & stays
    greet(z_peers + [y_peer, x_peer, c_peer])

    def band(oi):
        return raw.at[:, :, pl.ds(pl.multiple_of(oi * width, width), width)]

    own_raw = pieces.at[2:4]
    raw_local = pltpu.make_async_copy(own_raw, band(o), r_send.at[3])
    raw_x = remote(own_raw, band(o), r_send.at[0], r_recv.at[0], x_peer)
    raw_c = remote(own_raw, band(o), r_send.at[1], r_recv.at[1], c_peer)
    raw_xc = remote(band(ox), band(ox), r_send.at[2], r_recv.at[2], c_peer)
    raw_x.start()
    raw_c.start()
    raw_local.start()

    def span(c):
        return pl.ds(c * rows, rows)

    def piece(c):
        return low.at[span(c), :]

    def half(i):
        return pl.ds(pl.multiple_of(i * part, part), part)

    def g_tile(b, yi, c):
        return grads.at[b, span(c), half(yi)]

    def a_tile(i, c):
        return acts.at[span(c), half(i)]

    def own_grad(c):
        return pltpu.make_async_copy(piece(c), g_tile(mine, y, c), local.at[c])

    def own_act(c):
        return pltpu.make_async_copy(piece(c), a_tile(h, c), local.at[c])

    def to_plane(src, b, c):
        return remote(src, g_tile(b, y, c), g_send.at[b * CHUNKS + c], g_recv.at[b * CHUNKS + c], {"tok": lax.rem(z + 5 - 2 * b, 4), "out": o, "grp": y})

    def y_copy(src, b, c):
        return remote(src, g_tile(b, y, c), y_send.at[b * CHUNKS + c], y_recv.at[b * CHUNKS + c], y_peer)

    def to_hub(c):
        return remote(piece(c), a_tile(h, c), a_send.at[c], a_recv.at[c], goal)

    def over_x(c, i):
        return remote(a_tile(i, c), a_tile(i, c), x_send.at[c], x_recv.at[c], x_peer)

    def over_core(c, i):
        place = i * CHUNKS + c
        return remote(a_tile(i, c), a_tile(i, c), c_send.at[place], c_recv.at[place], c_peer)

    for c in range(CHUNKS):
        for b in range(2):

            @pl.when(z == 3 * b)
            def _():
                to_plane(piece(c), b, c).start()
                y_copy(piece(c), b, c).start()

        @pl.when(is_grad)
        def _():
            own_grad(c).start()

        @pl.when(here)
        def _():
            own_act(c).start()

        @pl.when(is_act & jnp.logical_not(stays))
        def _():
            to_hub(c).start()

    strips = [(b, i) for b in range(2) for i in range(2)]

    def load(n):
        b, i = strips[n]
        place = (b, pl.ds(i * strip, strip), slice(None))
        return pltpu.make_async_copy(weight.at[place], held_weight.at[place], w_sem.at[n])

    for n in range(4):
        load(n).start()

    def multiply(n):
        b, i = strips[n]
        load(n).wait()
        total = jnp.zeros((raw.shape[1], strip), jnp.float32)
        for k in range(2):
            total += lax.dot_general(
                raw[k],
                held_weight[b, pl.ds(i * strip, strip), pl.ds(k * block, block)],
                (((1,), (1,)), ((), ())),
                preferred_element_type=jnp.float32,
            )
        product[b, :, pl.ds(i * strip, strip)] = total.astype(product.dtype)

    def hub_step(c):
        @pl.when(here)
        def _():
            own_act(c).wait()

        @pl.when(is_hub & jnp.logical_not(here))
        def _():
            ref = a_tile(h, c)
            remote(ref, ref, a_send.at[0], a_recv.at[c], c_peer).wait_recv()

        @pl.when(is_hub)
        def _():
            over_x(c, h).start()
            over_core(c, h).start()

    def cross_step(c):
        @pl.when(is_hub)
        def _():
            over_x(c, 1 - h).wait_recv()
            over_core(c, 1 - h).start()

    def take(b, c):
        ref = g_tile(b, y, c)
        remote(ref, ref, g_send.at[0], g_recv.at[b * CHUNKS + c], c_peer).wait_recv()

        @pl.when(is_act)
        def _():
            to_plane(ref, b, c).start()

        y_copy(ref, b, c).start()

    for step in range(CHUNKS + LAG):
        if step < CHUNKS:

            @pl.when(is_act)
            def _():
                take(near, step)

            hub_step(step)
        if step >= LAG:
            take(far, step - LAG)
        if step == 1:
            raw_x.wait_recv()
            raw_xc.start()
        if step == 2:
            raw_c.wait_recv()
            raw_xc.wait()
            raw_local.wait()
        if 3 <= step < 7:
            multiply(step - 3)
    for c in range(CHUNKS):
        cross_step(c)
    for c in range(CHUNKS):
        for b in range(2):
            ref = g_tile(b, 1 - y, c)
            remote(ref, ref, y_send.at[0], y_recv.at[b * CHUNKS + c], c_peer).wait_recv()
            y_copy(g_tile(b, y, c), b, c).wait_send()

            @pl.when(z != 3 - 3 * b)
            def _():
                to_plane(g_tile(b, y, c), b, c).wait_send()

        @pl.when(is_grad)
        def _():
            own_grad(c).wait()

        @pl.when(is_act & jnp.logical_not(stays))
        def _():
            to_hub(c).wait_send()

        for i in range(2):

            @pl.when(is_hub)
            def _():
                over_core(c, i).wait_send()

            @pl.when(jnp.logical_not(is_hub))
            def _():
                over_core(c, i).wait_recv()

        @pl.when(is_hub)
        def _():
            over_x(c, h).wait_send()

    raw_x.wait_send()
    raw_c.wait_send()


def deliver(low, pieces, weight):
    tokens, part = low.shape
    _, rows, width = pieces.shape
    dma = pltpu.SemaphoreType.DMA
    vmem = pl.BlockSpec(memory_space=pltpu.VMEM)
    return pl.pallas_call(
        deliver_kernel,
        out_shape=(
            jax.ShapeDtypeStruct((2, tokens, 2 * part), low.dtype),
            jax.ShapeDtypeStruct((tokens, 2 * part), low.dtype),
            jax.ShapeDtypeStruct((2, rows, width), low.dtype),
        ),
        in_specs=[vmem, vmem, pl.BlockSpec(memory_space=pl.ANY)],
        out_specs=(vmem, vmem, vmem),
        scratch_shapes=[
            pltpu.VMEM((2, rows, 4 * width), low.dtype),
            pltpu.VMEM(weight.shape, weight.dtype),
            dma((4,)),
            dma((4,)),
            dma((3,)),
            dma((2 * CHUNKS,)),
            dma((2 * CHUNKS,)),
            dma((2 * CHUNKS,)),
            dma((2 * CHUNKS,)),
            dma((CHUNKS,)),
            dma((CHUNKS,)),
            dma((CHUNKS,)),
            dma((CHUNKS,)),
            dma((2 * CHUNKS,)),
            dma((2 * CHUNKS,)),
            dma((CHUNKS,)),
        ],
        compiler_params=pltpu.CompilerParams(collective_id=1, has_side_effects=True),
        name="deliver",
    )(low, pieces, weight)


def planes(activations, out_grads, weight):
    tok_dev, _, width = activations.shape
    part = width // lax.axis_size("grp")
    token_count = tok_dev * lax.axis_size(("tok", "grp"))
    pieces = jnp.swapaxes(jnp.concatenate([activations, out_grads], axis=1), 0, 1)
    grads_low, acts_low, product = deliver(gather(pieces, part), pieces, weight)
    update = jnp.einsum("ta,btc->abc", acts_low, grads_low, preferred_element_type=jnp.float32)
    update = (update / math.sqrt(token_count)).astype(jnp.bfloat16)
    input_grad = jnp.swapaxes(product, 0, 1)
    return (update, input_grad)


def solution(mesh):
    in_specs = (
        P(("tok", "grp"), None, "out"),
        P(("tok", "grp"), None, "out"),
        P(None, "out", None),
    )
    out_specs = (P(("tok", "grp"), None, "out"), P(("tok", "grp"), None, "out"))

    def body(activations, out_grads, weight):
        blocks = activations.shape[1]
        tok, grp, out = (mesh.shape[name] for name in ("tok", "grp", "out"))
        fits = (blocks, tok, grp, out) == (2, 4, 2, 4)
        return (planes if fits else local)(activations, out_grads, weight)

    return jax.shard_map(body, mesh=mesh, in_specs=in_specs, out_specs=out_specs, check_vma=False)
```

```python
import math

import jax
import jax.numpy as jnp
from jax import lax
from jax.experimental import pallas as pl
from jax.experimental.pallas import tpu as pltpu
from jax.sharding import PartitionSpec as P

POWER = 3


DAMPING = 0.1
HIGH = lax.Precision.HIGHEST


def spread(piece):
    return lax.all_gather(piece, "out", axis=2, tiled=True)


def token_sums(maker, rows):
    return lax.psum_scatter(
        maker(jnp.int32(0), rows * lax.axis_size(("tok", "grp"))),
        ("tok", "grp"),
        scatter_dimension=0,
        tiled=True,
    )


def shared_rows(piece):
    return lax.all_gather(piece, ("tok", "grp"), axis=0, tiled=True)


def shared_total(vector):
    return lax.psum(vector, ("tok", "out", "grp"))


def diagonal_mask(rows, width, row_start, col_start):
    row_ids = row_start + lax.broadcasted_iota(jnp.int32, (rows, 1, width), 0)
    col_ids = col_start + lax.broadcasted_iota(jnp.int32, (rows, 1, width), 2)
    return jnp.where(row_ids == col_ids, 1.0, 0.0).astype(jnp.float32)


def multiply(left, right, gather_columns):
    row_band = spread(left)
    column_band = gather_columns(right)
    return jnp.einsum("rkj,jkc->rkc", row_band, column_band, preferred_element_type=jnp.float32)


def inverse_roots(tile, row_start, col_start, gather_columns, total):
    rows, count, width = tile.shape
    block = width * lax.axis_size("out")
    mask = diagonal_mask(rows, width, row_start, col_start)
    vector = jnp.ones((count, block), jnp.float32)
    image = vector
    for step in range(POWER):
        columns = lax.dynamic_slice_in_dim(vector, col_start, width, 1)
        part = jnp.einsum("rkc,kc->kr", tile, columns, precision=HIGH)
        placed = lax.dynamic_update_slice_in_dim(
            jnp.zeros((count, block), jnp.float32), part, row_start, 1
        )
        image = total(placed)
        if step + 1 < POWER:
            vector = image / jnp.sqrt(jnp.sum(image * image, axis=1, keepdims=True))
    scale = jnp.sum(vector * image, axis=1) / jnp.sum(vector * vector, axis=1)
    start = tile / scale[None, :, None]
    start_low = start.astype(jnp.bfloat16)
    first_low = ((3.0 * mask - start) / 2.0).astype(jnp.bfloat16)
    square_low = multiply(first_low, first_low, gather_columns).astype(jnp.bfloat16)
    moved = multiply(square_low, start_low, gather_columns)
    second_low = ((3.0 * mask - moved) / 2.0).astype(jnp.bfloat16)
    roots = multiply(first_low, second_low, gather_columns) / jnp.sqrt(scale)[None, :, None]
    return roots.astype(jnp.bfloat16)


def local(activations, out_grads, weight):
    tok_dev, blocks, width = activations.shape
    block = width * lax.axis_size("out")
    token_count = tok_dev * lax.axis_size("tok") * lax.axis_size("grp")
    col_start = lax.axis_index("out") * width
    local_sides = jnp.concatenate([activations, out_grads], axis=1)
    whole_sides = spread(local_sides)
    grads_whole = whole_sides[:, blocks:, :]
    weight_rows = weight.reshape(blocks, width, blocks, block)
    input_grad = jnp.einsum(
        "tjq,bcjq->tbc", grads_whole, weight_rows, preferred_element_type=jnp.float32
    ).astype(jnp.bfloat16)
    rows = block // (lax.axis_size("tok") * lax.axis_size("grp"))
    row_start = lax.axis_index(("tok", "grp")) * rows

    def shared_terms(start, span):
        return jnp.einsum(
            "tkr,tkc->rkc", whole_sides, local_sides, preferred_element_type=jnp.float32
        )

    sums = token_sums(shared_terms, rows)
    tile = sums / token_count + DAMPING * diagonal_mask(rows, width, row_start, col_start)
    roots = inverse_roots(tile, row_start, col_start, shared_rows, shared_total)
    bands = shared_rows(roots)
    whitened = jnp.einsum(
        "tkj,jkc->tkc", whole_sides, bands, preferred_element_type=jnp.float32
    ).astype(jnp.bfloat16)
    acts_whole = spread(whitened[:, :blocks, :]).reshape(tok_dev, blocks * block)
    grads_low = whitened[:, blocks:, :]
    owned_acts = lax.all_to_all(acts_whole, ("tok", "grp"), split_axis=1, concat_axis=0, tiled=True)
    update = jnp.einsum(
        "ta,tbc->abc",
        owned_acts,
        lax.all_gather(grads_low, ("tok", "grp"), axis=0, tiled=True),
        preferred_element_type=jnp.float32,
    )
    update = (update / math.sqrt(token_count)).astype(jnp.bfloat16)
    return (update, input_grad)


MESH = pl.DeviceIdType.MESH
CHUNKS = 8
PARTS = 4
PLAN = (
    ("y", 0, 0), ("x", 0, 0), ("y", 0, 1), ("x", 0, 1), ("z", 1, 0), ("y", 0, 2), ("x", 0, 2),
    ("z", 2, 0), ("y", 0, 3), ("x", 0, 3), ("z", 3, 0), ("z", 1, 1), ("z", 2, 1), ("y", 1, 0),
    ("y", 2, 0), ("x", 1, 0), ("z", 1, 2), ("z", 3, 1), ("x", 2, 0), ("z", 2, 2), ("x", 1, 1),
    ("y", 1, 1), ("x", 3, 0), ("z", 1, 3), ("y", 3, 0), ("c", 0, 0), ("z", 3, 2), ("x", 2, 1),
    ("x", 1, 2), ("y", 1, 2), ("y", 2, 1), ("z", 2, 3), ("y", 3, 1), ("c", 0, 1), ("z", 3, 3),
    ("x", 3, 1), ("y", 2, 2), ("x", 2, 2), ("x", 1, 3), ("d", 0, 0), ("x", 3, 2), ("y", 1, 3),
    ("y", 3, 2), ("c", 0, 2), ("x", 2, 3), ("d", 0, 1), ("y", 2, 3), ("x", 3, 3), ("y", 3, 3),
    ("c", 0, 3), ("d", 0, 2), ("d", 0, 3),
)
LAG = 3


def greet(peers):
    barrier = pltpu.get_barrier_semaphore()
    for peer in peers:
        pl.semaphore_signal(barrier, inc=1, device_id=peer, device_id_type=MESH)
    pl.semaphore_wait(barrier, len(peers))


def remote(src, dst, send, recv, peer):
    return pltpu.make_async_remote_copy(
        src_ref=src, dst_ref=dst, send_sem=send, recv_sem=recv, device_id=peer, device_id_type=MESH
    )


def held(z):
    return z + 2 - 3 * ((z + 2) // 3) + z // 3


def neighbours():
    z, o, y = lax.axis_index("tok"), lax.axis_index("out"), lax.axis_index("grp")
    ox = lax.rem(o + 2, 4)
    oc = o + 1 - 2 * lax.rem(o, 2)
    at = lambda a, b, c: {"tok": a, "out": b, "grp": c}
    zs = [lax.rem(z + j, 4) for j in range(4)]
    peers = [at(zs[j], o, y) for j in (1, 2, 3)]
    return z, o, y, ox, oc, zs, peers, at(z, o, 1 - y), at(z, ox, y), at(z, oc, y)


def hops(z):
    return (z, z + 1 - 2 * lax.rem(z, 2), 2 - z // 2, 3 - 3 * (z // 2))


def gather_kernel(
    pieces, out, sides, low, head, left, right, tail, rays,
    z_send, send, recv, c_send, c_recv, local,
):
    z, o, y, ox, oc, zs, z_peers, y_peer, x_peer, c_peer = neighbours()
    oxc = lax.rem(oc + 2, 4)
    width = pieces.shape[2]
    rows = pieces.shape[1] // PARTS
    group = rows * 8
    tokens, block = sides.shape
    part = out.shape[1]
    near = hops(z)
    across = (((1,), (1,)), ((), ()))
    sent = []

    def columns(oi):
        return pl.ds(pl.multiple_of(oi * width, width), width)

    def tile(oi, yi, zi, s):
        start = pl.multiple_of(((s * 2 + yi) * 4 + zi) * rows, rows)
        return sides.at[pl.ds(start, rows), columns(oi)]

    def piece(zi, s):
        return pieces.at[held(zi), pl.ds(s * rows, rows), :]

    def sem_of(oi, yi, zi, s):
        return recv.at[((oi // 2) * 8 + yi * 4 + zi) * PARTS + s]

    def push(src, where, peer):
        copy = remote(src, tile(*where), send.at[len(sent)], sem_of(*where), peer)
        copy.start()
        sent.append(copy)

    def arrived(*where):
        ref = tile(*where)
        remote(ref, ref, send.at[0], sem_of(*where), c_peer).wait_recv()
        return ref

    def band(oi, s):
        return sides.at[pl.ds(s * group, group), columns(oi)]

    def over_core(oi, s, place):
        n = s * 2 + place
        return remote(band(oi, s), band(oi, s), c_send.at[n], c_recv.at[n], c_peer)

    d_peer = {"tok": z, "out": ox, "grp": 1 - y}
    greet(z_peers + [y_peer, x_peer, c_peer, d_peer])
    z_sent = []
    for s in range(PARTS):
        for j in (3, 2, 1):
            copy = remote(
                piece(near[j], s), tile(o, y, z, s), z_send.at[len(z_sent)], sem_of(o, y, z, s),
                {"tok": near[j], "out": o, "grp": y},
            )
            copy.start()
            z_sent.append(copy)
        push(piece(z, s), (o, y, z, s), y_peer)
        push(piece(z, s), (o, y, z, s), x_peer)
    owns = []
    for s in range(PARTS):
        owns.append(pltpu.make_async_copy(piece(z, s), tile(o, y, z, s), local.at[s]))
        owns[-1].start()

    ones = jnp.ones((16, block), sides.dtype)

    def rows_of(s):
        return pl.ds(s * group, group)

    def gram_group(s, known):
        here = rows_of(s)
        sums = lax.dot_general(ones, sides[here, :], across, preferred_element_type=jnp.float32)
        rays[0:8, here] = sums[0:8]
        for i in known + [s]:
            there = rows_of(i)
            product = lax.dot_general(
                sides[there, :], sides[here, :], across, preferred_element_type=jnp.float32
            )
            product = product * (1.0 / tokens)
            low[there, here] = product.astype(low.dtype)
            if i != s:
                low[here, there] = jnp.transpose(product).astype(low.dtype)

    def straight(j, s):
        return j == 3 and s == PARTS - 1

    def finish(s):
        over_core(oc, s, 0).wait_recv()
        over_core(oxc, s, 1).wait_recv()
        gram_group(s, known)
        known.append(s)

    known = []
    waiting = []
    for kind, j, s in PLAN:
        if kind == "z":
            where = (o, y, near[j], s)
            ref = arrived(*where)
            push(ref, where, y_peer)
            push(ref, where, x_peer)
            if straight(j, s):
                push(ref, where, d_peer)
        elif kind == "y":
            where = (o, 1 - y, near[j], s)
            ref = arrived(*where)
            if (j + s) % 2 == 0 and not straight(j, s):
                push(ref, where, x_peer)
        elif kind == "x":
            where = (ox, y, near[j], s)
            ref = arrived(*where)
            if (j + s) % 2 == 1 and not straight(j, s):
                push(ref, where, y_peer)
        elif kind == "c":
            owns[s].wait()
            over_core(o, s, 0).start()
        else:
            for i in range(4):
                arrived(ox, 1 - y, near[i], s)
            over_core(ox, s, 1).start()
            if waiting:
                finish(waiting.pop())
            waiting.append(s)
    finish(waiting.pop())

    def pair(a, b):
        return jnp.sum(a * b, axis=1, keepdims=True)

    def advance(ray):
        high = ray.astype(low.dtype)
        rest = ray - high.astype(jnp.float32)
        middle = rest.astype(low.dtype)
        least = (rest - middle.astype(jnp.float32)).astype(low.dtype)
        zero = jnp.zeros((13, tokens), low.dtype)
        stack = jnp.concatenate([high, middle, least, zero], axis=0)
        image = jnp.dot(stack, low[...], preferred_element_type=jnp.float32)
        return image[0:1] + image[1:2] + image[2:3] + DAMPING * ray

    ray_0 = rays[0:1, :]
    ray_1 = advance(ray_0)
    ray_2 = advance(ray_1)
    dots = [
        pair(ray_0, ray_0),
        pair(ray_0, ray_1),
        pair(ray_1, ray_1),
        pair(ray_1, ray_2),
        pair(ray_2, ray_2),
    ]

    def moment(power):
        total = jnp.full((1, 1), DAMPING**power * block, jnp.float32)
        for i in range(power):
            total = total + DAMPING ** (power - 1 - i) * dots[i] / tokens
        return total

    scale = moment(2 * POWER - 1) / moment(2 * POWER - 2)
    inverse = 1.0 / scale
    root = 1.0 / jnp.sqrt(scale)
    act_start = 2 * (lax.rem(o, 2) * 2 + y) + o // 2
    is_grad = (z // 3) + (3 - z) // 3
    start = (is_grad * (2 * o + y) + (1 - is_grad) * act_start) * part
    cols = pl.ds(pl.multiple_of(start, part), part)
    tall = min(512, tokens)
    steps = tokens // tall

    def span(i):
        return pl.ds(pl.multiple_of(i * tall, tall), tall)

    def apply(i, source, value):
        image = jnp.dot(low[span(i), :], source[...], preferred_element_type=jnp.float32)
        return (image + DAMPING * value) * inverse

    left[...] = sides[:, cols]

    @pl.loop(0, steps)
    def _(i):
        value = left[span(i), :].astype(jnp.float32)
        value = 1.5 * value - 0.5 * apply(i, left, value)
        head[span(i), :] = value
        right[span(i), :] = value.astype(right.dtype)

    @pl.loop(0, steps)
    def _(i):
        value = apply(i, right, head[span(i), :])
        tail[span(i), :] = value
        left[span(i), :] = value.astype(left.dtype)

    @pl.loop(0, steps)
    def _(i):
        value = tail[span(i), :]
        value = 1.5 * value - 0.5 * apply(i, left, value)
        tail[span(i), :] = value
        right[span(i), :] = value.astype(right.dtype)

    @pl.loop(0, steps)
    def _(i):
        value = tail[span(i), :]
        value = 1.5 * value - 0.5 * apply(i, right, value)
        out[span(i), :] = ((1.5 * head[span(i), :] - 0.5 * value) * root).astype(out.dtype)

    for copy in z_sent:
        copy.wait_send()
    for copy in sent:
        copy.wait_send()
    for s in range(PARTS):
        over_core(o, s, 0).wait_send()
        over_core(ox, s, 1).wait_send()


def gather(pieces, part):
    _, rows, width = pieces.shape
    tokens, block = rows * 8, width * 4
    dma = pltpu.SemaphoreType.DMA
    vmem = pl.BlockSpec(memory_space=pltpu.VMEM)
    sends = (2 * 4 + 2 * 4) * PARTS
    return pl.pallas_call(
        gather_kernel,
        out_shape=jax.ShapeDtypeStruct((tokens, part), pieces.dtype),
        in_specs=[vmem],
        out_specs=vmem,
        scratch_shapes=[
            pltpu.VMEM((tokens, block), pieces.dtype),
            pltpu.VMEM((tokens, tokens), pieces.dtype),
            pltpu.VMEM((tokens, part), jnp.float32),
            pltpu.VMEM((tokens, part), pieces.dtype),
            pltpu.VMEM((tokens, part), pieces.dtype),
            pltpu.VMEM((tokens, part), jnp.float32),
            pltpu.VMEM((8, tokens), jnp.float32),
            dma((3 * PARTS,)),
            dma((sends,)),
            dma((16 * PARTS,)),
            dma((2 * PARTS,)),
            dma((2 * PARTS,)),
            dma((PARTS,)),
        ],
        compiler_params=pltpu.CompilerParams(collective_id=0, has_side_effects=True),
        name="gather",
    )(pieces)


def deliver_kernel(
    low, pieces, weight, grads, acts, product,
    raw, held_weight, w_sem, r_send, r_recv, g_send, y_send, g_recv, y_recv,
    a_send, a_recv, x_send, x_recv, c_send, c_recv, local,
):
    z, o, y, ox, oc, zs, z_peers, y_peer, x_peer, c_peer = neighbours()
    tokens, part = low.shape
    rows = tokens // CHUNKS
    width = pieces.shape[2]
    block = raw.shape[2]
    strip = width // 2
    is_grad = (z == 0) | (z == 3)
    is_act = jnp.logical_not(is_grad)
    mine = z // 3
    h = o // 2
    goal_z = (z // 2) * 2 + lax.rem(o, 2)
    stays = goal_z == z
    goal = {"tok": goal_z, "out": o, "grp": y}
    near, far = z // 2, 1 - z // 2
    is_hub = lax.rem(o, 2) == lax.rem(z, 2)
    here = is_act & stays
    greet(z_peers + [y_peer, x_peer, c_peer])

    def band(oi):
        return raw.at[:, :, pl.ds(pl.multiple_of(oi * width, width), width)]

    own_raw = pieces.at[2:4]
    raw_local = pltpu.make_async_copy(own_raw, band(o), r_send.at[3])
    raw_x = remote(own_raw, band(o), r_send.at[0], r_recv.at[0], x_peer)
    raw_c = remote(own_raw, band(o), r_send.at[1], r_recv.at[1], c_peer)
    raw_xc = remote(band(ox), band(ox), r_send.at[2], r_recv.at[2], c_peer)
    raw_x.start()
    raw_c.start()
    raw_local.start()

    def span(c):
        return pl.ds(c * rows, rows)

    def piece(c):
        return low.at[span(c), :]

    def half(i):
        return pl.ds(pl.multiple_of(i * part, part), part)

    def g_tile(b, yi, c):
        return grads.at[b, span(c), half(yi)]

    def a_tile(i, c):
        return acts.at[span(c), half(i)]

    def own_grad(c):
        return pltpu.make_async_copy(piece(c), g_tile(mine, y, c), local.at[c])

    def own_act(c):
        return pltpu.make_async_copy(piece(c), a_tile(h, c), local.at[c])

    def to_plane(src, b, c):
        return remote(src, g_tile(b, y, c), g_send.at[b * CHUNKS + c], g_recv.at[b * CHUNKS + c], {"tok": lax.rem(z + 5 - 2 * b, 4), "out": o, "grp": y})

    def y_copy(src, b, c):
        return remote(src, g_tile(b, y, c), y_send.at[b * CHUNKS + c], y_recv.at[b * CHUNKS + c], y_peer)

    def to_hub(c):
        return remote(piece(c), a_tile(h, c), a_send.at[c], a_recv.at[c], goal)

    def over_x(c, i):
        return remote(a_tile(i, c), a_tile(i, c), x_send.at[c], x_recv.at[c], x_peer)

    def over_core(c, i):
        place = i * CHUNKS + c
        return remote(a_tile(i, c), a_tile(i, c), c_send.at[place], c_recv.at[place], c_peer)

    for c in range(CHUNKS):
        for b in range(2):

            @pl.when(z == 3 * b)
            def _():
                to_plane(piece(c), b, c).start()
                y_copy(piece(c), b, c).start()

        @pl.when(is_grad)
        def _():
            own_grad(c).start()

        @pl.when(here)
        def _():
            own_act(c).start()

        @pl.when(is_act & jnp.logical_not(stays))
        def _():
            to_hub(c).start()

    strips = [(b, i) for b in range(2) for i in range(2)]

    def load(n):
        b, i = strips[n]
        place = (b, pl.ds(i * strip, strip), slice(None))
        return pltpu.make_async_copy(weight.at[place], held_weight.at[place], w_sem.at[n])

    for n in range(4):
        load(n).start()

    def multiply(n):
        b, i = strips[n]
        load(n).wait()
        total = jnp.zeros((raw.shape[1], strip), jnp.float32)
        for k in range(2):
            total += lax.dot_general(
                raw[k],
                held_weight[b, pl.ds(i * strip, strip), pl.ds(k * block, block)],
                (((1,), (1,)), ((), ())),
                preferred_element_type=jnp.float32,
            )
        product[b, :, pl.ds(i * strip, strip)] = total.astype(product.dtype)

    def hub_step(c):
        @pl.when(here)
        def _():
            own_act(c).wait()

        @pl.when(is_hub & jnp.logical_not(here))
        def _():
            ref = a_tile(h, c)
            remote(ref, ref, a_send.at[0], a_recv.at[c], c_peer).wait_recv()

        @pl.when(is_hub)
        def _():
            over_x(c, h).start()
            over_core(c, h).start()

    def cross_step(c):
        @pl.when(is_hub)
        def _():
            over_x(c, 1 - h).wait_recv()
            over_core(c, 1 - h).start()

    def take(b, c):
        ref = g_tile(b, y, c)
        remote(ref, ref, g_send.at[0], g_recv.at[b * CHUNKS + c], c_peer).wait_recv()

        @pl.when(is_act)
        def _():
            to_plane(ref, b, c).start()

        y_copy(ref, b, c).start()

    for step in range(CHUNKS + LAG):
        if step < CHUNKS:

            @pl.when(is_act)
            def _():
                take(near, step)

            hub_step(step)
        if step >= LAG:
            take(far, step - LAG)
        if step == 1:
            raw_x.wait_recv()
            raw_xc.start()
        if step == 2:
            raw_c.wait_recv()
            raw_xc.wait()
            raw_local.wait()
        if 3 <= step < 7:
            multiply(step - 3)
    for c in range(CHUNKS):
        cross_step(c)
    for c in range(CHUNKS):
        for b in range(2):
            ref = g_tile(b, 1 - y, c)
            remote(ref, ref, y_send.at[0], y_recv.at[b * CHUNKS + c], c_peer).wait_recv()
            y_copy(g_tile(b, y, c), b, c).wait_send()

            @pl.when(z != 3 - 3 * b)
            def _():
                to_plane(g_tile(b, y, c), b, c).wait_send()

        @pl.when(is_grad)
        def _():
            own_grad(c).wait()

        @pl.when(is_act & jnp.logical_not(stays))
        def _():
            to_hub(c).wait_send()

        for i in range(2):

            @pl.when(is_hub)
            def _():
                over_core(c, i).wait_send()

            @pl.when(jnp.logical_not(is_hub))
            def _():
                over_core(c, i).wait_recv()

        @pl.when(is_hub)
        def _():
            over_x(c, h).wait_send()

    raw_x.wait_send()
    raw_c.wait_send()


def deliver(low, pieces, weight):
    tokens, part = low.shape
    _, rows, width = pieces.shape
    dma = pltpu.SemaphoreType.DMA
    vmem = pl.BlockSpec(memory_space=pltpu.VMEM)
    return pl.pallas_call(
        deliver_kernel,
        out_shape=(
            jax.ShapeDtypeStruct((2, tokens, 2 * part), low.dtype),
            jax.ShapeDtypeStruct((tokens, 2 * part), low.dtype),
            jax.ShapeDtypeStruct((2, rows, width), low.dtype),
        ),
        in_specs=[vmem, vmem, pl.BlockSpec(memory_space=pl.ANY)],
        out_specs=(vmem, vmem, vmem),
        scratch_shapes=[
            pltpu.VMEM((2, rows, 4 * width), low.dtype),
            pltpu.VMEM(weight.shape, weight.dtype),
            dma((4,)),
            dma((4,)),
            dma((3,)),
            dma((2 * CHUNKS,)),
            dma((2 * CHUNKS,)),
            dma((2 * CHUNKS,)),
            dma((2 * CHUNKS,)),
            dma((CHUNKS,)),
            dma((CHUNKS,)),
            dma((CHUNKS,)),
            dma((CHUNKS,)),
            dma((2 * CHUNKS,)),
            dma((2 * CHUNKS,)),
            dma((CHUNKS,)),
        ],
        compiler_params=pltpu.CompilerParams(collective_id=1, has_side_effects=True),
        name="deliver",
    )(low, pieces, weight)


def planes(activations, out_grads, weight):
    tok_dev, _, width = activations.shape
    part = width // lax.axis_size("grp")
    token_count = tok_dev * lax.axis_size(("tok", "grp"))
    pieces = jnp.swapaxes(jnp.concatenate([activations, out_grads], axis=1), 0, 1)
    grads_low, acts_low, product = deliver(gather(pieces, part), pieces, weight)
    update = jnp.einsum("ta,btc->abc", acts_low, grads_low, preferred_element_type=jnp.float32)
    update = (update / math.sqrt(token_count)).astype(jnp.bfloat16)
    input_grad = jnp.swapaxes(product, 0, 1)
    return (update, input_grad)


def solution(mesh):
    in_specs = (
        P(("tok", "grp"), None, "out"),
        P(("tok", "grp"), None, "out"),
        P(None, "out", None),
    )
    out_specs = (P(("tok", "grp"), None, "out"), P(("tok", "grp"), None, "out"))

    def body(activations, out_grads, weight):
        blocks = activations.shape[1]
        tok, grp, out = (mesh.shape[name] for name in ("tok", "grp", "out"))
        fits = (blocks, tok, grp, out) == (2, 4, 2, 4)
        return (planes if fits else local)(activations, out_grads, weight)

    return jax.shard_map(body, mesh=mesh, in_specs=in_specs, out_specs=out_specs, check_vma=False)
```

```python
import math

import jax
import jax.numpy as jnp
from jax import lax
from jax.experimental import pallas as pl
from jax.experimental.pallas import tpu as pltpu
from jax.sharding import PartitionSpec as P

POWER = 3


DAMPING = 0.1
HIGH = lax.Precision.HIGHEST


def spread(piece):
    return lax.all_gather(piece, "out", axis=2, tiled=True)


def token_sums(maker, rows):
    return lax.psum_scatter(
        maker(jnp.int32(0), rows * lax.axis_size(("tok", "grp"))),
        ("tok", "grp"),
        scatter_dimension=0,
        tiled=True,
    )


def shared_rows(piece):
    return lax.all_gather(piece, ("tok", "grp"), axis=0, tiled=True)


def shared_total(vector):
    return lax.psum(vector, ("tok", "out", "grp"))


def diagonal_mask(rows, width, row_start, col_start):
    row_ids = row_start + lax.broadcasted_iota(jnp.int32, (rows, 1, width), 0)
    col_ids = col_start + lax.broadcasted_iota(jnp.int32, (rows, 1, width), 2)
    return jnp.where(row_ids == col_ids, 1.0, 0.0).astype(jnp.float32)


def multiply(left, right, gather_columns):
    row_band = spread(left)
    column_band = gather_columns(right)
    return jnp.einsum("rkj,jkc->rkc", row_band, column_band, preferred_element_type=jnp.float32)


def inverse_roots(tile, row_start, col_start, gather_columns, total):
    rows, count, width = tile.shape
    block = width * lax.axis_size("out")
    mask = diagonal_mask(rows, width, row_start, col_start)
    vector = jnp.ones((count, block), jnp.float32)
    image = vector
    for step in range(POWER):
        columns = lax.dynamic_slice_in_dim(vector, col_start, width, 1)
        part = jnp.einsum("rkc,kc->kr", tile, columns, precision=HIGH)
        placed = lax.dynamic_update_slice_in_dim(
            jnp.zeros((count, block), jnp.float32), part, row_start, 1
        )
        image = total(placed)
        if step + 1 < POWER:
            vector = image / jnp.sqrt(jnp.sum(image * image, axis=1, keepdims=True))
    scale = jnp.sum(vector * image, axis=1) / jnp.sum(vector * vector, axis=1)
    start = tile / scale[None, :, None]
    start_low = start.astype(jnp.bfloat16)
    first_low = ((3.0 * mask - start) / 2.0).astype(jnp.bfloat16)
    square_low = multiply(first_low, first_low, gather_columns).astype(jnp.bfloat16)
    moved = multiply(square_low, start_low, gather_columns)
    second_low = ((3.0 * mask - moved) / 2.0).astype(jnp.bfloat16)
    roots = multiply(first_low, second_low, gather_columns) / jnp.sqrt(scale)[None, :, None]
    return roots.astype(jnp.bfloat16)


def local(activations, out_grads, weight):
    tok_dev, blocks, width = activations.shape
    block = width * lax.axis_size("out")
    token_count = tok_dev * lax.axis_size("tok") * lax.axis_size("grp")
    col_start = lax.axis_index("out") * width
    local_sides = jnp.concatenate([activations, out_grads], axis=1)
    whole_sides = spread(local_sides)
    grads_whole = whole_sides[:, blocks:, :]
    weight_rows = weight.reshape(blocks, width, blocks, block)
    input_grad = jnp.einsum(
        "tjq,bcjq->tbc", grads_whole, weight_rows, preferred_element_type=jnp.float32
    ).astype(jnp.bfloat16)
    rows = block // (lax.axis_size("tok") * lax.axis_size("grp"))
    row_start = lax.axis_index(("tok", "grp")) * rows

    def shared_terms(start, span):
        return jnp.einsum(
            "tkr,tkc->rkc", whole_sides, local_sides, preferred_element_type=jnp.float32
        )

    sums = token_sums(shared_terms, rows)
    tile = sums / token_count + DAMPING * diagonal_mask(rows, width, row_start, col_start)
    roots = inverse_roots(tile, row_start, col_start, shared_rows, shared_total)
    bands = shared_rows(roots)
    whitened = jnp.einsum(
        "tkj,jkc->tkc", whole_sides, bands, preferred_element_type=jnp.float32
    ).astype(jnp.bfloat16)
    acts_whole = spread(whitened[:, :blocks, :]).reshape(tok_dev, blocks * block)
    grads_low = whitened[:, blocks:, :]
    owned_acts = lax.all_to_all(acts_whole, ("tok", "grp"), split_axis=1, concat_axis=0, tiled=True)
    update = jnp.einsum(
        "ta,tbc->abc",
        owned_acts,
        lax.all_gather(grads_low, ("tok", "grp"), axis=0, tiled=True),
        preferred_element_type=jnp.float32,
    )
    update = (update / math.sqrt(token_count)).astype(jnp.bfloat16)
    return (update, input_grad)


MESH = pl.DeviceIdType.MESH
CHUNKS = 8
TURNED = 2
PARTS = 4
PLAN = (
    ("y", 0, 0), ("x", 0, 0), ("y", 0, 1), ("x", 0, 1), ("z", 1, 0), ("y", 0, 2), ("x", 0, 2),
    ("z", 2, 0), ("y", 0, 3), ("x", 0, 3), ("z", 3, 0), ("z", 1, 1), ("z", 2, 1), ("y", 1, 0),
    ("y", 2, 0), ("x", 1, 0), ("z", 1, 2), ("z", 3, 1), ("x", 2, 0), ("z", 2, 2), ("x", 1, 1),
    ("y", 1, 1), ("x", 3, 0), ("z", 1, 3), ("y", 3, 0), ("c", 0, 0), ("z", 3, 2), ("x", 2, 1),
    ("x", 1, 2), ("y", 1, 2), ("y", 2, 1), ("z", 2, 3), ("y", 3, 1), ("c", 0, 1), ("z", 3, 3),
    ("x", 3, 1), ("y", 2, 2), ("x", 2, 2), ("x", 1, 3), ("d", 0, 0), ("x", 3, 2), ("y", 1, 3),
    ("y", 3, 2), ("c", 0, 2), ("x", 2, 3), ("d", 0, 1), ("y", 2, 3), ("x", 3, 3), ("y", 3, 3),
    ("c", 0, 3), ("d", 0, 2), ("d", 0, 3),
)
LAG = 3


def greet(peers):
    barrier = pltpu.get_barrier_semaphore()
    for peer in peers:
        pl.semaphore_signal(barrier, inc=1, device_id=peer, device_id_type=MESH)
    pl.semaphore_wait(barrier, len(peers))


def remote(src, dst, send, recv, peer):
    return pltpu.make_async_remote_copy(
        src_ref=src, dst_ref=dst, send_sem=send, recv_sem=recv, device_id=peer, device_id_type=MESH
    )


def held(z):
    return z + 2 - 3 * ((z + 2) // 3) + z // 3


def neighbours():
    z, o, y = lax.axis_index("tok"), lax.axis_index("out"), lax.axis_index("grp")
    ox = lax.rem(o + 2, 4)
    oc = o + 1 - 2 * lax.rem(o, 2)
    at = lambda a, b, c: {"tok": a, "out": b, "grp": c}
    zs = [lax.rem(z + j, 4) for j in range(4)]
    peers = [at(zs[j], o, y) for j in (1, 2, 3)]
    return z, o, y, ox, oc, zs, peers, at(z, o, 1 - y), at(z, ox, y), at(z, oc, y)


def hops(z):
    return (z, z + 1 - 2 * lax.rem(z, 2), 2 - z // 2, 3 - 3 * (z // 2))


def fused_kernel(
    pieces, weight, grads, acts, product,
    sides, low, head, left, right, tail, rays, raw, held_weight,
    z_send, send, recv, c_send, c_recv, local, w_sem, r_send, r_recv,
    g_send, y_send, t_send, g_recv, y_recv, a_send, a_recv, h_send, h_recv, k_send, k_recv, put,
):
    z, o, y, ox, oc, zs, z_peers, y_peer, x_peer, c_peer = neighbours()
    oxc = lax.rem(oc + 2, 4)
    width = pieces.shape[2]
    rows = pieces.shape[1] // PARTS
    group = rows * 8
    tokens, block = sides.shape
    part = left.shape[1]
    near = hops(z)
    across = (((1,), (1,)), ((), ()))
    sent = []

    def columns(oi):
        return pl.ds(pl.multiple_of(oi * width, width), width)

    def tile(oi, yi, zi, s):
        start = pl.multiple_of(((s * 2 + yi) * 4 + zi) * rows, rows)
        return sides.at[pl.ds(start, rows), columns(oi)]

    def piece(zi, s):
        return pieces.at[held(zi), pl.ds(s * rows, rows), :]

    def sem_of(oi, yi, zi, s):
        return recv.at[((oi // 2) * 8 + yi * 4 + zi) * PARTS + s]

    def push(src, where, peer):
        copy = remote(src, tile(*where), send.at[len(sent)], sem_of(*where), peer)
        copy.start()
        sent.append(copy)

    def arrived(*where):
        ref = tile(*where)
        remote(ref, ref, send.at[0], sem_of(*where), c_peer).wait_recv()
        return ref

    def band(oi, s):
        return sides.at[pl.ds(s * group, group), columns(oi)]

    def over_core(oi, s, place):
        n = s * 2 + place
        return remote(band(oi, s), band(oi, s), c_send.at[n], c_recv.at[n], c_peer)

    d_peer = {"tok": z, "out": ox, "grp": 1 - y}
    greet(z_peers + [y_peer, x_peer, c_peer, d_peer])
    strip = width // 2
    strips = [(b, i) for b in range(2) for i in range(2)]

    def load(n):
        b, i = strips[n]
        place = (b, pl.ds(i * strip, strip), slice(None))
        return pltpu.make_async_copy(weight.at[place], held_weight.at[place], w_sem.at[n])

    def raw_band(oi):
        return raw.at[:, :, columns(oi)]

    own_raw = pieces.at[2:4]
    raw_local = pltpu.make_async_copy(own_raw, raw_band(o), r_send.at[3])
    raw_x = remote(own_raw, raw_band(o), r_send.at[0], r_recv.at[0], x_peer)
    raw_c = remote(own_raw, raw_band(o), r_send.at[1], r_recv.at[1], c_peer)
    raw_xc = remote(raw_band(ox), raw_band(ox), r_send.at[2], r_recv.at[2], c_peer)
    z_sent = []
    for s in range(PARTS):
        for j in (3, 2, 1):
            copy = remote(
                piece(near[j], s), tile(o, y, z, s), z_send.at[len(z_sent)], sem_of(o, y, z, s),
                {"tok": near[j], "out": o, "grp": y},
            )
            copy.start()
            z_sent.append(copy)
        push(piece(z, s), (o, y, z, s), y_peer)
        push(piece(z, s), (o, y, z, s), x_peer)
    owns = []
    for s in range(PARTS):
        owns.append(pltpu.make_async_copy(piece(z, s), tile(o, y, z, s), local.at[s]))
        owns[-1].start()

    for n in range(4):
        load(n).start()
    raw_local.start()
    raw_c.start()
    ones = jnp.ones((16, block), sides.dtype)

    def rows_of(s):
        return pl.ds(s * group, group)

    def gram_group(s, known):
        here = rows_of(s)
        sums = lax.dot_general(ones, sides[here, :], across, preferred_element_type=jnp.float32)
        rays[0:8, here] = sums[0:8]
        for i in known + [s]:
            there = rows_of(i)
            product = lax.dot_general(
                sides[there, :], sides[here, :], across, preferred_element_type=jnp.float32
            )
            product = product * (1.0 / tokens)
            low[there, here] = product.astype(low.dtype)
            if i != s:
                low[here, there] = jnp.transpose(product).astype(low.dtype)

    def straight(j, s):
        return j == 3 and s == PARTS - 1

    def finish(s):
        over_core(oc, s, 0).wait_recv()
        over_core(oxc, s, 1).wait_recv()
        gram_group(s, known)
        known.append(s)

    known = []
    waiting = []
    for kind, j, s in PLAN:
        if kind == "z":
            where = (o, y, near[j], s)
            ref = arrived(*where)
            push(ref, where, y_peer)
            push(ref, where, x_peer)
            if straight(j, s):
                push(ref, where, d_peer)
        elif kind == "y":
            where = (o, 1 - y, near[j], s)
            ref = arrived(*where)
            if (j + s) % 2 == 0 and not straight(j, s):
                push(ref, where, x_peer)
        elif kind == "x":
            where = (ox, y, near[j], s)
            ref = arrived(*where)
            if (j + s) % 2 == 1 and not straight(j, s):
                push(ref, where, y_peer)
        elif kind == "c":
            owns[s].wait()
            over_core(o, s, 0).start()
        else:
            for i in range(4):
                arrived(ox, 1 - y, near[i], s)
            over_core(ox, s, 1).start()
            if waiting:
                finish(waiting.pop())
            waiting.append(s)
    raw_x.start()
    finish(waiting.pop())

    def pair(a, b):
        return jnp.sum(a * b, axis=1, keepdims=True)

    def advance(ray):
        high = ray.astype(low.dtype)
        rest = ray - high.astype(jnp.float32)
        middle = rest.astype(low.dtype)
        least = (rest - middle.astype(jnp.float32)).astype(low.dtype)
        zero = jnp.zeros((13, tokens), low.dtype)
        stack = jnp.concatenate([high, middle, least, zero], axis=0)
        image = jnp.dot(stack, low[...], preferred_element_type=jnp.float32)
        return image[0:1] + image[1:2] + image[2:3] + DAMPING * ray

    ray_0 = rays[0:1, :]
    ray_1 = advance(ray_0)
    ray_2 = advance(ray_1)
    dots = [
        pair(ray_0, ray_0),
        pair(ray_0, ray_1),
        pair(ray_1, ray_1),
        pair(ray_1, ray_2),
        pair(ray_2, ray_2),
    ]

    def moment(power):
        total = jnp.full((1, 1), DAMPING**power * block, jnp.float32)
        for i in range(power):
            total = total + DAMPING ** (power - 1 - i) * dots[i] / tokens
        return total

    scale = moment(2 * POWER - 1) / moment(2 * POWER - 2)
    inverse = 1.0 / scale
    root = 1.0 / jnp.sqrt(scale)
    act_start = 2 * (lax.rem(o, 2) * 2 + y) + o // 2
    is_grad = (z // 3) + (3 - z) // 3
    start = (is_grad * (2 * o + y) + (1 - is_grad) * act_start) * part
    cols = pl.ds(pl.multiple_of(start, part), part)
    tall = min(512, tokens)
    steps = tokens // tall

    def span(i):
        return pl.ds(pl.multiple_of(i * tall, tall), tall)

    def apply(i, source, value):
        image = jnp.dot(low[span(i), :], source[...], preferred_element_type=jnp.float32)
        return (image + DAMPING * value) * inverse

    left[...] = sides[:, cols]

    @pl.loop(0, steps, unroll=True)
    def _(i):
        value = left[span(i), :].astype(jnp.float32)
        value = 1.5 * value - 0.5 * apply(i, left, value)
        head[span(i), :] = value
        right[span(i), :] = value.astype(right.dtype)

    @pl.loop(0, steps, unroll=True)
    def _(i):
        value = apply(i, right, head[span(i), :])
        tail[span(i), :] = value
        left[span(i), :] = value.astype(left.dtype)

    @pl.loop(0, steps, unroll=True)
    def _(i):
        value = tail[span(i), :]
        value = 1.5 * value - 0.5 * apply(i, left, value)
        tail[span(i), :] = value
        right[span(i), :] = value.astype(right.dtype)

    raw_x.wait_recv()
    raw_xc.start()

    @pl.loop(0, steps, unroll=True)
    def _(i):
        value = tail[span(i), :]
        value = 1.5 * value - 0.5 * apply(i, right, value)
        left[span(i), :] = ((1.5 * head[span(i), :] - 0.5 * value) * root).astype(left.dtype)

    span_rows = tokens // CHUNKS
    is_end = is_grad == 1
    is_middle = is_grad == 0
    mine = z // 3
    h = o // 2
    goal_z = (z // 2) * 2 + lax.rem(o, 2)
    stays = goal_z == z
    goal = {"tok": goal_z, "out": o, "grp": y}
    first, second = z // 2, 1 - z // 2
    is_hub = lax.rem(o, 2) == lax.rem(z, 2)
    here = is_middle & stays
    plain = [c for c in range(CHUNKS - TURNED)]
    turned = [c for c in range(CHUNKS - TURNED, CHUNKS)]

    def rung(c):
        return pl.ds(c * span_rows, span_rows)

    def piece_of(c):
        return left.at[rung(c), :]

    def half(i):
        return pl.ds(pl.multiple_of(i * part, part), part)

    def g_tile(b, yi, c):
        return grads.at[b, rung(c), half(yi)]

    def a_tile(i, c):
        return acts.at[rung(c), half(i)]

    def own_grad(c):
        return pltpu.make_async_copy(piece_of(c), g_tile(mine, y, c), put.at[c])

    def own_act(c):
        return pltpu.make_async_copy(piece_of(c), a_tile(h, c), put.at[c])

    def onward(b):
        return {"tok": lax.rem(z + 5 - 2 * b, 4), "out": o, "grp": y}

    def to_plane(src, b, c):
        n = b * CHUNKS + c
        return remote(src, g_tile(b, y, c), g_send.at[n], g_recv.at[n], onward(b))

    def other_to_plane(b, c):
        n = b * CHUNKS + c
        ref = g_tile(b, 1 - y, c)
        return remote(ref, ref, t_send.at[n], y_recv.at[n], onward(b))

    def y_copy(src, b, c):
        n = b * CHUNKS + c
        return remote(src, g_tile(b, y, c), y_send.at[n], y_recv.at[n], y_peer)

    def to_hub(c):
        return remote(piece_of(c), a_tile(h, c), a_send.at[c], a_recv.at[c], goal)

    def over_x(c, i):
        return remote(a_tile(i, c), a_tile(i, c), h_send.at[c], h_recv.at[c], x_peer)

    def act_core(c, i):
        n = i * CHUNKS + c
        return remote(a_tile(i, c), a_tile(i, c), k_send.at[n], k_recv.at[n], c_peer)

    for b in range(2):

        @pl.when(z == 3 * b)
        def _():
            for c in turned + plain:
                y_copy(piece_of(c), b, c).start()
            for c in plain + turned:
                to_plane(piece_of(c), b, c).start()

    for c in range(CHUNKS):

        @pl.when(is_end)
        def _():
            own_grad(c).start()

        @pl.when(here)
        def _():
            own_act(c).start()

        @pl.when(is_middle & jnp.logical_not(stays))
        def _():
            to_hub(c).start()

    def multiply(n):
        b, i = strips[n]
        load(n).wait()
        total = jnp.zeros((raw.shape[1], strip), jnp.float32)
        for k in range(2):
            total += lax.dot_general(
                raw[k],
                held_weight[b, pl.ds(i * strip, strip), pl.ds(k * block, block)],
                (((1,), (1,)), ((), ())),
                preferred_element_type=jnp.float32,
            )
        product[b, :, pl.ds(i * strip, strip)] = total.astype(product.dtype)

    def hub_step(c):
        @pl.when(here)
        def _():
            own_act(c).wait()

        @pl.when(is_hub & jnp.logical_not(here))
        def _():
            ref = a_tile(h, c)
            remote(ref, ref, a_send.at[0], a_recv.at[c], c_peer).wait_recv()

        @pl.when(is_hub)
        def _():
            over_x(c, h).start()
            act_core(c, h).start()

    def cross_step(c):
        @pl.when(is_hub)
        def _():
            over_x(c, 1 - h).wait_recv()
            act_core(c, 1 - h).start()

    def g_wait(b, c):
        ref = g_tile(b, y, c)
        remote(ref, ref, g_send.at[0], g_recv.at[b * CHUNKS + c], c_peer).wait_recv()
        return ref

    def y_wait(b, c):
        ref = g_tile(b, 1 - y, c)
        remote(ref, ref, y_send.at[0], y_recv.at[b * CHUNKS + c], c_peer).wait_recv()

    def take(b, kind, c):
        if kind == "own":
            ref = g_wait(b, c)

            @pl.when(is_middle)
            def _():
                to_plane(ref, b, c).start()

            if c not in turned:
                y_copy(ref, b, c).start()
        else:
            y_wait(b, c)

            @pl.when(is_middle)
            def _():
                other_to_plane(b, c).start()

    raw_local.wait()
    raw_c.wait_recv()
    raw_xc.wait_recv()
    for n in range(4):
        multiply(n)

    @pl.when(is_end)
    def _():
        for c in turned:
            y_wait(mine, c)
            other_to_plane(mine, c).start()

    flow = [("own", c) for c in plain + turned] + [("other", c) for c in turned]
    for step in range(len(flow) + LAG):
        if step < len(flow):

            @pl.when(is_middle)
            def _():
                take(first, *flow[step])

        if step < CHUNKS:
            hub_step(step)
        if step >= LAG:
            take(second, *flow[step - LAG])
    for c in range(CHUNKS):
        cross_step(c)
    for c in range(CHUNKS):
        for b in range(2):
            if c in turned:

                @pl.when(z == 3 * b)
                def _():
                    y_copy(piece_of(c), b, c).wait_send()

                @pl.when(z != 3 - 3 * b)
                def _():
                    other_to_plane(b, c).wait_send()

            else:
                y_wait(b, c)
                y_copy(g_tile(b, y, c), b, c).wait_send()

            @pl.when(z != 3 - 3 * b)
            def _():
                to_plane(g_tile(b, y, c), b, c).wait_send()

        @pl.when(is_end)
        def _():
            own_grad(c).wait()

        @pl.when(is_middle & jnp.logical_not(stays))
        def _():
            to_hub(c).wait_send()

        for i in range(2):

            @pl.when(is_hub)
            def _():
                act_core(c, i).wait_send()

            @pl.when(jnp.logical_not(is_hub))
            def _():
                act_core(c, i).wait_recv()

        @pl.when(is_hub)
        def _():
            over_x(c, h).wait_send()

    raw_x.wait_send()
    raw_c.wait_send()
    raw_xc.wait_send()
    for copy in z_sent:
        copy.wait_send()
    for copy in sent:
        copy.wait_send()
    for s in range(PARTS):
        over_core(o, s, 0).wait_send()
        over_core(ox, s, 1).wait_send()


def fused(pieces, weight, part):
    _, rows, width = pieces.shape
    tokens, block = rows * 8, width * 4
    dma = pltpu.SemaphoreType.DMA
    vmem = pl.BlockSpec(memory_space=pltpu.VMEM)
    low = pieces.dtype
    return pl.pallas_call(
        fused_kernel,
        out_shape=(
            jax.ShapeDtypeStruct((2, tokens, 2 * part), low),
            jax.ShapeDtypeStruct((tokens, 2 * part), low),
            jax.ShapeDtypeStruct((2, rows, width), low),
        ),
        in_specs=[vmem, pl.BlockSpec(memory_space=pl.ANY)],
        out_specs=(vmem, vmem, vmem),
        scratch_shapes=[
            pltpu.VMEM((tokens, block), low),
            pltpu.VMEM((tokens, tokens), low),
            pltpu.VMEM((tokens, part), jnp.float32),
            pltpu.VMEM((tokens, part), low),
            pltpu.VMEM((tokens, part), low),
            pltpu.VMEM((tokens, part), jnp.float32),
            pltpu.VMEM((8, tokens), jnp.float32),
            pltpu.VMEM((2, rows, block), low),
            pltpu.VMEM(weight.shape, weight.dtype),
            dma((3 * PARTS,)),
            dma((16 * PARTS,)),
            dma((16 * PARTS,)),
            dma((2 * PARTS,)),
            dma((2 * PARTS,)),
            dma((PARTS,)),
            dma((4,)),
            dma((4,)),
            dma((3,)),
            dma((2 * CHUNKS,)),
            dma((2 * CHUNKS,)),
            dma((2 * CHUNKS,)),
            dma((2 * CHUNKS,)),
            dma((2 * CHUNKS,)),
            dma((CHUNKS,)),
            dma((CHUNKS,)),
            dma((CHUNKS,)),
            dma((CHUNKS,)),
            dma((2 * CHUNKS,)),
            dma((2 * CHUNKS,)),
            dma((CHUNKS,)),
        ],
        compiler_params=pltpu.CompilerParams(collective_id=0, has_side_effects=True),
        name="fused",
    )(pieces, weight)


def planes(activations, out_grads, weight):
    tok_dev, _, width = activations.shape
    part = width // lax.axis_size("grp")
    token_count = tok_dev * lax.axis_size(("tok", "grp"))
    pieces = jnp.swapaxes(jnp.concatenate([activations, out_grads], axis=1), 0, 1)
    grads_low, acts_low, product = fused(pieces, weight, part)
    update = jnp.einsum("ta,btc->abc", acts_low, grads_low, preferred_element_type=jnp.float32)
    update = (update / math.sqrt(token_count)).astype(jnp.bfloat16)
    input_grad = jnp.swapaxes(product, 0, 1)
    return (update, input_grad)


def solution(mesh):
    in_specs = (
        P(("tok", "grp"), None, "out"),
        P(("tok", "grp"), None, "out"),
        P(None, "out", None),
    )
    out_specs = (P(("tok", "grp"), None, "out"), P(("tok", "grp"), None, "out"))

    def body(activations, out_grads, weight):
        blocks = activations.shape[1]
        tok, grp, out = (mesh.shape[name] for name in ("tok", "grp", "out"))
        fits = (blocks, tok, grp, out) == (2, 4, 2, 4)
        return (planes if fits else local)(activations, out_grads, weight)

    return jax.shard_map(body, mesh=mesh, in_specs=in_specs, out_specs=out_specs, check_vma=False)
```

```python
import math

import jax
import jax.numpy as jnp
from jax import lax
from jax.experimental import pallas as pl
from jax.experimental.pallas import tpu as pltpu
from jax.sharding import PartitionSpec as P

POWER = 3


DAMPING = 0.1
HIGH = lax.Precision.HIGHEST


def spread(piece):
    return lax.all_gather(piece, "out", axis=2, tiled=True)


def token_sums(maker, rows):
    return lax.psum_scatter(
        maker(jnp.int32(0), rows * lax.axis_size(("tok", "grp"))),
        ("tok", "grp"),
        scatter_dimension=0,
        tiled=True,
    )


def shared_rows(piece):
    return lax.all_gather(piece, ("tok", "grp"), axis=0, tiled=True)


def shared_total(vector):
    return lax.psum(vector, ("tok", "out", "grp"))


def diagonal_mask(rows, width, row_start, col_start):
    row_ids = row_start + lax.broadcasted_iota(jnp.int32, (rows, 1, width), 0)
    col_ids = col_start + lax.broadcasted_iota(jnp.int32, (rows, 1, width), 2)
    return jnp.where(row_ids == col_ids, 1.0, 0.0).astype(jnp.float32)


def multiply(left, right, gather_columns):
    row_band = spread(left)
    column_band = gather_columns(right)
    return jnp.einsum("rkj,jkc->rkc", row_band, column_band, preferred_element_type=jnp.float32)


def inverse_roots(tile, row_start, col_start, gather_columns, total):
    rows, count, width = tile.shape
    block = width * lax.axis_size("out")
    mask = diagonal_mask(rows, width, row_start, col_start)
    vector = jnp.ones((count, block), jnp.float32)
    image = vector
    for step in range(POWER):
        columns = lax.dynamic_slice_in_dim(vector, col_start, width, 1)
        part = jnp.einsum("rkc,kc->kr", tile, columns, precision=HIGH)
        placed = lax.dynamic_update_slice_in_dim(
            jnp.zeros((count, block), jnp.float32), part, row_start, 1
        )
        image = total(placed)
        if step + 1 < POWER:
            vector = image / jnp.sqrt(jnp.sum(image * image, axis=1, keepdims=True))
    scale = jnp.sum(vector * image, axis=1) / jnp.sum(vector * vector, axis=1)
    start = tile / scale[None, :, None]
    start_low = start.astype(jnp.bfloat16)
    first_low = ((3.0 * mask - start) / 2.0).astype(jnp.bfloat16)
    square_low = multiply(first_low, first_low, gather_columns).astype(jnp.bfloat16)
    moved = multiply(square_low, start_low, gather_columns)
    second_low = ((3.0 * mask - moved) / 2.0).astype(jnp.bfloat16)
    roots = multiply(first_low, second_low, gather_columns) / jnp.sqrt(scale)[None, :, None]
    return roots.astype(jnp.bfloat16)


def local(activations, out_grads, weight):
    tok_dev, blocks, width = activations.shape
    block = width * lax.axis_size("out")
    token_count = tok_dev * lax.axis_size("tok") * lax.axis_size("grp")
    col_start = lax.axis_index("out") * width
    local_sides = jnp.concatenate([activations, out_grads], axis=1)
    whole_sides = spread(local_sides)
    grads_whole = whole_sides[:, blocks:, :]
    weight_rows = weight.reshape(blocks, width, blocks, block)
    input_grad = jnp.einsum(
        "tjq,bcjq->tbc", grads_whole, weight_rows, preferred_element_type=jnp.float32
    ).astype(jnp.bfloat16)
    rows = block // (lax.axis_size("tok") * lax.axis_size("grp"))
    row_start = lax.axis_index(("tok", "grp")) * rows

    def shared_terms(start, span):
        return jnp.einsum(
            "tkr,tkc->rkc", whole_sides, local_sides, preferred_element_type=jnp.float32
        )

    sums = token_sums(shared_terms, rows)
    tile = sums / token_count + DAMPING * diagonal_mask(rows, width, row_start, col_start)
    roots = inverse_roots(tile, row_start, col_start, shared_rows, shared_total)
    bands = shared_rows(roots)
    whitened = jnp.einsum(
        "tkj,jkc->tkc", whole_sides, bands, preferred_element_type=jnp.float32
    ).astype(jnp.bfloat16)
    acts_whole = spread(whitened[:, :blocks, :]).reshape(tok_dev, blocks * block)
    grads_low = whitened[:, blocks:, :]
    owned_acts = lax.all_to_all(acts_whole, ("tok", "grp"), split_axis=1, concat_axis=0, tiled=True)
    update = jnp.einsum(
        "ta,tbc->abc",
        owned_acts,
        lax.all_gather(grads_low, ("tok", "grp"), axis=0, tiled=True),
        preferred_element_type=jnp.float32,
    )
    update = (update / math.sqrt(token_count)).astype(jnp.bfloat16)
    return (update, input_grad)


MESH = pl.DeviceIdType.MESH
CHUNKS = 8
TURNED = 2
ROOM = 50 * 2**20
PARTS = 4
PLAN = (
    ("y", 0, 0), ("x", 0, 0), ("y", 0, 1), ("x", 0, 1), ("z", 1, 0), ("y", 0, 2), ("x", 0, 2),
    ("z", 2, 0), ("y", 0, 3), ("x", 0, 3), ("z", 3, 0), ("z", 1, 1), ("z", 2, 1), ("y", 1, 0),
    ("y", 2, 0), ("x", 1, 0), ("z", 1, 2), ("z", 3, 1), ("x", 2, 0), ("z", 2, 2), ("x", 1, 1),
    ("y", 1, 1), ("x", 3, 0), ("z", 1, 3), ("y", 3, 0), ("c", 0, 0), ("z", 3, 2), ("x", 2, 1),
    ("x", 1, 2), ("y", 1, 2), ("y", 2, 1), ("z", 2, 3), ("y", 3, 1), ("c", 0, 1), ("z", 3, 3),
    ("x", 3, 1), ("y", 2, 2), ("x", 2, 2), ("x", 1, 3), ("d", 0, 0), ("x", 3, 2), ("y", 1, 3),
    ("y", 3, 2), ("c", 0, 2), ("x", 2, 3), ("d", 0, 1), ("y", 2, 3), ("x", 3, 3), ("y", 3, 3),
    ("c", 0, 3), ("d", 0, 2), ("d", 0, 3),
)
LAG = 3


def greet(peers):
    barrier = pltpu.get_barrier_semaphore()
    for peer in peers:
        pl.semaphore_signal(barrier, inc=1, device_id=peer, device_id_type=MESH)
    pl.semaphore_wait(barrier, len(peers))


def remote(src, dst, send, recv, peer):
    return pltpu.make_async_remote_copy(
        src_ref=src, dst_ref=dst, send_sem=send, recv_sem=recv, device_id=peer, device_id_type=MESH
    )


def held(z):
    return z + 2 - 3 * ((z + 2) // 3) + z // 3


def neighbours():
    z, o, y = lax.axis_index("tok"), lax.axis_index("out"), lax.axis_index("grp")
    ox = lax.rem(o + 2, 4)
    oc = o + 1 - 2 * lax.rem(o, 2)
    at = lambda a, b, c: {"tok": a, "out": b, "grp": c}
    zs = [lax.rem(z + j, 4) for j in range(4)]
    peers = [at(zs[j], o, y) for j in (1, 2, 3)]
    return z, o, y, ox, oc, zs, peers, at(z, o, 1 - y), at(z, ox, y), at(z, oc, y)


def hops(z):
    return (z, z + 1 - 2 * lax.rem(z, 2), 2 - z // 2, 3 - 3 * (z // 2))


def fused_kernel(
    pieces, weight, grads, acts, product,
    sides, low, head, left, right, tail, rays, raw, held_weight,
    z_send, send, recv, c_send, c_recv, local, w_sem, r_send, r_recv,
    g_send, y_send, t_send, g_recv, y_recv, a_send, a_recv, h_send, h_recv, k_send, k_recv, put,
):
    z, o, y, ox, oc, zs, z_peers, y_peer, x_peer, c_peer = neighbours()
    oxc = lax.rem(oc + 2, 4)
    width = pieces.shape[2]
    rows = pieces.shape[1] // PARTS
    group = rows * 8
    tokens, block = sides.shape
    part = left.shape[1]
    near = hops(z)
    across = (((1,), (1,)), ((), ()))
    sent = []

    def columns(oi):
        return pl.ds(pl.multiple_of(oi * width, width), width)

    def tile(oi, yi, zi, s):
        start = pl.multiple_of(((s * 2 + yi) * 4 + zi) * rows, rows)
        return sides.at[pl.ds(start, rows), columns(oi)]

    def piece(zi, s):
        return pieces.at[held(zi), pl.ds(s * rows, rows), :]

    def sem_of(oi, yi, zi, s):
        return recv.at[((oi // 2) * 8 + yi * 4 + zi) * PARTS + s]

    def push(src, where, peer):
        copy = remote(src, tile(*where), send.at[len(sent)], sem_of(*where), peer)
        copy.start()
        sent.append(copy)

    def arrived(*where):
        ref = tile(*where)
        remote(ref, ref, send.at[0], sem_of(*where), c_peer).wait_recv()
        return ref

    def band(oi, s):
        return sides.at[pl.ds(s * group, group), columns(oi)]

    def over_core(oi, s, place):
        n = s * 2 + place
        return remote(band(oi, s), band(oi, s), c_send.at[n], c_recv.at[n], c_peer)

    d_peer = {"tok": z, "out": ox, "grp": 1 - y}
    greet(z_peers + [y_peer, x_peer, c_peer, d_peer])
    strip = width // 2
    strips = [(b, i) for b in range(2) for i in range(2)]

    def load(n):
        b, i = strips[n]
        place = (b, pl.ds(i * strip, strip), slice(None))
        return pltpu.make_async_copy(weight.at[place], held_weight.at[place], w_sem.at[n])

    def raw_band(oi):
        return raw.at[:, :, columns(oi)]

    own_raw = pieces.at[2:4]
    raw_local = pltpu.make_async_copy(own_raw, raw_band(o), r_send.at[3])
    raw_x = remote(own_raw, raw_band(o), r_send.at[0], r_recv.at[0], x_peer)
    raw_c = remote(own_raw, raw_band(o), r_send.at[1], r_recv.at[1], c_peer)
    raw_xc = remote(raw_band(ox), raw_band(ox), r_send.at[2], r_recv.at[2], c_peer)
    z_sent = []
    for s in range(PARTS):
        for j in (3, 2, 1):
            copy = remote(
                piece(near[j], s), tile(o, y, z, s), z_send.at[len(z_sent)], sem_of(o, y, z, s),
                {"tok": near[j], "out": o, "grp": y},
            )
            copy.start()
            z_sent.append(copy)
        push(piece(z, s), (o, y, z, s), y_peer)
        push(piece(z, s), (o, y, z, s), x_peer)
    owns = []
    for s in range(PARTS):
        owns.append(pltpu.make_async_copy(piece(z, s), tile(o, y, z, s), local.at[s]))
        owns[-1].start()

    for n in range(4):
        load(n).start()
    raw_local.start()
    raw_c.start()
    ones = jnp.ones((16, block), sides.dtype)

    def rows_of(s):
        return pl.ds(s * group, group)

    def gram_group(s, known):
        here = rows_of(s)
        sums = lax.dot_general(ones, sides[here, :], across, preferred_element_type=jnp.float32)
        rays[0:8, here] = sums[0:8]
        for i in known + [s]:
            there = rows_of(i)
            product = lax.dot_general(
                sides[there, :], sides[here, :], across, preferred_element_type=jnp.float32
            )
            product = product * (1.0 / tokens)
            low[there, here] = product.astype(low.dtype)
            if i != s:
                low[here, there] = jnp.transpose(product).astype(low.dtype)

    def straight(j, s):
        return j == 3 and s == PARTS - 1

    def finish(s):
        over_core(oc, s, 0).wait_recv()
        over_core(oxc, s, 1).wait_recv()
        gram_group(s, known)
        known.append(s)

    known = []
    waiting = []
    for kind, j, s in PLAN:
        if kind == "z":
            where = (o, y, near[j], s)
            ref = arrived(*where)
            push(ref, where, y_peer)
            push(ref, where, x_peer)
            if straight(j, s):
                push(ref, where, d_peer)
        elif kind == "y":
            where = (o, 1 - y, near[j], s)
            ref = arrived(*where)
            if (j + s) % 2 == 0 and not straight(j, s):
                push(ref, where, x_peer)
        elif kind == "x":
            where = (ox, y, near[j], s)
            ref = arrived(*where)
            if (j + s) % 2 == 1 and not straight(j, s):
                push(ref, where, y_peer)
        elif kind == "c":
            owns[s].wait()
            over_core(o, s, 0).start()
        else:
            for i in range(4):
                arrived(ox, 1 - y, near[i], s)
            over_core(ox, s, 1).start()
            if waiting:
                finish(waiting.pop())
            waiting.append(s)
    raw_x.start()
    finish(waiting.pop())

    def pair(a, b):
        return jnp.sum(a * b, axis=1, keepdims=True)

    def advance(ray):
        high = ray.astype(low.dtype)
        rest = ray - high.astype(jnp.float32)
        middle = rest.astype(low.dtype)
        least = (rest - middle.astype(jnp.float32)).astype(low.dtype)
        zero = jnp.zeros((13, tokens), low.dtype)
        stack = jnp.concatenate([high, middle, least, zero], axis=0)
        image = jnp.dot(stack, low[...], preferred_element_type=jnp.float32)
        return image[0:1] + image[1:2] + image[2:3] + DAMPING * ray

    ray_0 = rays[0:1, :]
    ray_1 = advance(ray_0)
    ray_2 = advance(ray_1)
    dots = [
        pair(ray_0, ray_0),
        pair(ray_0, ray_1),
        pair(ray_1, ray_1),
        pair(ray_1, ray_2),
        pair(ray_2, ray_2),
    ]

    def moment(power):
        total = jnp.full((1, 1), DAMPING**power * block, jnp.float32)
        for i in range(power):
            total = total + DAMPING ** (power - 1 - i) * dots[i] / tokens
        return total

    scale = moment(2 * POWER - 1) / moment(2 * POWER - 2)
    inverse = 1.0 / scale
    root = 1.0 / jnp.sqrt(scale)
    act_start = 2 * (lax.rem(o, 2) * 2 + y) + o // 2
    is_grad = (z // 3) + (3 - z) // 3
    start = (is_grad * (2 * o + y) + (1 - is_grad) * act_start) * part
    cols = pl.ds(pl.multiple_of(start, part), part)
    tall = min(512, tokens)
    steps = tokens // tall

    def span(i):
        return pl.ds(pl.multiple_of(i * tall, tall), tall)

    def apply(i, source, value):
        image = jnp.dot(low[span(i), :], source[...], preferred_element_type=jnp.float32)
        return (image + DAMPING * value) * inverse

    left[...] = sides[:, cols]

    @pl.loop(0, steps, unroll=True)
    def _(i):
        value = left[span(i), :].astype(jnp.float32)
        value = 1.5 * value - 0.5 * apply(i, left, value)
        head[span(i), :] = value
        right[span(i), :] = value.astype(right.dtype)

    @pl.loop(0, steps, unroll=True)
    def _(i):
        value = apply(i, right, head[span(i), :])
        tail[span(i), :] = value
        left[span(i), :] = value.astype(left.dtype)

    @pl.loop(0, steps, unroll=True)
    def _(i):
        value = tail[span(i), :]
        value = 1.5 * value - 0.5 * apply(i, left, value)
        tail[span(i), :] = value
        right[span(i), :] = value.astype(right.dtype)

    @pl.loop(0, steps, unroll=True)
    def _(i):
        value = tail[span(i), :]
        value = 1.5 * value - 0.5 * apply(i, right, value)
        left[span(i), :] = ((1.5 * head[span(i), :] - 0.5 * value) * root).astype(left.dtype)

    span_rows = tokens // CHUNKS
    is_end = is_grad == 1
    is_middle = is_grad == 0
    mine = z // 3
    h = o // 2
    goal_z = (z // 2) * 2 + lax.rem(o, 2)
    stays = goal_z == z
    goal = {"tok": goal_z, "out": o, "grp": y}
    first, second = z // 2, 1 - z // 2
    is_hub = lax.rem(o, 2) == lax.rem(z, 2)
    here = is_middle & stays
    plain = [c for c in range(CHUNKS - TURNED)]
    turned = [c for c in range(CHUNKS - TURNED, CHUNKS)]

    def rung(c):
        return pl.ds(c * span_rows, span_rows)

    def piece_of(c):
        return left.at[rung(c), :]

    def half(i):
        return pl.ds(pl.multiple_of(i * part, part), part)

    def g_tile(b, yi, c):
        return grads.at[b, rung(c), half(yi)]

    def a_tile(i, c):
        return acts.at[rung(c), half(i)]

    def own_grad(c):
        return pltpu.make_async_copy(piece_of(c), g_tile(mine, y, c), put.at[c])

    def own_act(c):
        return pltpu.make_async_copy(piece_of(c), a_tile(h, c), put.at[c])

    def onward(b):
        return {"tok": lax.rem(z + 5 - 2 * b, 4), "out": o, "grp": y}

    def to_plane(src, b, c):
        n = b * CHUNKS + c
        return remote(src, g_tile(b, y, c), g_send.at[n], g_recv.at[n], onward(b))

    def other_to_plane(b, c):
        n = b * CHUNKS + c
        ref = g_tile(b, 1 - y, c)
        return remote(ref, ref, t_send.at[n], y_recv.at[n], onward(b))

    def y_copy(src, b, c):
        n = b * CHUNKS + c
        return remote(src, g_tile(b, y, c), y_send.at[n], y_recv.at[n], y_peer)

    def to_hub(c):
        return remote(piece_of(c), a_tile(h, c), a_send.at[c], a_recv.at[c], goal)

    def over_x(c, i):
        return remote(a_tile(i, c), a_tile(i, c), h_send.at[c], h_recv.at[c], x_peer)

    def act_core(c, i):
        n = i * CHUNKS + c
        return remote(a_tile(i, c), a_tile(i, c), k_send.at[n], k_recv.at[n], c_peer)

    for b in range(2):

        @pl.when(z == 3 * b)
        def _():
            for c in turned + plain:
                y_copy(piece_of(c), b, c).start()
            for c in plain + turned:
                to_plane(piece_of(c), b, c).start()

    for c in range(CHUNKS):

        @pl.when(is_end)
        def _():
            own_grad(c).start()

        @pl.when(here)
        def _():
            own_act(c).start()

        @pl.when(is_middle & jnp.logical_not(stays))
        def _():
            to_hub(c).start()

    def multiply(n):
        b, i = strips[n]
        load(n).wait()
        total = jnp.zeros((raw.shape[1], strip), jnp.float32)
        for k in range(2):
            total += lax.dot_general(
                raw[k],
                held_weight[b, pl.ds(i * strip, strip), pl.ds(k * block, block)],
                (((1,), (1,)), ((), ())),
                preferred_element_type=jnp.float32,
            )
        product[b, :, pl.ds(i * strip, strip)] = total.astype(product.dtype)

    def hub_step(c):
        @pl.when(here)
        def _():
            own_act(c).wait()

        @pl.when(is_hub & jnp.logical_not(here))
        def _():
            ref = a_tile(h, c)
            remote(ref, ref, a_send.at[0], a_recv.at[c], c_peer).wait_recv()

        @pl.when(is_hub)
        def _():
            over_x(c, h).start()
            act_core(c, h).start()

    def cross_step(c):
        @pl.when(is_hub)
        def _():
            over_x(c, 1 - h).wait_recv()
            act_core(c, 1 - h).start()

    def g_wait(b, c):
        ref = g_tile(b, y, c)
        remote(ref, ref, g_send.at[0], g_recv.at[b * CHUNKS + c], c_peer).wait_recv()
        return ref

    def y_wait(b, c):
        ref = g_tile(b, 1 - y, c)
        remote(ref, ref, y_send.at[0], y_recv.at[b * CHUNKS + c], c_peer).wait_recv()

    def take(b, kind, c):
        if kind == "own":
            ref = g_wait(b, c)

            @pl.when(is_middle)
            def _():
                to_plane(ref, b, c).start()

            if c not in turned:
                y_copy(ref, b, c).start()
        else:
            y_wait(b, c)

            @pl.when(is_middle)
            def _():
                other_to_plane(b, c).start()

    raw_x.wait_recv()
    raw_xc.start()
    raw_local.wait()
    raw_c.wait_recv()

    def multiply_all():
        raw_xc.wait_recv()
        for n in range(4):
            multiply(n)

    @pl.when(is_end)
    def _():
        for c in turned:
            y_wait(mine, c)
            other_to_plane(mine, c).start()

    pl.when(is_end)(multiply_all)
    flow = [("own", c) for c in plain + turned] + [("other", c) for c in turned]
    for step in range(len(flow) + LAG):
        if step < len(flow):

            @pl.when(is_middle)
            def _():
                take(first, *flow[step])

        if step < CHUNKS:
            hub_step(step)
        if step >= LAG:
            take(second, *flow[step - LAG])
    for c in range(CHUNKS):
        cross_step(c)
    pl.when(is_middle)(multiply_all)
    for c in range(CHUNKS):
        for b in range(2):
            if c in turned:

                @pl.when(z == 3 * b)
                def _():
                    y_copy(piece_of(c), b, c).wait_send()

                @pl.when(z != 3 - 3 * b)
                def _():
                    other_to_plane(b, c).wait_send()

            else:
                y_wait(b, c)
                y_copy(g_tile(b, y, c), b, c).wait_send()

            @pl.when(z != 3 - 3 * b)
            def _():
                to_plane(g_tile(b, y, c), b, c).wait_send()

        @pl.when(is_end)
        def _():
            own_grad(c).wait()

        @pl.when(is_middle & jnp.logical_not(stays))
        def _():
            to_hub(c).wait_send()

        for i in range(2):

            @pl.when(is_hub)
            def _():
                act_core(c, i).wait_send()

            @pl.when(jnp.logical_not(is_hub))
            def _():
                act_core(c, i).wait_recv()

        @pl.when(is_hub)
        def _():
            over_x(c, h).wait_send()

    raw_x.wait_send()
    raw_c.wait_send()
    raw_xc.wait_send()
    for copy in z_sent:
        copy.wait_send()
    for copy in sent:
        copy.wait_send()
    for s in range(PARTS):
        over_core(o, s, 0).wait_send()
        over_core(ox, s, 1).wait_send()


def fused(pieces, weight, part):
    _, rows, width = pieces.shape
    tokens, block = rows * 8, width * 4
    dma = pltpu.SemaphoreType.DMA
    vmem = pl.BlockSpec(memory_space=pltpu.VMEM)
    low = pieces.dtype
    return pl.pallas_call(
        fused_kernel,
        out_shape=(
            jax.ShapeDtypeStruct((2, tokens, 2 * part), low),
            jax.ShapeDtypeStruct((tokens, 2 * part), low),
            jax.ShapeDtypeStruct((2, rows, width), low),
        ),
        in_specs=[vmem, pl.BlockSpec(memory_space=pltpu.HBM)],
        out_specs=(vmem, vmem, vmem),
        scratch_shapes=[
            pltpu.VMEM((tokens, block), low),
            pltpu.VMEM((tokens, tokens), low),
            pltpu.VMEM((tokens, part), jnp.float32),
            pltpu.VMEM((tokens, part), low),
            pltpu.VMEM((tokens, part), low),
            pltpu.VMEM((tokens, part), jnp.float32),
            pltpu.VMEM((8, tokens), jnp.float32),
            pltpu.VMEM((2, rows, block), low),
            pltpu.VMEM(weight.shape, weight.dtype),
            dma((3 * PARTS,)),
            dma((16 * PARTS,)),
            dma((16 * PARTS,)),
            dma((2 * PARTS,)),
            dma((2 * PARTS,)),
            dma((PARTS,)),
            dma((4,)),
            dma((4,)),
            dma((3,)),
            dma((2 * CHUNKS,)),
            dma((2 * CHUNKS,)),
            dma((2 * CHUNKS,)),
            dma((2 * CHUNKS,)),
            dma((2 * CHUNKS,)),
            dma((CHUNKS,)),
            dma((CHUNKS,)),
            dma((CHUNKS,)),
            dma((CHUNKS,)),
            dma((2 * CHUNKS,)),
            dma((2 * CHUNKS,)),
            dma((CHUNKS,)),
        ],
        compiler_params=pltpu.CompilerParams(collective_id=0, has_side_effects=True, vmem_limit_bytes=ROOM),
        name="fused",
    )(pieces, weight)


def planes(activations, out_grads, weight):
    tok_dev, _, width = activations.shape
    part = width // lax.axis_size("grp")
    token_count = tok_dev * lax.axis_size(("tok", "grp"))
    pieces = jnp.swapaxes(jnp.concatenate([activations, out_grads], axis=1), 0, 1)
    grads_low, acts_low, product = fused(pieces, weight, part)
    update = jnp.einsum("ta,btc->abc", acts_low, grads_low, preferred_element_type=jnp.float32)
    update = (update / math.sqrt(token_count)).astype(jnp.bfloat16)
    input_grad = jnp.swapaxes(product, 0, 1)
    return (update, input_grad)


def solution(mesh):
    in_specs = (
        P(("tok", "grp"), None, "out"),
        P(("tok", "grp"), None, "out"),
        P(None, "out", None),
    )
    out_specs = (P(("tok", "grp"), None, "out"), P(("tok", "grp"), None, "out"))

    def body(activations, out_grads, weight):
        blocks = activations.shape[1]
        tok, grp, out = (mesh.shape[name] for name in ("tok", "grp", "out"))
        fits = (blocks, tok, grp, out) == (2, 4, 2, 4)
        return (planes if fits else local)(activations, out_grads, weight)

    return jax.shard_map(body, mesh=mesh, in_specs=in_specs, out_specs=out_specs, check_vma=False)
```

```python
import math

import jax
import jax.numpy as jnp
from jax import lax
from jax.experimental import pallas as pl
from jax.experimental.pallas import tpu as pltpu
from jax.sharding import PartitionSpec as P

POWER = 3


DAMPING = 0.1
HIGH = lax.Precision.HIGHEST


def spread(piece):
    return lax.all_gather(piece, "out", axis=2, tiled=True)


def token_sums(maker, rows):
    return lax.psum_scatter(
        maker(jnp.int32(0), rows * lax.axis_size(("tok", "grp"))),
        ("tok", "grp"),
        scatter_dimension=0,
        tiled=True,
    )


def shared_rows(piece):
    return lax.all_gather(piece, ("tok", "grp"), axis=0, tiled=True)


def shared_total(vector):
    return lax.psum(vector, ("tok", "out", "grp"))


def diagonal_mask(rows, width, row_start, col_start):
    row_ids = row_start + lax.broadcasted_iota(jnp.int32, (rows, 1, width), 0)
    col_ids = col_start + lax.broadcasted_iota(jnp.int32, (rows, 1, width), 2)
    return jnp.where(row_ids == col_ids, 1.0, 0.0).astype(jnp.float32)


def multiply(left, right, gather_columns):
    row_band = spread(left)
    column_band = gather_columns(right)
    return jnp.einsum("rkj,jkc->rkc", row_band, column_band, preferred_element_type=jnp.float32)


def inverse_roots(tile, row_start, col_start, gather_columns, total):
    rows, count, width = tile.shape
    block = width * lax.axis_size("out")
    mask = diagonal_mask(rows, width, row_start, col_start)
    vector = jnp.ones((count, block), jnp.float32)
    image = vector
    for step in range(POWER):
        columns = lax.dynamic_slice_in_dim(vector, col_start, width, 1)
        part = jnp.einsum("rkc,kc->kr", tile, columns, precision=HIGH)
        placed = lax.dynamic_update_slice_in_dim(
            jnp.zeros((count, block), jnp.float32), part, row_start, 1
        )
        image = total(placed)
        if step + 1 < POWER:
            vector = image / jnp.sqrt(jnp.sum(image * image, axis=1, keepdims=True))
    scale = jnp.sum(vector * image, axis=1) / jnp.sum(vector * vector, axis=1)
    start = tile / scale[None, :, None]
    start_low = start.astype(jnp.bfloat16)
    first_low = ((3.0 * mask - start) / 2.0).astype(jnp.bfloat16)
    square_low = multiply(first_low, first_low, gather_columns).astype(jnp.bfloat16)
    moved = multiply(square_low, start_low, gather_columns)
    second_low = ((3.0 * mask - moved) / 2.0).astype(jnp.bfloat16)
    roots = multiply(first_low, second_low, gather_columns) / jnp.sqrt(scale)[None, :, None]
    return roots.astype(jnp.bfloat16)


def local(activations, out_grads, weight):
    tok_dev, blocks, width = activations.shape
    block = width * lax.axis_size("out")
    token_count = tok_dev * lax.axis_size("tok") * lax.axis_size("grp")
    col_start = lax.axis_index("out") * width
    local_sides = jnp.concatenate([activations, out_grads], axis=1)
    whole_sides = spread(local_sides)
    grads_whole = whole_sides[:, blocks:, :]
    weight_rows = weight.reshape(blocks, width, blocks, block)
    input_grad = jnp.einsum(
        "tjq,bcjq->tbc", grads_whole, weight_rows, preferred_element_type=jnp.float32
    ).astype(jnp.bfloat16)
    rows = block // (lax.axis_size("tok") * lax.axis_size("grp"))
    row_start = lax.axis_index(("tok", "grp")) * rows

    def shared_terms(start, span):
        return jnp.einsum(
            "tkr,tkc->rkc", whole_sides, local_sides, preferred_element_type=jnp.float32
        )

    sums = token_sums(shared_terms, rows)
    tile = sums / token_count + DAMPING * diagonal_mask(rows, width, row_start, col_start)
    roots = inverse_roots(tile, row_start, col_start, shared_rows, shared_total)
    bands = shared_rows(roots)
    whitened = jnp.einsum(
        "tkj,jkc->tkc", whole_sides, bands, preferred_element_type=jnp.float32
    ).astype(jnp.bfloat16)
    acts_whole = spread(whitened[:, :blocks, :]).reshape(tok_dev, blocks * block)
    grads_low = whitened[:, blocks:, :]
    owned_acts = lax.all_to_all(acts_whole, ("tok", "grp"), split_axis=1, concat_axis=0, tiled=True)
    update = jnp.einsum(
        "ta,tbc->abc",
        owned_acts,
        lax.all_gather(grads_low, ("tok", "grp"), axis=0, tiled=True),
        preferred_element_type=jnp.float32,
    )
    update = (update / math.sqrt(token_count)).astype(jnp.bfloat16)
    return (update, input_grad)


MESH = pl.DeviceIdType.MESH
CHUNKS = 8
TURNED = 2
CORNER = 3
ROOM = 50 * 2**20
PARTS = 4
PLAN = (
    ("y", 0, 0), ("x", 0, 0), ("y", 0, 1), ("x", 0, 1), ("z", 1, 0), ("y", 0, 2), ("x", 0, 2),
    ("z", 2, 0), ("y", 0, 3), ("x", 0, 3), ("z", 3, 0), ("z", 1, 1), ("z", 2, 1), ("y", 1, 0),
    ("y", 2, 0), ("x", 1, 0), ("z", 1, 2), ("z", 3, 1), ("x", 2, 0), ("z", 2, 2), ("x", 1, 1),
    ("y", 1, 1), ("x", 3, 0), ("z", 1, 3), ("y", 3, 0), ("c", 0, 0), ("z", 3, 2), ("x", 2, 1),
    ("x", 1, 2), ("y", 1, 2), ("y", 2, 1), ("z", 2, 3), ("y", 3, 1), ("c", 0, 1), ("z", 3, 3),
    ("x", 3, 1), ("y", 2, 2), ("x", 2, 2), ("x", 1, 3), ("d", 0, 0), ("x", 3, 2), ("y", 1, 3),
    ("y", 3, 2), ("c", 0, 2), ("x", 2, 3), ("d", 0, 1), ("y", 2, 3), ("x", 3, 3), ("y", 3, 3),
    ("c", 0, 3), ("d", 0, 2), ("d", 0, 3),
)
LAG = 3


def greet(peers):
    barrier = pltpu.get_barrier_semaphore()
    for peer in peers:
        pl.semaphore_signal(barrier, inc=1, device_id=peer, device_id_type=MESH)
    pl.semaphore_wait(barrier, len(peers))


def remote(src, dst, send, recv, peer):
    return pltpu.make_async_remote_copy(
        src_ref=src, dst_ref=dst, send_sem=send, recv_sem=recv, device_id=peer, device_id_type=MESH
    )


def held(z):
    return z + 2 - 3 * ((z + 2) // 3) + z // 3


def neighbours():
    z, o, y = lax.axis_index("tok"), lax.axis_index("out"), lax.axis_index("grp")
    ox = lax.rem(o + 2, 4)
    oc = o + 1 - 2 * lax.rem(o, 2)
    at = lambda a, b, c: {"tok": a, "out": b, "grp": c}
    zs = [lax.rem(z + j, 4) for j in range(4)]
    peers = [at(zs[j], o, y) for j in (1, 2, 3)]
    return z, o, y, ox, oc, zs, peers, at(z, o, 1 - y), at(z, ox, y), at(z, oc, y)


def hops(z):
    return (z, z + 1 - 2 * lax.rem(z, 2), 2 - z // 2, 3 - 3 * (z // 2))


def fused_kernel(
    pieces, weight, grads, acts, product,
    sides, low, head, left, right, tail, rays, raw, held_weight,
    z_send, send, recv, d_recv, c_send, c_recv, local, w_sem, r_send, r_recv,
    g_send, y_send, t_send, g_recv, y_recv, t_recv, a_send, a_recv, h_send, h_recv, k_send, k_recv, put,
):
    z, o, y, ox, oc, zs, z_peers, y_peer, x_peer, c_peer = neighbours()
    oxc = lax.rem(oc + 2, 4)
    width = pieces.shape[2]
    rows = pieces.shape[1] // PARTS
    group = rows * 8
    tokens, block = sides.shape
    part = left.shape[1]
    near = hops(z)
    across = (((1,), (1,)), ((), ()))
    sent = []

    def columns(oi):
        return pl.ds(pl.multiple_of(oi * width, width), width)

    def tile(oi, yi, zi, s):
        start = pl.multiple_of(((s * 2 + yi) * 4 + zi) * rows, rows)
        return sides.at[pl.ds(start, rows), columns(oi)]

    def piece(zi, s):
        return pieces.at[held(zi), pl.ds(s * rows, rows), :]

    def sem_of(kind, zi, s):
        if kind == CORNER:
            return d_recv.at[s]
        return recv.at[(kind * 4 + zi) * PARTS + s]

    def push(src, where, kind):
        peer = (None, y_peer, x_peer, d_peer)[kind]
        remote(src, tile(*where), send.at[0], sem_of(kind, where[2], where[3]), peer).start()
        sent.append(where)

    def relay(src, where, kind, peer):
        remote(src, tile(*where), send.at[0], sem_of(kind, where[2], where[3]), peer).start()
        sent.append(where)

    def arrived(kind, *where):
        ref = tile(*where)
        remote(ref, ref, send.at[0], sem_of(kind, where[2], where[3]), c_peer).wait_recv()
        return ref

    def band(oi, s):
        return sides.at[pl.ds(s * group, group), columns(oi)]

    def over_core(oi, s, place):
        n = s * 2 + place
        return remote(band(oi, s), band(oi, s), c_send.at[0], c_recv.at[n], c_peer)

    d_peer = {"tok": z, "out": ox, "grp": 1 - y}
    greet(z_peers + [y_peer, x_peer, c_peer, d_peer])
    strip = width // 2
    strips = [(b, i) for b in range(2) for i in range(2)]

    def load(n):
        b, i = strips[n]
        place = (b, pl.ds(i * strip, strip), slice(None))
        return pltpu.make_async_copy(weight.at[place], held_weight.at[place], w_sem.at[n])

    def raw_band(oi):
        return raw.at[:, :, columns(oi)]

    own_raw = pieces.at[2:4]
    raw_local = pltpu.make_async_copy(own_raw, raw_band(o), r_send.at[3])
    raw_x = remote(own_raw, raw_band(o), r_send.at[0], r_recv.at[0], x_peer)
    raw_c = remote(own_raw, raw_band(o), r_send.at[1], r_recv.at[1], c_peer)
    raw_xc = remote(raw_band(ox), raw_band(ox), r_send.at[2], r_recv.at[2], c_peer)
    for s in range(PARTS):
        for j in (3, 2, 1):
            copy = remote(
                piece(near[j], s), tile(o, y, z, s), z_send.at[0], sem_of(0, z, s),
                {"tok": near[j], "out": o, "grp": y},
            )
            copy.start()
        push(piece(z, s), (o, y, z, s), 1)
        push(piece(z, s), (o, y, z, s), 2)
    for s in range(PARTS):
        pltpu.make_async_copy(piece(z, s), tile(o, y, z, s), local.at[0]).start()

    for n in range(4):
        load(n).start()
    raw_local.start()
    raw_c.start()
    ones = jnp.ones((16, block), sides.dtype)

    def rows_of(s):
        return pl.ds(s * group, group)

    def gram_group(s, known):
        here = rows_of(s)
        sums = lax.dot_general(ones, sides[here, :], across, preferred_element_type=jnp.float32)
        rays[0:8, here] = sums[0:8]
        for i in known + [s]:
            there = rows_of(i)
            product = lax.dot_general(
                sides[there, :], sides[here, :], across, preferred_element_type=jnp.float32
            )
            product = product * (1.0 / tokens)
            low[there, here] = product.astype(low.dtype)
            if i != s:
                low[here, there] = jnp.transpose(product).astype(low.dtype)

    def straight(j, s):
        return j == 3 and s == PARTS - 1

    def finish(s):
        over_core(oc, s, 0).wait_recv()
        over_core(oxc, s, 1).wait_recv()
        gram_group(s, known)
        known.append(s)

    known = []
    placed = []
    waiting = []
    for kind, j, s in PLAN:
        if kind == "z":
            where = (o, y, near[j], s)
            ref = arrived(0, *where)
            push(ref, where, 1)
            push(ref, where, 2)
            if straight(j, s):
                push(ref, where, CORNER)
        elif kind == "y":
            where = (o, 1 - y, near[j], s)
            ref = arrived(1, *where)
            if (j + s) % 2 == 0 and not straight(j, s):
                relay(ref, where, CORNER, x_peer)
        elif kind == "x":
            where = (ox, y, near[j], s)
            ref = arrived(2, *where)
            if (j + s) % 2 == 1 and not straight(j, s):
                relay(ref, where, CORNER, y_peer)
        elif kind == "c":
            if not placed:
                pltpu.make_async_copy(pieces.at[0], pieces.at[0], local.at[0]).wait()
                placed.append(s)
            over_core(o, s, 0).start()
        else:
            corner = pl.multiple_of((s * 2 + 1 - y) * 4 * rows, rows)
            ref = sides.at[pl.ds(corner, 4 * rows), columns(ox)]
            remote(ref, ref, send.at[0], d_recv.at[s], c_peer).wait_recv()
            over_core(ox, s, 1).start()
            if waiting:
                finish(waiting.pop())
            waiting.append(s)
    raw_x.start()
    finish(waiting.pop())

    def pair(a, b):
        return jnp.sum(a * b, axis=1, keepdims=True)

    def advance(ray):
        high = ray.astype(low.dtype)
        rest = ray - high.astype(jnp.float32)
        middle = rest.astype(low.dtype)
        least = (rest - middle.astype(jnp.float32)).astype(low.dtype)
        zero = jnp.zeros((13, tokens), low.dtype)
        stack = jnp.concatenate([high, middle, least, zero], axis=0)
        image = jnp.dot(stack, low[...], preferred_element_type=jnp.float32)
        return image[0:1] + image[1:2] + image[2:3] + DAMPING * ray

    ray_0 = rays[0:1, :]
    ray_1 = advance(ray_0)
    ray_2 = advance(ray_1)
    dots = [
        pair(ray_0, ray_0),
        pair(ray_0, ray_1),
        pair(ray_1, ray_1),
        pair(ray_1, ray_2),
        pair(ray_2, ray_2),
    ]

    def moment(power):
        total = jnp.full((1, 1), DAMPING**power * block, jnp.float32)
        for i in range(power):
            total = total + DAMPING ** (power - 1 - i) * dots[i] / tokens
        return total

    scale = moment(2 * POWER - 1) / moment(2 * POWER - 2)
    inverse = 1.0 / scale
    root = 1.0 / jnp.sqrt(scale)
    act_start = 2 * (lax.rem(o, 2) * 2 + y) + o // 2
    is_grad = (z // 3) + (3 - z) // 3
    start = (is_grad * (2 * o + y) + (1 - is_grad) * act_start) * part
    cols = pl.ds(pl.multiple_of(start, part), part)
    tall = min(512, tokens)
    steps = tokens // tall

    def span(i):
        return pl.ds(pl.multiple_of(i * tall, tall), tall)

    def apply(i, source, value):
        image = jnp.dot(low[span(i), :], source[...], preferred_element_type=jnp.float32)
        return (image + DAMPING * value) * inverse

    left[...] = sides[:, cols]

    @pl.loop(0, steps, unroll=True)
    def _(i):
        value = left[span(i), :].astype(jnp.float32)
        value = 1.5 * value - 0.5 * apply(i, left, value)
        head[span(i), :] = value
        right[span(i), :] = value.astype(right.dtype)

    @pl.loop(0, steps, unroll=True)
    def _(i):
        value = apply(i, right, head[span(i), :])
        tail[span(i), :] = value
        left[span(i), :] = value.astype(left.dtype)

    @pl.loop(0, steps, unroll=True)
    def _(i):
        value = tail[span(i), :]
        value = 1.5 * value - 0.5 * apply(i, left, value)
        tail[span(i), :] = value
        right[span(i), :] = value.astype(right.dtype)

    @pl.loop(0, steps, unroll=True)
    def _(i):
        value = tail[span(i), :]
        value = 1.5 * value - 0.5 * apply(i, right, value)
        left[span(i), :] = ((1.5 * head[span(i), :] - 0.5 * value) * root).astype(left.dtype)

    span_rows = tokens // CHUNKS
    is_end = is_grad == 1
    is_middle = is_grad == 0
    mine = z // 3
    h = o // 2
    goal_z = (z // 2) * 2 + lax.rem(o, 2)
    stays = goal_z == z
    goal = {"tok": goal_z, "out": o, "grp": y}
    first, second = z // 2, 1 - z // 2
    is_hub = lax.rem(o, 2) == lax.rem(z, 2)
    here = is_middle & stays
    plain = [c for c in range(CHUNKS - TURNED)]
    turned = [c for c in range(CHUNKS - TURNED, CHUNKS)]

    def rung(c):
        return pl.ds(c * span_rows, span_rows)

    def piece_of(c):
        return left.at[rung(c), :]

    def half(i):
        return pl.ds(pl.multiple_of(i * part, part), part)

    def g_tile(b, yi, c):
        return grads.at[b, rung(c), half(yi)]

    def a_tile(i, c):
        return acts.at[rung(c), half(i)]

    def own_grad():
        return pltpu.make_async_copy(left, grads.at[mine, :, half(y)], put.at[0])

    def own_act():
        return pltpu.make_async_copy(left, acts.at[:, half(h)], put.at[0])

    def onward(b):
        return {"tok": lax.rem(z + 5 - 2 * b, 4), "out": o, "grp": y}

    def to_plane(src, b, c):
        n = b * CHUNKS + c
        return remote(src, g_tile(b, y, c), g_send.at[b], g_recv.at[n], onward(b))

    def lands(b, c):
        if c in turned:
            return t_recv.at[b * TURNED + turned.index(c)]
        return y_recv.at[b]

    def other_to_plane(b, c):
        ref = g_tile(b, 1 - y, c)
        return remote(ref, ref, t_send.at[b], lands(b, c), onward(b))

    def y_copy(src, b, c):
        return remote(src, g_tile(b, y, c), y_send.at[b], lands(b, c), y_peer)

    def to_hub(c):
        return remote(piece_of(c), a_tile(h, c), a_send.at[0], a_recv.at[c], goal)

    def over_x(c, i):
        return remote(a_tile(i, c), a_tile(i, c), h_send.at[0], h_recv.at[c], x_peer)

    def act_core(c, i):
        return remote(a_tile(i, c), a_tile(i, c), k_send.at[0], k_recv.at[0], c_peer)

    for b in range(2):

        @pl.when(z == 3 * b)
        def _():
            for c in turned + plain:
                y_copy(piece_of(c), b, c).start()
            for c in plain + turned:
                to_plane(piece_of(c), b, c).start()

    @pl.when(is_end)
    def _():
        own_grad().start()

    @pl.when(here)
    def _():
        own_act().start()

    @pl.when(is_middle & jnp.logical_not(stays))
    def _():
        for c in range(CHUNKS):
            to_hub(c).start()

    def multiply(n):
        b, i = strips[n]
        load(n).wait()
        total = jnp.zeros((raw.shape[1], strip), jnp.float32)
        for k in range(2):
            total += lax.dot_general(
                raw[k],
                held_weight[b, pl.ds(i * strip, strip), pl.ds(k * block, block)],
                (((1,), (1,)), ((), ())),
                preferred_element_type=jnp.float32,
            )
        product[b, :, pl.ds(i * strip, strip)] = total.astype(product.dtype)

    def hub_step(c):
        if c == 0:

            @pl.when(here)
            def _():
                own_act().wait()

        @pl.when(is_hub & jnp.logical_not(here))
        def _():
            ref = a_tile(h, c)
            remote(ref, ref, a_send.at[0], a_recv.at[c], c_peer).wait_recv()

        @pl.when(is_hub)
        def _():
            over_x(c, h).start()
            act_core(c, h).start()

    def cross_step(c):
        @pl.when(is_hub)
        def _():
            over_x(c, 1 - h).wait_recv()
            act_core(c, 1 - h).start()

    def g_wait(b, c):
        ref = g_tile(b, y, c)
        remote(ref, ref, g_send.at[0], g_recv.at[b * CHUNKS + c], c_peer).wait_recv()
        return ref

    def y_wait(b, c):
        ref = g_tile(b, 1 - y, c)
        remote(ref, ref, y_send.at[0], lands(b, c), c_peer).wait_recv()

    def take(b, kind, c):
        if kind == "own":
            ref = g_wait(b, c)

            @pl.when(is_middle)
            def _():
                to_plane(ref, b, c).start()

            if c not in turned:
                y_copy(ref, b, c).start()
        else:
            y_wait(b, c)

            @pl.when(is_middle)
            def _():
                other_to_plane(b, c).start()

    raw_x.wait_recv()
    raw_xc.start()
    raw_local.wait()
    raw_c.wait_recv()

    def multiply_all():
        raw_xc.wait_recv()
        for n in range(4):
            multiply(n)

    @pl.when(is_end)
    def _():
        for c in turned:
            y_wait(mine, c)
            other_to_plane(mine, c).start()

    pl.when(is_end)(multiply_all)
    flow = [("own", c) for c in plain + turned] + [("other", c) for c in turned]
    for step in range(len(flow) + LAG):
        if step < len(flow):

            @pl.when(is_middle)
            def _():
                take(first, *flow[step])

        if step < CHUNKS:
            hub_step(step)
        if step >= LAG:
            take(second, *flow[step - LAG])
    for c in range(CHUNKS):
        cross_step(c)
    pl.when(is_middle)(multiply_all)
    straight_rows = pl.ds(0, span_rows * len(plain))
    turned_rows = pl.ds(span_rows * len(plain), span_rows * TURNED)

    def settle(ref, sem):
        remote(ref, ref, sem, sem, c_peer).wait_send()

    for b in range(2):
        ref = grads.at[b, straight_rows, half(1 - y)]
        remote(ref, ref, y_send.at[0], y_recv.at[b], c_peer).wait_recv()

        @pl.when(z == 3 * b)
        def _():
            settle(left, y_send.at[b])

        @pl.when(z != 3 * b)
        def _():
            settle(grads.at[b, straight_rows, half(y)], y_send.at[b])

        @pl.when(z != 3 - 3 * b)
        def _():
            settle(left, g_send.at[b])
            settle(grads.at[b, turned_rows, half(1 - y)], t_send.at[b])

    @pl.when(is_end)
    def _():
        own_grad().wait()

    @pl.when(is_middle & jnp.logical_not(stays))
    def _():
        settle(left, a_send.at[0])

    @pl.when(is_hub)
    def _():
        settle(acts, k_send.at[0])
        settle(acts.at[:, half(h)], h_send.at[0])

    @pl.when(jnp.logical_not(is_hub))
    def _():
        remote(acts, acts, k_send.at[0], k_recv.at[0], c_peer).wait_recv()

    raw_x.wait_send()
    raw_c.wait_send()
    raw_xc.wait_send()
    settle(pieces.at[0:3], z_send.at[0])
    settle(sides.at[pl.ds(0, len(sent) * rows * width // block), :], send.at[0])
    settle(sides.at[pl.ds(0, tokens // 2), :], c_send.at[0])


def fused(pieces, weight, part):
    _, rows, width = pieces.shape
    tokens, block = rows * 8, width * 4
    dma = pltpu.SemaphoreType.DMA
    vmem = pl.BlockSpec(memory_space=pltpu.VMEM)
    low = pieces.dtype
    return pl.pallas_call(
        fused_kernel,
        out_shape=(
            jax.ShapeDtypeStruct((2, tokens, 2 * part), low),
            jax.ShapeDtypeStruct((tokens, 2 * part), low),
            jax.ShapeDtypeStruct((2, rows, width), low),
        ),
        in_specs=[vmem, pl.BlockSpec(memory_space=pltpu.HBM)],
        out_specs=(vmem, vmem, vmem),
        scratch_shapes=[
            pltpu.VMEM((tokens, block), low),
            pltpu.VMEM((tokens, tokens), low),
            pltpu.VMEM((tokens, part), jnp.float32),
            pltpu.VMEM((tokens, part), low),
            pltpu.VMEM((tokens, part), low),
            pltpu.VMEM((tokens, part), jnp.float32),
            pltpu.VMEM((8, tokens), jnp.float32),
            pltpu.VMEM((2, rows, block), low),
            pltpu.VMEM(weight.shape, weight.dtype),
            dma((1,)),
            dma((1,)),
            dma((12 * PARTS,)),
            dma((PARTS,)),
            dma((1,)),
            dma((2 * PARTS,)),
            dma((1,)),
            dma((4,)),
            dma((4,)),
            dma((3,)),
            dma((2,)),
            dma((2,)),
            dma((2,)),
            dma((2 * CHUNKS,)),
            dma((2,)),
            dma((2 * TURNED,)),
            dma((1,)),
            dma((CHUNKS,)),
            dma((1,)),
            dma((CHUNKS,)),
            dma((1,)),
            dma((1,)),
            dma((1,)),
        ],
        compiler_params=pltpu.CompilerParams(collective_id=0, has_side_effects=True, vmem_limit_bytes=ROOM),
        name="fused",
    )(pieces, weight)


def planes(activations, out_grads, weight):
    tok_dev, _, width = activations.shape
    part = width // lax.axis_size("grp")
    token_count = tok_dev * lax.axis_size(("tok", "grp"))
    pieces = jnp.swapaxes(jnp.concatenate([activations, out_grads], axis=1), 0, 1)
    grads_low, acts_low, product = fused(pieces, weight, part)
    update = jnp.einsum("ta,btc->abc", acts_low, grads_low, preferred_element_type=jnp.float32)
    update = (update / math.sqrt(token_count)).astype(jnp.bfloat16)
    input_grad = jnp.swapaxes(product, 0, 1)
    return (update, input_grad)


def solution(mesh):
    in_specs = (
        P(("tok", "grp"), None, "out"),
        P(("tok", "grp"), None, "out"),
        P(None, "out", None),
    )
    out_specs = (P(("tok", "grp"), None, "out"), P(("tok", "grp"), None, "out"))

    def body(activations, out_grads, weight):
        blocks = activations.shape[1]
        tok, grp, out = (mesh.shape[name] for name in ("tok", "grp", "out"))
        fits = (blocks, tok, grp, out) == (2, 4, 2, 4)
        return (planes if fits else local)(activations, out_grads, weight)

    return jax.shard_map(body, mesh=mesh, in_specs=in_specs, out_specs=out_specs, check_vma=False)
```

```python
import math

import jax
import jax.numpy as jnp
from jax import lax
from jax.experimental import pallas as pl
from jax.experimental.pallas import tpu as pltpu
from jax.sharding import PartitionSpec as P

POWER = 3


DAMPING = 0.1
HIGH = lax.Precision.HIGHEST


def spread(piece):
    return lax.all_gather(piece, "out", axis=2, tiled=True)


def token_sums(maker, rows):
    return lax.psum_scatter(
        maker(jnp.int32(0), rows * lax.axis_size(("tok", "grp"))),
        ("tok", "grp"),
        scatter_dimension=0,
        tiled=True,
    )


def shared_rows(piece):
    return lax.all_gather(piece, ("tok", "grp"), axis=0, tiled=True)


def shared_total(vector):
    return lax.psum(vector, ("tok", "out", "grp"))


def diagonal_mask(rows, width, row_start, col_start):
    row_ids = row_start + lax.broadcasted_iota(jnp.int32, (rows, 1, width), 0)
    col_ids = col_start + lax.broadcasted_iota(jnp.int32, (rows, 1, width), 2)
    return jnp.where(row_ids == col_ids, 1.0, 0.0).astype(jnp.float32)


def multiply(left, right, gather_columns):
    row_band = spread(left)
    column_band = gather_columns(right)
    return jnp.einsum("rkj,jkc->rkc", row_band, column_band, preferred_element_type=jnp.float32)


def inverse_roots(tile, row_start, col_start, gather_columns, total):
    rows, count, width = tile.shape
    block = width * lax.axis_size("out")
    mask = diagonal_mask(rows, width, row_start, col_start)
    vector = jnp.ones((count, block), jnp.float32)
    image = vector
    for step in range(POWER):
        columns = lax.dynamic_slice_in_dim(vector, col_start, width, 1)
        part = jnp.einsum("rkc,kc->kr", tile, columns, precision=HIGH)
        placed = lax.dynamic_update_slice_in_dim(
            jnp.zeros((count, block), jnp.float32), part, row_start, 1
        )
        image = total(placed)
        if step + 1 < POWER:
            vector = image / jnp.sqrt(jnp.sum(image * image, axis=1, keepdims=True))
    scale = jnp.sum(vector * image, axis=1) / jnp.sum(vector * vector, axis=1)
    start = tile / scale[None, :, None]
    start_low = start.astype(jnp.bfloat16)
    first_low = ((3.0 * mask - start) / 2.0).astype(jnp.bfloat16)
    square_low = multiply(first_low, first_low, gather_columns).astype(jnp.bfloat16)
    moved = multiply(square_low, start_low, gather_columns)
    second_low = ((3.0 * mask - moved) / 2.0).astype(jnp.bfloat16)
    roots = multiply(first_low, second_low, gather_columns) / jnp.sqrt(scale)[None, :, None]
    return roots.astype(jnp.bfloat16)


def local(activations, out_grads, weight):
    tok_dev, blocks, width = activations.shape
    block = width * lax.axis_size("out")
    token_count = tok_dev * lax.axis_size("tok") * lax.axis_size("grp")
    col_start = lax.axis_index("out") * width
    local_sides = jnp.concatenate([activations, out_grads], axis=1)
    whole_sides = spread(local_sides)
    grads_whole = whole_sides[:, blocks:, :]
    weight_rows = weight.reshape(blocks, width, blocks, block)
    input_grad = jnp.einsum(
        "tjq,bcjq->tbc", grads_whole, weight_rows, preferred_element_type=jnp.float32
    ).astype(jnp.bfloat16)
    rows = block // (lax.axis_size("tok") * lax.axis_size("grp"))
    row_start = lax.axis_index(("tok", "grp")) * rows

    def shared_terms(start, span):
        return jnp.einsum(
            "tkr,tkc->rkc", whole_sides, local_sides, preferred_element_type=jnp.float32
        )

    sums = token_sums(shared_terms, rows)
    tile = sums / token_count + DAMPING * diagonal_mask(rows, width, row_start, col_start)
    roots = inverse_roots(tile, row_start, col_start, shared_rows, shared_total)
    bands = shared_rows(roots)
    whitened = jnp.einsum(
        "tkj,jkc->tkc", whole_sides, bands, preferred_element_type=jnp.float32
    ).astype(jnp.bfloat16)
    acts_whole = spread(whitened[:, :blocks, :]).reshape(tok_dev, blocks * block)
    grads_low = whitened[:, blocks:, :]
    owned_acts = lax.all_to_all(acts_whole, ("tok", "grp"), split_axis=1, concat_axis=0, tiled=True)
    update = jnp.einsum(
        "ta,tbc->abc",
        owned_acts,
        lax.all_gather(grads_low, ("tok", "grp"), axis=0, tiled=True),
        preferred_element_type=jnp.float32,
    )
    update = (update / math.sqrt(token_count)).astype(jnp.bfloat16)
    return (update, input_grad)


MESH = pl.DeviceIdType.MESH
CHUNKS = 8
TURNED = 1
CORNER = 3
ROOM = 50 * 2**20
STEPS = 2
PARTS = 4
PLAN = (
    ("y", 0, 0), ("x", 0, 0), ("y", 0, 1), ("x", 0, 1), ("z", 1, 0), ("y", 0, 2), ("x", 0, 2),
    ("z", 2, 0), ("y", 0, 3), ("x", 0, 3), ("z", 3, 0), ("z", 1, 1), ("z", 2, 1), ("y", 1, 0),
    ("y", 2, 0), ("x", 1, 0), ("z", 1, 2), ("z", 3, 1), ("x", 2, 0), ("z", 2, 2), ("x", 1, 1),
    ("y", 1, 1), ("x", 3, 0), ("z", 1, 3), ("y", 3, 0), ("c", 0, 0), ("z", 3, 2), ("x", 2, 1),
    ("x", 1, 2), ("y", 1, 2), ("y", 2, 1), ("z", 2, 3), ("y", 3, 1), ("c", 0, 1), ("z", 3, 3),
    ("x", 3, 1), ("y", 2, 2), ("x", 2, 2), ("x", 1, 3), ("d", 0, 0), ("x", 3, 2), ("y", 1, 3),
    ("y", 3, 2), ("c", 0, 2), ("x", 2, 3), ("d", 0, 1), ("y", 2, 3), ("x", 3, 3), ("y", 3, 3),
    ("c", 0, 3), ("d", 0, 2), ("d", 0, 3),
)
LAG = 2


def greet(peers):
    barrier = pltpu.get_barrier_semaphore()
    for peer in peers:
        pl.semaphore_signal(barrier, inc=1, device_id=peer, device_id_type=MESH)
    pl.semaphore_wait(barrier, len(peers))


def remote(src, dst, send, recv, peer):
    return pltpu.make_async_remote_copy(
        src_ref=src, dst_ref=dst, send_sem=send, recv_sem=recv, device_id=peer, device_id_type=MESH
    )


def held(z):
    return z + 2 - 3 * ((z + 2) // 3) + z // 3


def neighbours():
    z, o, y = lax.axis_index("tok"), lax.axis_index("out"), lax.axis_index("grp")
    ox = lax.rem(o + 2, 4)
    oc = o + 1 - 2 * lax.rem(o, 2)
    at = lambda a, b, c: {"tok": a, "out": b, "grp": c}
    zs = [lax.rem(z + j, 4) for j in range(4)]
    peers = [at(zs[j], o, y) for j in (1, 2, 3)]
    return z, o, y, ox, oc, zs, peers, at(z, o, 1 - y), at(z, ox, y), at(z, oc, y)


def hops(z):
    return (z, z + 1 - 2 * lax.rem(z, 2), 2 - z // 2, 3 - 3 * (z // 2))


def fused_kernel(
    pieces, weight, grads, acts, product,
    sides, low, head, left, right, tail, rays, raw, held_weight,
    z_send, send, recv, d_recv, c_send, c_recv, local, w_sem, r_send, r_recv,
    g_send, y_send, t_send, g_recv, y_recv, t_recv, a_send, a_recv, h_send, h_recv, k_send, k_recv, put,
):
    z, o, y, ox, oc, zs, z_peers, y_peer, x_peer, c_peer = neighbours()
    oxc = lax.rem(oc + 2, 4)
    width = pieces.shape[2]
    rows = pieces.shape[1] // PARTS
    group = rows * 8
    tokens, block = sides.shape
    part = left.shape[1]
    near = hops(z)
    across = (((1,), (1,)), ((), ()))
    sent = []

    def columns(oi):
        return pl.ds(pl.multiple_of(oi * width, width), width)

    def tile(oi, yi, zi, s):
        start = pl.multiple_of(((s * 2 + yi) * 4 + zi) * rows, rows)
        return sides.at[pl.ds(start, rows), columns(oi)]

    def piece(zi, s):
        return pieces.at[held(zi), pl.ds(s * rows, rows), :]

    def sem_of(kind, zi, s):
        if kind == CORNER:
            return d_recv.at[s]
        return recv.at[(kind * 4 + zi) * PARTS + s]

    def push(src, where, kind):
        peer = (None, y_peer, x_peer, d_peer)[kind]
        remote(src, tile(*where), send.at[0], sem_of(kind, where[2], where[3]), peer).start()
        sent.append(where)

    def relay(src, where, kind, peer):
        remote(src, tile(*where), send.at[0], sem_of(kind, where[2], where[3]), peer).start()
        sent.append(where)

    def arrived(kind, *where):
        ref = tile(*where)
        remote(ref, ref, send.at[0], sem_of(kind, where[2], where[3]), c_peer).wait_recv()
        return ref

    def band(oi, s):
        return sides.at[pl.ds(s * group, group), columns(oi)]

    def over_core(oi, s, place):
        n = s * 2 + place
        return remote(band(oi, s), band(oi, s), c_send.at[0], c_recv.at[n], c_peer)

    d_peer = {"tok": z, "out": ox, "grp": 1 - y}
    greet(z_peers + [y_peer, x_peer, c_peer, d_peer])
    strip = width // 2
    strips = [(b, i) for b in range(2) for i in range(2)]

    def load(n):
        b, i = strips[n]
        place = (b, pl.ds(i * strip, strip), slice(None))
        return pltpu.make_async_copy(weight.at[place], held_weight.at[place], w_sem.at[n])

    def raw_band(oi):
        return raw.at[:, :, columns(oi)]

    own_raw = pieces.at[2:4]
    raw_local = pltpu.make_async_copy(own_raw, raw_band(o), r_send.at[3])
    raw_x = remote(own_raw, raw_band(o), r_send.at[0], r_recv.at[0], x_peer)
    raw_c = remote(own_raw, raw_band(o), r_send.at[1], r_recv.at[1], c_peer)
    raw_xc = remote(raw_band(ox), raw_band(ox), r_send.at[2], r_recv.at[2], c_peer)
    for s in range(PARTS):
        for j in (3, 2, 1):
            copy = remote(
                piece(near[j], s), tile(o, y, z, s), z_send.at[0], sem_of(0, z, s),
                {"tok": near[j], "out": o, "grp": y},
            )
            copy.start()
        push(piece(z, s), (o, y, z, s), 1)
        push(piece(z, s), (o, y, z, s), 2)
    for s in range(PARTS):
        pltpu.make_async_copy(piece(z, s), tile(o, y, z, s), local.at[0]).start()

    for n in range(4):
        load(n).start()
    raw_local.start()
    raw_c.start()
    ones = jnp.ones((16, block), sides.dtype)

    def rows_of(s):
        return pl.ds(s * group, group)

    def gram_group(s, known):
        here = rows_of(s)
        sums = lax.dot_general(ones, sides[here, :], across, preferred_element_type=jnp.float32)
        rays[0:8, here] = sums[0:8]
        for i in known + [s]:
            there = rows_of(i)
            product = lax.dot_general(
                sides[there, :], sides[here, :], across, preferred_element_type=jnp.float32
            )
            product = product * (1.0 / tokens)
            low[there, here] = product.astype(low.dtype)
            if i != s:
                low[here, there] = jnp.transpose(product).astype(low.dtype)

    def straight(j, s):
        return j == 3 and s == PARTS - 1

    def finish(s):
        over_core(oc, s, 0).wait_recv()
        over_core(oxc, s, 1).wait_recv()
        gram_group(s, known)
        known.append(s)

    known = []
    placed = []
    waiting = []
    for kind, j, s in PLAN:
        if kind == "z":
            where = (o, y, near[j], s)
            ref = arrived(0, *where)
            push(ref, where, 1)
            push(ref, where, 2)
            if straight(j, s):
                push(ref, where, CORNER)
        elif kind == "y":
            where = (o, 1 - y, near[j], s)
            ref = arrived(1, *where)
            if (j + s) % 2 == 0 and not straight(j, s):
                relay(ref, where, CORNER, x_peer)
        elif kind == "x":
            where = (ox, y, near[j], s)
            ref = arrived(2, *where)
            if (j + s) % 2 == 1 and not straight(j, s):
                relay(ref, where, CORNER, y_peer)
        elif kind == "c":
            if not placed:
                pltpu.make_async_copy(pieces.at[0], pieces.at[0], local.at[0]).wait()
                placed.append(s)
            over_core(o, s, 0).start()
        else:
            corner = pl.multiple_of((s * 2 + 1 - y) * 4 * rows, rows)
            ref = sides.at[pl.ds(corner, 4 * rows), columns(ox)]
            remote(ref, ref, send.at[0], d_recv.at[s], c_peer).wait_recv()
            over_core(ox, s, 1).start()
            if waiting:
                finish(waiting.pop())
            waiting.append(s)
    raw_x.start()
    finish(waiting.pop())

    def pair(a, b):
        return jnp.sum(a * b, axis=1, keepdims=True)

    def advance(ray):
        high = ray.astype(low.dtype)
        rest = ray - high.astype(jnp.float32)
        middle = rest.astype(low.dtype)
        least = (rest - middle.astype(jnp.float32)).astype(low.dtype)
        zero = jnp.zeros((13, tokens), low.dtype)
        stack = jnp.concatenate([high, middle, least, zero], axis=0)
        image = jnp.dot(stack, low[...], preferred_element_type=jnp.float32)
        return image[0:1] + image[1:2] + image[2:3] + DAMPING * ray

    ray_0 = rays[0:1, :]
    ray_1 = advance(ray_0)
    ray_2 = advance(ray_1)
    dots = [
        pair(ray_0, ray_0),
        pair(ray_0, ray_1),
        pair(ray_1, ray_1),
        pair(ray_1, ray_2),
        pair(ray_2, ray_2),
    ]

    def moment(power):
        total = jnp.full((1, 1), DAMPING**power * block, jnp.float32)
        for i in range(power):
            total = total + DAMPING ** (power - 1 - i) * dots[i] / tokens
        return total

    scale = moment(2 * POWER - 1) / moment(2 * POWER - 2)
    inverse = 1.0 / scale
    root = 1.0 / jnp.sqrt(scale)
    act_start = 2 * (lax.rem(o, 2) * 2 + y) + o // 2
    is_grad = (z // 3) + (3 - z) // 3
    start = (is_grad * (2 * o + y) + (1 - is_grad) * act_start) * part
    cols = pl.ds(pl.multiple_of(start, part), part)
    tall = min(512, tokens)
    steps = tokens // tall

    def span(i):
        return pl.ds(pl.multiple_of(i * tall, tall), tall)

    def apply(i, source, value):
        image = jnp.dot(low[span(i), :], source[...], preferred_element_type=jnp.float32)
        return (image + DAMPING * value) * inverse

    left[...] = sides[:, cols]

    @pl.loop(0, steps, unroll=True)
    def _(i):
        value = left[span(i), :].astype(jnp.float32)
        value = 1.5 * value - 0.5 * apply(i, left, value)
        head[span(i), :] = value
        right[span(i), :] = value.astype(right.dtype)

    @pl.loop(0, steps, unroll=True)
    def _(i):
        value = apply(i, right, head[span(i), :])
        tail[span(i), :] = value
        left[span(i), :] = value.astype(left.dtype)

    @pl.loop(0, steps, unroll=True)
    def _(i):
        value = tail[span(i), :]
        value = 1.5 * value - 0.5 * apply(i, left, value)
        tail[span(i), :] = value
        right[span(i), :] = value.astype(right.dtype)

    @pl.loop(0, steps, unroll=True)
    def _(i):
        value = tail[span(i), :]
        value = 1.5 * value - 0.5 * apply(i, right, value)
        left[span(i), :] = ((1.5 * head[span(i), :] - 0.5 * value) * root).astype(left.dtype)

    span_rows = tokens // CHUNKS
    is_end = is_grad == 1
    is_middle = is_grad == 0
    mine = z // 3
    h = o // 2
    goal_z = (z // 2) * 2 + lax.rem(o, 2)
    stays = goal_z == z
    goal = {"tok": goal_z, "out": o, "grp": y}
    first, second = z // 2, 1 - z // 2
    is_hub = lax.rem(o, 2) == lax.rem(z, 2)
    here = is_middle & stays
    plain = [c for c in range(CHUNKS - TURNED)]
    turned = [c for c in range(CHUNKS - TURNED, CHUNKS)]

    def rung(c):
        return pl.ds(c * span_rows, span_rows)

    def piece_of(c):
        return left.at[rung(c), :]

    def half(i):
        return pl.ds(pl.multiple_of(i * part, part), part)

    def g_tile(b, yi, c):
        return grads.at[b, rung(c), half(yi)]

    def a_tile(i, c):
        return acts.at[rung(c), half(i)]

    def own_grad():
        return pltpu.make_async_copy(left, grads.at[mine, :, half(y)], put.at[0])

    def own_act():
        return pltpu.make_async_copy(left, acts.at[:, half(h)], put.at[0])

    def onward(b):
        return {"tok": lax.rem(z + 5 - 2 * b, 4), "out": o, "grp": y}

    def to_plane(src, b, c):
        n = b * CHUNKS + c
        return remote(src, g_tile(b, y, c), g_send.at[b], g_recv.at[n], onward(b))

    def lands(b, c):
        if c in turned:
            return t_recv.at[b * TURNED + turned.index(c)]
        return y_recv.at[b]

    def other_to_plane(b, c):
        ref = g_tile(b, 1 - y, c)
        return remote(ref, ref, t_send.at[b], lands(b, c), onward(b))

    def y_copy(src, b, c):
        return remote(src, g_tile(b, y, c), y_send.at[b], lands(b, c), y_peer)

    def to_hub(c):
        return remote(piece_of(c), a_tile(h, c), a_send.at[0], a_recv.at[c], goal)

    def over_x(c, i):
        return remote(a_tile(i, c), a_tile(i, c), h_send.at[0], h_recv.at[c], x_peer)

    def act_core(c, i):
        return remote(a_tile(i, c), a_tile(i, c), k_send.at[0], k_recv.at[0], c_peer)

    for b in range(2):

        @pl.when(z == 3 * b)
        def _():
            for c in turned + plain:
                y_copy(piece_of(c), b, c).start()
            for c in plain + turned:
                to_plane(piece_of(c), b, c).start()

    @pl.when(is_end)
    def _():
        own_grad().start()

    @pl.when(here)
    def _():
        own_act().start()

    @pl.when(is_middle & jnp.logical_not(stays))
    def _():
        for c in range(CHUNKS):
            to_hub(c).start()

    def strip_product(n):
        b, i = strips[n]
        load(n).wait()
        total = jnp.zeros((raw.shape[1], strip), jnp.float32)
        for k in range(2):
            total += lax.dot_general(
                raw[k],
                held_weight[b, pl.ds(i * strip, strip), pl.ds(k * block, block)],
                (((1,), (1,)), ((), ())),
                preferred_element_type=jnp.float32,
            )
        return total

    def multiply(i):
        pair_of = jnp.stack([strip_product(i), strip_product(2 + i)], axis=1)
        product[:, :, pl.ds(i * strip, strip)] = pair_of.astype(product.dtype)

    def hub_step(c):
        if c == 0:

            @pl.when(here)
            def _():
                own_act().wait()

        @pl.when(is_hub & jnp.logical_not(here))
        def _():
            ref = a_tile(h, c)
            remote(ref, ref, a_send.at[0], a_recv.at[c], c_peer).wait_recv()

        @pl.when(is_hub)
        def _():
            over_x(c, h).start()
            act_core(c, h).start()

    def cross_step(c):
        @pl.when(is_hub)
        def _():
            over_x(c, 1 - h).wait_recv()
            act_core(c, 1 - h).start()

    def g_wait(b, c):
        ref = g_tile(b, y, c)
        remote(ref, ref, g_send.at[0], g_recv.at[b * CHUNKS + c], c_peer).wait_recv()
        return ref

    def y_wait(b, c):
        ref = g_tile(b, 1 - y, c)
        remote(ref, ref, y_send.at[0], lands(b, c), c_peer).wait_recv()

    def take(b, kind, c):
        if kind == "own":
            ref = g_wait(b, c)

            @pl.when(is_middle)
            def _():
                to_plane(ref, b, c).start()

            if c not in turned:
                y_copy(ref, b, c).start()
        else:
            y_wait(b, c)

            @pl.when(is_middle)
            def _():
                other_to_plane(b, c).start()

    raw_x.wait_recv()
    raw_xc.start()
    raw_local.wait()
    raw_c.wait_recv()

    def multiply_all():
        raw_xc.wait_recv()
        for i in range(2):
            multiply(i)

    @pl.when(is_end)
    def _():
        for c in turned:
            y_wait(mine, c)
            other_to_plane(mine, c).start()

    pl.when(is_end)(multiply_all)
    flow = [("own", c) for c in plain + turned] + [("other", c) for c in turned]
    for step in range(len(flow) + LAG):
        if step < len(flow):

            @pl.when(is_middle)
            def _():
                take(first, *flow[step])

        if step < CHUNKS:
            hub_step(step)
        if step >= LAG:
            take(second, *flow[step - LAG])
    for c in range(CHUNKS):
        cross_step(c)
    pl.when(is_middle)(multiply_all)
    straight_rows = pl.ds(0, span_rows * len(plain))
    turned_rows = pl.ds(span_rows * len(plain), span_rows * TURNED)

    def settle(ref, sem):
        remote(ref, ref, sem, sem, c_peer).wait_send()

    for b in range(2):
        ref = grads.at[b, straight_rows, half(1 - y)]
        remote(ref, ref, y_send.at[0], y_recv.at[b], c_peer).wait_recv()

        @pl.when(z == 3 * b)
        def _():
            settle(left, y_send.at[b])

        @pl.when(z != 3 * b)
        def _():
            settle(grads.at[b, straight_rows, half(y)], y_send.at[b])

        @pl.when(z != 3 - 3 * b)
        def _():
            settle(left, g_send.at[b])
            settle(grads.at[b, turned_rows, half(1 - y)], t_send.at[b])

    @pl.when(is_end)
    def _():
        own_grad().wait()

    @pl.when(is_middle & jnp.logical_not(stays))
    def _():
        settle(left, a_send.at[0])

    @pl.when(is_hub)
    def _():
        settle(acts, k_send.at[0])
        settle(acts.at[:, half(h)], h_send.at[0])

    @pl.when(jnp.logical_not(is_hub))
    def _():
        remote(acts, acts, k_send.at[0], k_recv.at[0], c_peer).wait_recv()

    raw_x.wait_send()
    raw_c.wait_send()
    raw_xc.wait_send()
    settle(pieces.at[0:3], z_send.at[0])
    settle(sides.at[pl.ds(0, len(sent) * rows * width // block), :], send.at[0])
    settle(sides.at[pl.ds(0, tokens // 2), :], c_send.at[0])


def fused(pieces, weight, part):
    _, rows, width = pieces.shape
    tokens, block = rows * 8, width * 4
    dma = pltpu.SemaphoreType.DMA
    vmem = pl.BlockSpec(memory_space=pltpu.VMEM)
    low = pieces.dtype
    return pl.pallas_call(
        fused_kernel,
        out_shape=(
            jax.ShapeDtypeStruct((2, tokens, 2 * part), low),
            jax.ShapeDtypeStruct((tokens, 2 * part), low),
            jax.ShapeDtypeStruct((rows, 2, width), low),
        ),
        in_specs=[vmem, pl.BlockSpec(memory_space=pltpu.HBM)],
        out_specs=(vmem, vmem, vmem),
        scratch_shapes=[
            pltpu.VMEM((tokens, block), low),
            pltpu.VMEM((tokens, tokens), low),
            pltpu.VMEM((tokens, part), jnp.float32),
            pltpu.VMEM((tokens, part), low),
            pltpu.VMEM((tokens, part), low),
            pltpu.VMEM((tokens, part), jnp.float32),
            pltpu.VMEM((8, tokens), jnp.float32),
            pltpu.VMEM((2, rows, block), low),
            pltpu.VMEM(weight.shape, weight.dtype),
            dma((1,)),
            dma((1,)),
            dma((12 * PARTS,)),
            dma((PARTS,)),
            dma((1,)),
            dma((2 * PARTS,)),
            dma((1,)),
            dma((4,)),
            dma((4,)),
            dma((3,)),
            dma((2,)),
            dma((2,)),
            dma((2,)),
            dma((2 * CHUNKS,)),
            dma((2,)),
            dma((2 * TURNED,)),
            dma((1,)),
            dma((CHUNKS,)),
            dma((1,)),
            dma((CHUNKS,)),
            dma((1,)),
            dma((1,)),
            dma((1,)),
        ],
        compiler_params=pltpu.CompilerParams(collective_id=0, has_side_effects=True, vmem_limit_bytes=ROOM),
        name="fused",
    )(pieces, weight)


def update_kernel(grads, acts, product, update, input_grad, sem):
    i = pl.program_id(0)
    tokens = acts.shape[0]
    tall = update.shape[0]
    copy = pltpu.make_async_copy(product, input_grad, sem)

    @pl.when(i == 0)
    def _():
        copy.start()

    left = acts[:, pl.ds(pl.multiple_of(i * tall, tall), tall)]
    down = (((0,), (0,)), ((), ()))
    both = [
        lax.dot_general(left, grads[b], down, preferred_element_type=jnp.float32)
        * (1.0 / math.sqrt(tokens))
        for b in range(2)
    ]
    update[...] = jnp.stack([u.astype(update.dtype) for u in both], axis=1)

    @pl.when(i == pl.num_programs(0) - 1)
    def _():
        copy.wait()


def update_product(grads, acts, product):
    count, tokens, width = grads.shape
    height = acts.shape[1]
    tall = height // STEPS
    vmem = pl.BlockSpec(memory_space=pltpu.VMEM)
    return pl.pallas_call(
        update_kernel,
        grid=(STEPS,),
        out_shape=(
            jax.ShapeDtypeStruct((height, count, width), grads.dtype),
            jax.ShapeDtypeStruct(product.shape, product.dtype),
        ),
        in_specs=[vmem, vmem, vmem],
        out_specs=(
            pl.BlockSpec((tall, count, width), lambda i: (i, 0, 0)),
            pl.BlockSpec(memory_space=pl.ANY),
        ),
        scratch_shapes=[pltpu.SemaphoreType.DMA],
        compiler_params=pltpu.CompilerParams(vmem_limit_bytes=ROOM),
        name="update",
    )(grads, acts, product)


def planes(activations, out_grads, weight):
    tok_dev, _, width = activations.shape
    part = width // lax.axis_size("grp")
    token_count = tok_dev * lax.axis_size(("tok", "grp"))
    pieces = jnp.swapaxes(jnp.concatenate([activations, out_grads], axis=1), 0, 1)
    grads_low, acts_low, product = fused(pieces, weight, part)
    return update_product(grads_low, acts_low, product)


def solution(mesh):
    in_specs = (
        P(("tok", "grp"), None, "out"),
        P(("tok", "grp"), None, "out"),
        P(None, "out", None),
    )
    out_specs = (P(("tok", "grp"), None, "out"), P(("tok", "grp"), None, "out"))

    def body(activations, out_grads, weight):
        blocks = activations.shape[1]
        tok, grp, out = (mesh.shape[name] for name in ("tok", "grp", "out"))
        fits = (blocks, tok, grp, out) == (2, 4, 2, 4)
        return (planes if fits else local)(activations, out_grads, weight)

    return jax.shard_map(body, mesh=mesh, in_specs=in_specs, out_specs=out_specs, check_vma=False)
```

```python
import math

import jax
import jax.numpy as jnp
from jax import lax
from jax.experimental import pallas as pl
from jax.experimental.pallas import tpu as pltpu
from jax.sharding import PartitionSpec as P

POWER = 3


DAMPING = 0.1
HIGH = lax.Precision.HIGHEST


def spread(piece):
    return lax.all_gather(piece, "out", axis=2, tiled=True)


def token_sums(maker, rows):
    return lax.psum_scatter(
        maker(jnp.int32(0), rows * lax.axis_size(("tok", "grp"))),
        ("tok", "grp"),
        scatter_dimension=0,
        tiled=True,
    )


def shared_rows(piece):
    return lax.all_gather(piece, ("tok", "grp"), axis=0, tiled=True)


def shared_total(vector):
    return lax.psum(vector, ("tok", "out", "grp"))


def diagonal_mask(rows, width, row_start, col_start):
    row_ids = row_start + lax.broadcasted_iota(jnp.int32, (rows, 1, width), 0)
    col_ids = col_start + lax.broadcasted_iota(jnp.int32, (rows, 1, width), 2)
    return jnp.where(row_ids == col_ids, 1.0, 0.0).astype(jnp.float32)


def multiply(left, right, gather_columns):
    row_band = spread(left)
    column_band = gather_columns(right)
    return jnp.einsum("rkj,jkc->rkc", row_band, column_band, preferred_element_type=jnp.float32)


def inverse_roots(tile, row_start, col_start, gather_columns, total):
    rows, count, width = tile.shape
    block = width * lax.axis_size("out")
    mask = diagonal_mask(rows, width, row_start, col_start)
    vector = jnp.ones((count, block), jnp.float32)
    image = vector
    for step in range(POWER):
        columns = lax.dynamic_slice_in_dim(vector, col_start, width, 1)
        part = jnp.einsum("rkc,kc->kr", tile, columns, precision=HIGH)
        placed = lax.dynamic_update_slice_in_dim(
            jnp.zeros((count, block), jnp.float32), part, row_start, 1
        )
        image = total(placed)
        if step + 1 < POWER:
            vector = image / jnp.sqrt(jnp.sum(image * image, axis=1, keepdims=True))
    scale = jnp.sum(vector * image, axis=1) / jnp.sum(vector * vector, axis=1)
    start = tile / scale[None, :, None]
    start_low = start.astype(jnp.bfloat16)
    first_low = ((3.0 * mask - start) / 2.0).astype(jnp.bfloat16)
    square_low = multiply(first_low, first_low, gather_columns).astype(jnp.bfloat16)
    moved = multiply(square_low, start_low, gather_columns)
    second_low = ((3.0 * mask - moved) / 2.0).astype(jnp.bfloat16)
    roots = multiply(first_low, second_low, gather_columns) / jnp.sqrt(scale)[None, :, None]
    return roots.astype(jnp.bfloat16)


def local(activations, out_grads, weight):
    tok_dev, blocks, width = activations.shape
    block = width * lax.axis_size("out")
    token_count = tok_dev * lax.axis_size("tok") * lax.axis_size("grp")
    col_start = lax.axis_index("out") * width
    local_sides = jnp.concatenate([activations, out_grads], axis=1)
    whole_sides = spread(local_sides)
    grads_whole = whole_sides[:, blocks:, :]
    weight_rows = weight.reshape(blocks, width, blocks, block)
    input_grad = jnp.einsum(
        "tjq,bcjq->tbc", grads_whole, weight_rows, preferred_element_type=jnp.float32
    ).astype(jnp.bfloat16)
    rows = block // (lax.axis_size("tok") * lax.axis_size("grp"))
    row_start = lax.axis_index(("tok", "grp")) * rows

    def shared_terms(start, span):
        return jnp.einsum(
            "tkr,tkc->rkc", whole_sides, local_sides, preferred_element_type=jnp.float32
        )

    sums = token_sums(shared_terms, rows)
    tile = sums / token_count + DAMPING * diagonal_mask(rows, width, row_start, col_start)
    roots = inverse_roots(tile, row_start, col_start, shared_rows, shared_total)
    bands = shared_rows(roots)
    whitened = jnp.einsum(
        "tkj,jkc->tkc", whole_sides, bands, preferred_element_type=jnp.float32
    ).astype(jnp.bfloat16)
    acts_whole = spread(whitened[:, :blocks, :]).reshape(tok_dev, blocks * block)
    grads_low = whitened[:, blocks:, :]
    owned_acts = lax.all_to_all(acts_whole, ("tok", "grp"), split_axis=1, concat_axis=0, tiled=True)
    update = jnp.einsum(
        "ta,tbc->abc",
        owned_acts,
        lax.all_gather(grads_low, ("tok", "grp"), axis=0, tiled=True),
        preferred_element_type=jnp.float32,
    )
    update = (update / math.sqrt(token_count)).astype(jnp.bfloat16)
    return (update, input_grad)


MESH = pl.DeviceIdType.MESH
CHUNKS = 8
TURNED = 1
CORNER = 3
ROOM = 50 * 2**20
STEPS = 2
PARTS = 4
PLAN = (
    ("y", 0, 0), ("x", 0, 0), ("y", 0, 1), ("x", 0, 1), ("z", 1, 0), ("y", 0, 2), ("x", 0, 2),
    ("z", 2, 0), ("y", 0, 3), ("x", 0, 3), ("z", 3, 0), ("z", 1, 1), ("z", 2, 1), ("y", 1, 0),
    ("y", 2, 0), ("x", 1, 0), ("z", 1, 2), ("z", 3, 1), ("x", 2, 0), ("z", 2, 2), ("x", 1, 1),
    ("y", 1, 1), ("x", 3, 0), ("z", 1, 3), ("y", 3, 0), ("c", 0, 0), ("z", 3, 2), ("x", 2, 1),
    ("x", 1, 2), ("y", 1, 2), ("y", 2, 1), ("z", 2, 3), ("y", 3, 1), ("c", 0, 1), ("z", 3, 3),
    ("x", 3, 1), ("y", 2, 2), ("x", 2, 2), ("x", 1, 3), ("d", 0, 0), ("x", 3, 2), ("y", 1, 3),
    ("y", 3, 2), ("c", 0, 2), ("x", 2, 3), ("d", 0, 1), ("y", 2, 3), ("x", 3, 3), ("y", 3, 3),
    ("c", 0, 3), ("d", 0, 2), ("d", 0, 3),
)
LAG = 2


def greet(peers, meanwhile):
    barrier = pltpu.get_barrier_semaphore()
    for peer in peers:
        pl.semaphore_signal(barrier, inc=1, device_id=peer, device_id_type=MESH)
    meanwhile()
    pl.semaphore_wait(barrier, len(peers))


def remote(src, dst, send, recv, peer):
    return pltpu.make_async_remote_copy(
        src_ref=src, dst_ref=dst, send_sem=send, recv_sem=recv, device_id=peer, device_id_type=MESH
    )


def held(z):
    return z + 2 - 3 * ((z + 2) // 3) + z // 3


def neighbours():
    z, o, y = lax.axis_index("tok"), lax.axis_index("out"), lax.axis_index("grp")
    ox = lax.rem(o + 2, 4)
    oc = o + 1 - 2 * lax.rem(o, 2)
    at = lambda a, b, c: {"tok": a, "out": b, "grp": c}
    zs = [lax.rem(z + j, 4) for j in range(4)]
    peers = [at(zs[j], o, y) for j in (1, 2, 3)]
    return z, o, y, ox, oc, zs, peers, at(z, o, 1 - y), at(z, ox, y), at(z, oc, y)


def hops(z):
    return (z, z + 1 - 2 * lax.rem(z, 2), 2 - z // 2, 3 - 3 * (z // 2))


def fused_kernel(
    activations, out_grads, weight, grads, acts, product,
    staged, f_sem, pieces, sides, low, head, left, right, tail, rays, raw, held_weight,
    z_send, send, recv, d_recv, c_send, c_recv, local, w_sem, r_send, r_recv,
    g_send, y_send, t_send, g_recv, y_recv, t_recv, a_send, a_recv, h_send, h_recv, k_send, k_recv, put,
):
    z, o, y, ox, oc, zs, z_peers, y_peer, x_peer, c_peer = neighbours()
    oxc = lax.rem(oc + 2, 4)
    width = pieces.shape[2]
    rows = pieces.shape[1] // PARTS
    group = rows * 8
    tokens, block = sides.shape
    part = left.shape[1]
    near = hops(z)
    across = (((1,), (1,)), ((), ()))
    sent = []

    def columns(oi):
        return pl.ds(pl.multiple_of(oi * width, width), width)

    def tile(oi, yi, zi, s):
        start = pl.multiple_of(((s * 2 + yi) * 4 + zi) * rows, rows)
        return sides.at[pl.ds(start, rows), columns(oi)]

    def piece(zi, s):
        return pieces.at[held(zi), pl.ds(s * rows, rows), :]

    def sem_of(kind, zi, s):
        if kind == CORNER:
            return d_recv.at[s]
        return recv.at[(kind * 4 + zi) * PARTS + s]

    def push(src, where, kind):
        peer = (None, y_peer, x_peer, d_peer)[kind]
        remote(src, tile(*where), send.at[0], sem_of(kind, where[2], where[3]), peer).start()
        sent.append(where)

    def relay(src, where, kind, peer):
        remote(src, tile(*where), send.at[0], sem_of(kind, where[2], where[3]), peer).start()
        sent.append(where)

    def arrived(kind, *where):
        ref = tile(*where)
        remote(ref, ref, send.at[0], sem_of(kind, where[2], where[3]), c_peer).wait_recv()
        return ref

    def band(oi, s):
        return sides.at[pl.ds(s * group, group), columns(oi)]

    def over_core(oi, s, place):
        n = s * 2 + place
        return remote(band(oi, s), band(oi, s), c_send.at[0], c_recv.at[n], c_peer)

    d_peer = {"tok": z, "out": ox, "grp": 1 - y}

    def fetch(i, source):
        return pltpu.make_async_copy(source, staged.at[i], f_sem.at[i])

    fetch(0, activations).start()
    fetch(1, out_grads).start()

    def part_blocks():
        for i, source in enumerate((activations, out_grads)):
            fetch(i, source).wait()
            value = staged[i]
            for k in range(2):
                pieces[2 * i + k] = value[:, k, :]

    greet(z_peers + [y_peer, x_peer, c_peer, d_peer], part_blocks)
    strip = width // 2
    strips = [(b, i) for b in range(2) for i in range(2)]

    def load(n):
        b, i = strips[n]
        place = (b, pl.ds(i * strip, strip), slice(None))
        return pltpu.make_async_copy(weight.at[place], held_weight.at[place], w_sem.at[n])

    def raw_band(oi):
        return raw.at[:, :, columns(oi)]

    own_raw = pieces.at[2:4]
    raw_local = pltpu.make_async_copy(own_raw, raw_band(o), r_send.at[3])
    raw_x = remote(own_raw, raw_band(o), r_send.at[0], r_recv.at[0], x_peer)
    raw_c = remote(own_raw, raw_band(o), r_send.at[1], r_recv.at[1], c_peer)
    raw_xc = remote(raw_band(ox), raw_band(ox), r_send.at[2], r_recv.at[2], c_peer)
    for s in range(PARTS):
        for j in (3, 2, 1):
            copy = remote(
                piece(near[j], s), tile(o, y, z, s), z_send.at[0], sem_of(0, z, s),
                {"tok": near[j], "out": o, "grp": y},
            )
            copy.start()
        push(piece(z, s), (o, y, z, s), 1)
        push(piece(z, s), (o, y, z, s), 2)
    for s in range(PARTS):
        pltpu.make_async_copy(piece(z, s), tile(o, y, z, s), local.at[0]).start()

    for n in range(4):
        load(n).start()
    raw_local.start()
    raw_c.start()
    ones = jnp.ones((16, block), sides.dtype)

    def rows_of(s):
        return pl.ds(s * group, group)

    def gram_group(s, known):
        here = rows_of(s)
        sums = lax.dot_general(ones, sides[here, :], across, preferred_element_type=jnp.float32)
        rays[0:8, here] = sums[0:8]
        for i in known + [s]:
            there = rows_of(i)
            product = lax.dot_general(
                sides[there, :], sides[here, :], across, preferred_element_type=jnp.float32
            )
            product = product * (1.0 / tokens)
            low[there, here] = product.astype(low.dtype)
            if i != s:
                low[here, there] = jnp.transpose(product).astype(low.dtype)

    def straight(j, s):
        return j == 3 and s == PARTS - 1

    def finish(s):
        over_core(oc, s, 0).wait_recv()
        over_core(oxc, s, 1).wait_recv()
        gram_group(s, known)
        known.append(s)

    known = []
    placed = []
    waiting = []
    for kind, j, s in PLAN:
        if kind == "z":
            where = (o, y, near[j], s)
            ref = arrived(0, *where)
            push(ref, where, 1)
            push(ref, where, 2)
            if straight(j, s):
                push(ref, where, CORNER)
        elif kind == "y":
            where = (o, 1 - y, near[j], s)
            ref = arrived(1, *where)
            if (j + s) % 2 == 0 and not straight(j, s):
                relay(ref, where, CORNER, x_peer)
        elif kind == "x":
            where = (ox, y, near[j], s)
            ref = arrived(2, *where)
            if (j + s) % 2 == 1 and not straight(j, s):
                relay(ref, where, CORNER, y_peer)
        elif kind == "c":
            if not placed:
                pltpu.make_async_copy(pieces.at[0], pieces.at[0], local.at[0]).wait()
                placed.append(s)
            over_core(o, s, 0).start()
        else:
            corner = pl.multiple_of((s * 2 + 1 - y) * 4 * rows, rows)
            ref = sides.at[pl.ds(corner, 4 * rows), columns(ox)]
            remote(ref, ref, send.at[0], d_recv.at[s], c_peer).wait_recv()
            over_core(ox, s, 1).start()
            if waiting:
                finish(waiting.pop())
            waiting.append(s)
    raw_x.start()
    finish(waiting.pop())

    def pair(a, b):
        return jnp.sum(a * b, axis=1, keepdims=True)

    def advance(ray):
        high = ray.astype(low.dtype)
        rest = ray - high.astype(jnp.float32)
        middle = rest.astype(low.dtype)
        least = (rest - middle.astype(jnp.float32)).astype(low.dtype)
        zero = jnp.zeros((13, tokens), low.dtype)
        stack = jnp.concatenate([high, middle, least, zero], axis=0)
        image = jnp.dot(stack, low[...], preferred_element_type=jnp.float32)
        return image[0:1] + image[1:2] + image[2:3] + DAMPING * ray

    ray_0 = rays[0:1, :]
    ray_1 = advance(ray_0)
    ray_2 = advance(ray_1)
    dots = [
        pair(ray_0, ray_0),
        pair(ray_0, ray_1),
        pair(ray_1, ray_1),
        pair(ray_1, ray_2),
        pair(ray_2, ray_2),
    ]

    def moment(power):
        total = jnp.full((1, 1), DAMPING**power * block, jnp.float32)
        for i in range(power):
            total = total + DAMPING ** (power - 1 - i) * dots[i] / tokens
        return total

    scale = moment(2 * POWER - 1) / moment(2 * POWER - 2)
    inverse = 1.0 / scale
    root = 1.0 / jnp.sqrt(scale)
    act_start = 2 * (lax.rem(o, 2) * 2 + y) + o // 2
    is_grad = (z // 3) + (3 - z) // 3
    start = (is_grad * (2 * o + y) + (1 - is_grad) * act_start) * part
    cols = pl.ds(pl.multiple_of(start, part), part)
    tall = min(512, tokens)
    steps = tokens // tall

    def span(i):
        return pl.ds(pl.multiple_of(i * tall, tall), tall)

    def apply(i, source, value):
        image = jnp.dot(low[span(i), :], source[...], preferred_element_type=jnp.float32)
        return (image + DAMPING * value) * inverse

    left[...] = sides[:, cols]

    @pl.loop(0, steps, unroll=True)
    def _(i):
        value = left[span(i), :].astype(jnp.float32)
        value = 1.5 * value - 0.5 * apply(i, left, value)
        head[span(i), :] = value
        right[span(i), :] = value.astype(right.dtype)

    @pl.loop(0, steps, unroll=True)
    def _(i):
        value = apply(i, right, head[span(i), :])
        tail[span(i), :] = value
        left[span(i), :] = value.astype(left.dtype)

    @pl.loop(0, steps, unroll=True)
    def _(i):
        value = tail[span(i), :]
        value = 1.5 * value - 0.5 * apply(i, left, value)
        tail[span(i), :] = value
        right[span(i), :] = value.astype(right.dtype)

    @pl.loop(0, steps, unroll=True)
    def _(i):
        value = tail[span(i), :]
        value = 1.5 * value - 0.5 * apply(i, right, value)
        left[span(i), :] = ((1.5 * head[span(i), :] - 0.5 * value) * root).astype(left.dtype)

    span_rows = tokens // CHUNKS
    is_end = is_grad == 1
    is_middle = is_grad == 0
    mine = z // 3
    h = o // 2
    goal_z = (z // 2) * 2 + lax.rem(o, 2)
    stays = goal_z == z
    goal = {"tok": goal_z, "out": o, "grp": y}
    first, second = z // 2, 1 - z // 2
    is_hub = lax.rem(o, 2) == lax.rem(z, 2)
    here = is_middle & stays
    plain = [c for c in range(CHUNKS - TURNED)]
    turned = [c for c in range(CHUNKS - TURNED, CHUNKS)]

    def rung(c):
        return pl.ds(c * span_rows, span_rows)

    def piece_of(c):
        return left.at[rung(c), :]

    def half(i):
        return pl.ds(pl.multiple_of(i * part, part), part)

    def g_tile(b, yi, c):
        return grads.at[b, rung(c), half(yi)]

    def a_tile(i, c):
        return acts.at[rung(c), half(i)]

    def own_grad():
        return pltpu.make_async_copy(left, grads.at[mine, :, half(y)], put.at[0])

    def own_act():
        return pltpu.make_async_copy(left, acts.at[:, half(h)], put.at[0])

    def onward(b):
        return {"tok": lax.rem(z + 5 - 2 * b, 4), "out": o, "grp": y}

    def to_plane(src, b, c):
        n = b * CHUNKS + c
        return remote(src, g_tile(b, y, c), g_send.at[b], g_recv.at[n], onward(b))

    def lands(b, c):
        if c in turned:
            return t_recv.at[b * TURNED + turned.index(c)]
        return y_recv.at[b]

    def other_to_plane(b, c):
        ref = g_tile(b, 1 - y, c)
        return remote(ref, ref, t_send.at[b], lands(b, c), onward(b))

    def y_copy(src, b, c):
        return remote(src, g_tile(b, y, c), y_send.at[b], lands(b, c), y_peer)

    def to_hub(c):
        return remote(piece_of(c), a_tile(h, c), a_send.at[0], a_recv.at[c], goal)

    def over_x(c, i):
        return remote(a_tile(i, c), a_tile(i, c), h_send.at[0], h_recv.at[c], x_peer)

    def act_core(c, i):
        return remote(a_tile(i, c), a_tile(i, c), k_send.at[0], k_recv.at[0], c_peer)

    for b in range(2):

        @pl.when(z == 3 * b)
        def _():
            for c in turned + plain:
                y_copy(piece_of(c), b, c).start()
            for c in plain + turned:
                to_plane(piece_of(c), b, c).start()

    @pl.when(is_end)
    def _():
        own_grad().start()

    @pl.when(here)
    def _():
        own_act().start()

    @pl.when(is_middle & jnp.logical_not(stays))
    def _():
        for c in range(CHUNKS):
            to_hub(c).start()

    def strip_product(n):
        b, i = strips[n]
        load(n).wait()
        total = jnp.zeros((raw.shape[1], strip), jnp.float32)
        for k in range(2):
            total += lax.dot_general(
                raw[k],
                held_weight[b, pl.ds(i * strip, strip), pl.ds(k * block, block)],
                (((1,), (1,)), ((), ())),
                preferred_element_type=jnp.float32,
            )
        return total

    def multiply(i):
        pair_of = jnp.stack([strip_product(i), strip_product(2 + i)], axis=1)
        product[:, :, pl.ds(i * strip, strip)] = pair_of.astype(product.dtype)

    def hub_step(c):
        if c == 0:

            @pl.when(here)
            def _():
                own_act().wait()

        @pl.when(is_hub & jnp.logical_not(here))
        def _():
            ref = a_tile(h, c)
            remote(ref, ref, a_send.at[0], a_recv.at[c], c_peer).wait_recv()

        @pl.when(is_hub)
        def _():
            over_x(c, h).start()
            act_core(c, h).start()

    def cross_step(c):
        @pl.when(is_hub)
        def _():
            over_x(c, 1 - h).wait_recv()
            act_core(c, 1 - h).start()

    def g_wait(b, c):
        ref = g_tile(b, y, c)
        remote(ref, ref, g_send.at[0], g_recv.at[b * CHUNKS + c], c_peer).wait_recv()
        return ref

    def y_wait(b, c):
        ref = g_tile(b, 1 - y, c)
        remote(ref, ref, y_send.at[0], lands(b, c), c_peer).wait_recv()

    def take(b, kind, c):
        if kind == "own":
            ref = g_wait(b, c)

            @pl.when(is_middle)
            def _():
                to_plane(ref, b, c).start()

            if c not in turned:
                y_copy(ref, b, c).start()
        else:
            y_wait(b, c)

            @pl.when(is_middle)
            def _():
                other_to_plane(b, c).start()

    raw_x.wait_recv()
    raw_xc.start()
    raw_local.wait()
    raw_c.wait_recv()

    def multiply_all():
        raw_xc.wait_recv()
        for i in range(2):
            multiply(i)

    @pl.when(is_end)
    def _():
        for c in turned:
            y_wait(mine, c)
            other_to_plane(mine, c).start()

    pl.when(is_end)(multiply_all)
    flow = [("own", c) for c in plain + turned] + [("other", c) for c in turned]
    for step in range(len(flow) + LAG):
        if step < len(flow):

            @pl.when(is_middle)
            def _():
                take(first, *flow[step])

        if step < CHUNKS:
            hub_step(step)
        if step >= LAG:
            take(second, *flow[step - LAG])
    for c in range(CHUNKS):
        cross_step(c)
    pl.when(is_middle)(multiply_all)
    straight_rows = pl.ds(0, span_rows * len(plain))
    turned_rows = pl.ds(span_rows * len(plain), span_rows * TURNED)

    def settle(ref, sem):
        remote(ref, ref, sem, sem, c_peer).wait_send()

    for b in range(2):
        ref = grads.at[b, straight_rows, half(1 - y)]
        remote(ref, ref, y_send.at[0], y_recv.at[b], c_peer).wait_recv()

        @pl.when(z == 3 * b)
        def _():
            settle(left, y_send.at[b])

        @pl.when(z != 3 * b)
        def _():
            settle(grads.at[b, straight_rows, half(y)], y_send.at[b])

        @pl.when(z != 3 - 3 * b)
        def _():
            settle(left, g_send.at[b])
            settle(grads.at[b, turned_rows, half(1 - y)], t_send.at[b])

    @pl.when(is_end)
    def _():
        own_grad().wait()

    @pl.when(is_middle & jnp.logical_not(stays))
    def _():
        settle(left, a_send.at[0])

    @pl.when(is_hub)
    def _():
        settle(acts, k_send.at[0])
        settle(acts.at[:, half(h)], h_send.at[0])

    @pl.when(jnp.logical_not(is_hub))
    def _():
        remote(acts, acts, k_send.at[0], k_recv.at[0], c_peer).wait_recv()

    raw_x.wait_send()
    raw_c.wait_send()
    raw_xc.wait_send()
    settle(pieces.at[0:3], z_send.at[0])
    settle(sides.at[pl.ds(0, len(sent) * rows * width // block), :], send.at[0])
    settle(sides.at[pl.ds(0, tokens // 2), :], c_send.at[0])


def fused(activations, out_grads, weight, part):
    rows, _, width = activations.shape
    tokens, block = rows * 8, width * 4
    dma = pltpu.SemaphoreType.DMA
    vmem = pl.BlockSpec(memory_space=pltpu.VMEM)
    low = activations.dtype
    return pl.pallas_call(
        fused_kernel,
        out_shape=(
            jax.ShapeDtypeStruct((2, tokens, 2 * part), low),
            jax.ShapeDtypeStruct((tokens, 2 * part), low),
            jax.ShapeDtypeStruct((rows, 2, width), low),
        ),
        in_specs=[pl.BlockSpec(memory_space=pltpu.HBM)] * 3,
        out_specs=(vmem, vmem, vmem),
        scratch_shapes=[
            pltpu.VMEM((2, rows, 2, width), low),
            dma((2,)),
            pltpu.VMEM((4, rows, width), low),
            pltpu.VMEM((tokens, block), low),
            pltpu.VMEM((tokens, tokens), low),
            pltpu.VMEM((tokens, part), jnp.float32),
            pltpu.VMEM((tokens, part), low),
            pltpu.VMEM((tokens, part), low),
            pltpu.VMEM((tokens, part), jnp.float32),
            pltpu.VMEM((8, tokens), jnp.float32),
            pltpu.VMEM((2, rows, block), low),
            pltpu.VMEM(weight.shape, weight.dtype),
            dma((1,)),
            dma((1,)),
            dma((12 * PARTS,)),
            dma((PARTS,)),
            dma((1,)),
            dma((2 * PARTS,)),
            dma((1,)),
            dma((4,)),
            dma((4,)),
            dma((3,)),
            dma((2,)),
            dma((2,)),
            dma((2,)),
            dma((2 * CHUNKS,)),
            dma((2,)),
            dma((2 * TURNED,)),
            dma((1,)),
            dma((CHUNKS,)),
            dma((1,)),
            dma((CHUNKS,)),
            dma((1,)),
            dma((1,)),
            dma((1,)),
        ],
        compiler_params=pltpu.CompilerParams(collective_id=0, has_side_effects=True, vmem_limit_bytes=ROOM),
        name="fused",
    )(
        pltpu.with_memory_space_constraint(activations, pltpu.HBM),
        pltpu.with_memory_space_constraint(out_grads, pltpu.HBM),
        weight,
    )


def update_kernel(grads, acts, product, update, input_grad, sem):
    i = pl.program_id(0)
    tokens = acts.shape[0]
    tall = update.shape[0]
    copy = pltpu.make_async_copy(product, input_grad, sem)

    @pl.when(i == 0)
    def _():
        copy.start()

    left = acts[:, pl.ds(pl.multiple_of(i * tall, tall), tall)]
    down = (((0,), (0,)), ((), ()))
    both = [
        lax.dot_general(left, grads[b], down, preferred_element_type=jnp.float32)
        * (1.0 / math.sqrt(tokens))
        for b in range(2)
    ]
    update[...] = jnp.stack([u.astype(update.dtype) for u in both], axis=1)

    @pl.when(i == pl.num_programs(0) - 1)
    def _():
        copy.wait()


def update_product(grads, acts, product):
    count, tokens, width = grads.shape
    height = acts.shape[1]
    tall = height // STEPS
    vmem = pl.BlockSpec(memory_space=pltpu.VMEM)
    return pl.pallas_call(
        update_kernel,
        grid=(STEPS,),
        out_shape=(
            jax.ShapeDtypeStruct((height, count, width), grads.dtype),
            jax.ShapeDtypeStruct(product.shape, product.dtype),
        ),
        in_specs=[vmem, vmem, vmem],
        out_specs=(
            pl.BlockSpec((tall, count, width), lambda i: (i, 0, 0)),
            pl.BlockSpec(memory_space=pl.ANY),
        ),
        scratch_shapes=[pltpu.SemaphoreType.DMA],
        compiler_params=pltpu.CompilerParams(vmem_limit_bytes=ROOM),
        name="update",
    )(grads, acts, product)


def planes(activations, out_grads, weight):
    tok_dev, _, width = activations.shape
    part = width // lax.axis_size("grp")
    token_count = tok_dev * lax.axis_size(("tok", "grp"))
    grads_low, acts_low, product = fused(activations, out_grads, weight, part)
    return update_product(grads_low, acts_low, product)


def solution(mesh):
    in_specs = (
        P(("tok", "grp"), None, "out"),
        P(("tok", "grp"), None, "out"),
        P(None, "out", None),
    )
    out_specs = (P(("tok", "grp"), None, "out"), P(("tok", "grp"), None, "out"))

    def body(activations, out_grads, weight):
        blocks = activations.shape[1]
        tok, grp, out = (mesh.shape[name] for name in ("tok", "grp", "out"))
        fits = (blocks, tok, grp, out) == (2, 4, 2, 4)
        return (planes if fits else local)(activations, out_grads, weight)

    return jax.shard_map(body, mesh=mesh, in_specs=in_specs, out_specs=out_specs, check_vma=False)
```

```python
import math

import jax
import jax.numpy as jnp
from jax import lax
from jax.experimental import pallas as pl
from jax.experimental.pallas import tpu as pltpu
from jax.sharding import PartitionSpec as P

POWER = 3


DAMPING = 0.1
HIGH = lax.Precision.HIGHEST


def spread(piece):
    return lax.all_gather(piece, "out", axis=2, tiled=True)


def token_sums(maker, rows):
    return lax.psum_scatter(
        maker(jnp.int32(0), rows * lax.axis_size(("tok", "grp"))),
        ("tok", "grp"),
        scatter_dimension=0,
        tiled=True,
    )


def shared_rows(piece):
    return lax.all_gather(piece, ("tok", "grp"), axis=0, tiled=True)


def shared_total(vector):
    return lax.psum(vector, ("tok", "out", "grp"))


def diagonal_mask(rows, width, row_start, col_start):
    row_ids = row_start + lax.broadcasted_iota(jnp.int32, (rows, 1, width), 0)
    col_ids = col_start + lax.broadcasted_iota(jnp.int32, (rows, 1, width), 2)
    return jnp.where(row_ids == col_ids, 1.0, 0.0).astype(jnp.float32)


def multiply(left, right, gather_columns):
    row_band = spread(left)
    column_band = gather_columns(right)
    return jnp.einsum("rkj,jkc->rkc", row_band, column_band, preferred_element_type=jnp.float32)


def inverse_roots(tile, row_start, col_start, gather_columns, total):
    rows, count, width = tile.shape
    block = width * lax.axis_size("out")
    mask = diagonal_mask(rows, width, row_start, col_start)
    vector = jnp.ones((count, block), jnp.float32)
    image = vector
    for step in range(POWER):
        columns = lax.dynamic_slice_in_dim(vector, col_start, width, 1)
        part = jnp.einsum("rkc,kc->kr", tile, columns, precision=HIGH)
        placed = lax.dynamic_update_slice_in_dim(
            jnp.zeros((count, block), jnp.float32), part, row_start, 1
        )
        image = total(placed)
        if step + 1 < POWER:
            vector = image / jnp.sqrt(jnp.sum(image * image, axis=1, keepdims=True))
    scale = jnp.sum(vector * image, axis=1) / jnp.sum(vector * vector, axis=1)
    start = tile / scale[None, :, None]
    start_low = start.astype(jnp.bfloat16)
    first_low = ((3.0 * mask - start) / 2.0).astype(jnp.bfloat16)
    square_low = multiply(first_low, first_low, gather_columns).astype(jnp.bfloat16)
    moved = multiply(square_low, start_low, gather_columns)
    second_low = ((3.0 * mask - moved) / 2.0).astype(jnp.bfloat16)
    roots = multiply(first_low, second_low, gather_columns) / jnp.sqrt(scale)[None, :, None]
    return roots.astype(jnp.bfloat16)


def local(activations, out_grads, weight):
    tok_dev, blocks, width = activations.shape
    block = width * lax.axis_size("out")
    token_count = tok_dev * lax.axis_size("tok") * lax.axis_size("grp")
    col_start = lax.axis_index("out") * width
    local_sides = jnp.concatenate([activations, out_grads], axis=1)
    whole_sides = spread(local_sides)
    grads_whole = whole_sides[:, blocks:, :]
    weight_rows = weight.reshape(blocks, width, blocks, block)
    input_grad = jnp.einsum(
        "tjq,bcjq->tbc", grads_whole, weight_rows, preferred_element_type=jnp.float32
    ).astype(jnp.bfloat16)
    rows = block // (lax.axis_size("tok") * lax.axis_size("grp"))
    row_start = lax.axis_index(("tok", "grp")) * rows

    def shared_terms(start, span):
        return jnp.einsum(
            "tkr,tkc->rkc", whole_sides, local_sides, preferred_element_type=jnp.float32
        )

    sums = token_sums(shared_terms, rows)
    tile = sums / token_count + DAMPING * diagonal_mask(rows, width, row_start, col_start)
    roots = inverse_roots(tile, row_start, col_start, shared_rows, shared_total)
    bands = shared_rows(roots)
    whitened = jnp.einsum(
        "tkj,jkc->tkc", whole_sides, bands, preferred_element_type=jnp.float32
    ).astype(jnp.bfloat16)
    acts_whole = spread(whitened[:, :blocks, :]).reshape(tok_dev, blocks * block)
    grads_low = whitened[:, blocks:, :]
    owned_acts = lax.all_to_all(acts_whole, ("tok", "grp"), split_axis=1, concat_axis=0, tiled=True)
    update = jnp.einsum(
        "ta,tbc->abc",
        owned_acts,
        lax.all_gather(grads_low, ("tok", "grp"), axis=0, tiled=True),
        preferred_element_type=jnp.float32,
    )
    update = (update / math.sqrt(token_count)).astype(jnp.bfloat16)
    return (update, input_grad)


MESH = pl.DeviceIdType.MESH
CHUNKS = 8
TURNED = 1
CORNER = 3
ROOM = 50 * 2**20
STEPS = 1
PARTS = 4
PLAN = (
    ("y", 0, 0), ("x", 0, 0), ("y", 0, 1), ("x", 0, 1), ("z", 1, 0), ("y", 0, 2), ("x", 0, 2),
    ("z", 2, 0), ("y", 0, 3), ("x", 0, 3), ("z", 3, 0), ("z", 1, 1), ("z", 2, 1), ("y", 1, 0),
    ("y", 2, 0), ("x", 1, 0), ("z", 1, 2), ("z", 3, 1), ("x", 2, 0), ("z", 2, 2), ("x", 1, 1),
    ("y", 1, 1), ("x", 3, 0), ("z", 1, 3), ("y", 3, 0), ("c", 0, 0), ("z", 3, 2), ("x", 2, 1),
    ("x", 1, 2), ("y", 1, 2), ("y", 2, 1), ("z", 2, 3), ("y", 3, 1), ("c", 0, 1), ("z", 3, 3),
    ("x", 3, 1), ("y", 2, 2), ("x", 2, 2), ("x", 1, 3), ("d", 0, 0), ("x", 3, 2), ("y", 1, 3),
    ("y", 3, 2), ("c", 0, 2), ("x", 2, 3), ("d", 0, 1), ("y", 2, 3), ("x", 3, 3), ("y", 3, 3),
    ("c", 0, 3), ("d", 0, 2), ("d", 0, 3),
)
LAG = 2


def greet(peers, meanwhile):
    barrier = pltpu.get_barrier_semaphore()
    for peer in peers:
        pl.semaphore_signal(barrier, inc=1, device_id=peer, device_id_type=MESH)
    meanwhile()
    pl.semaphore_wait(barrier, len(peers))


def remote(src, dst, send, recv, peer):
    return pltpu.make_async_remote_copy(
        src_ref=src, dst_ref=dst, send_sem=send, recv_sem=recv, device_id=peer, device_id_type=MESH
    )


def held(z):
    return z + 2 - 3 * ((z + 2) // 3) + z // 3


def neighbours():
    z, o, y = lax.axis_index("tok"), lax.axis_index("out"), lax.axis_index("grp")
    ox = lax.rem(o + 2, 4)
    oc = o + 1 - 2 * lax.rem(o, 2)
    at = lambda a, b, c: {"tok": a, "out": b, "grp": c}
    zs = [lax.rem(z + j, 4) for j in range(4)]
    peers = [at(zs[j], o, y) for j in (1, 2, 3)]
    return z, o, y, ox, oc, zs, peers, at(z, o, 1 - y), at(z, ox, y), at(z, oc, y)


def hops(z):
    return (z, z + 1 - 2 * lax.rem(z, 2), 2 - z // 2, 3 - 3 * (z // 2))


def fused_kernel(
    activations, out_grads, weight, grads, acts, product,
    staged, f_sem, pieces, sides, low, head, left, right, tail, rays, raw, held_weight,
    z_send, send, recv, d_recv, c_send, c_recv, local, w_sem, r_send, r_recv,
    g_send, y_send, t_send, g_recv, y_recv, t_recv, a_send, a_recv, h_send, h_recv, k_send, k_recv, put,
):
    z, o, y, ox, oc, zs, z_peers, y_peer, x_peer, c_peer = neighbours()
    oxc = lax.rem(oc + 2, 4)
    width = pieces.shape[2]
    rows = pieces.shape[1] // PARTS
    group = rows * 8
    tokens, block = sides.shape
    part = left.shape[1]
    near = hops(z)
    across = (((1,), (1,)), ((), ()))
    sent = []

    def columns(oi):
        return pl.ds(pl.multiple_of(oi * width, width), width)

    def tile(oi, yi, zi, s):
        start = pl.multiple_of(((s * 2 + yi) * 4 + zi) * rows, rows)
        return sides.at[pl.ds(start, rows), columns(oi)]

    def piece(zi, s):
        return pieces.at[held(zi), pl.ds(s * rows, rows), :]

    def sem_of(kind, zi, s):
        if kind == CORNER:
            return d_recv.at[s]
        return recv.at[(kind * 4 + zi) * PARTS + s]

    def push(src, where, kind):
        peer = (None, y_peer, x_peer, d_peer)[kind]
        remote(src, tile(*where), send.at[0], sem_of(kind, where[2], where[3]), peer).start()
        sent.append(where)

    def relay(src, where, kind, peer):
        remote(src, tile(*where), send.at[0], sem_of(kind, where[2], where[3]), peer).start()
        sent.append(where)

    def arrived(kind, *where):
        ref = tile(*where)
        remote(ref, ref, send.at[0], sem_of(kind, where[2], where[3]), c_peer).wait_recv()
        return ref

    def band(oi, s):
        return sides.at[pl.ds(s * group, group), columns(oi)]

    def over_core(oi, s, place):
        n = s * 2 + place
        return remote(band(oi, s), band(oi, s), c_send.at[0], c_recv.at[n], c_peer)

    d_peer = {"tok": z, "out": ox, "grp": 1 - y}

    def fetch(i, source):
        return pltpu.make_async_copy(source, staged.at[i], f_sem.at[i])

    fetch(0, activations).start()
    fetch(1, out_grads).start()

    def part_blocks():
        for i, source in enumerate((activations, out_grads)):
            fetch(i, source).wait()
            value = staged[i]
            for k in range(2):
                pieces[2 * i + k] = value[:, k, :]

    greet(z_peers + [y_peer, x_peer, c_peer, d_peer], part_blocks)
    strip = width // 2
    strips = [(b, i) for b in range(2) for i in range(2)]

    def load(n):
        b, i = strips[n]
        place = (b, pl.ds(i * strip, strip), slice(None))
        return pltpu.make_async_copy(weight.at[place], held_weight.at[place], w_sem.at[n])

    def raw_band(oi):
        return raw.at[:, :, columns(oi)]

    own_raw = pieces.at[2:4]
    raw_local = pltpu.make_async_copy(own_raw, raw_band(o), r_send.at[3])
    raw_x = remote(own_raw, raw_band(o), r_send.at[0], r_recv.at[0], x_peer)
    raw_c = remote(own_raw, raw_band(o), r_send.at[1], r_recv.at[1], c_peer)
    raw_xc = remote(raw_band(ox), raw_band(ox), r_send.at[2], r_recv.at[2], c_peer)
    for s in range(PARTS):
        for j in (3, 2, 1):
            copy = remote(
                piece(near[j], s), tile(o, y, z, s), z_send.at[0], sem_of(0, z, s),
                {"tok": near[j], "out": o, "grp": y},
            )
            copy.start()
        push(piece(z, s), (o, y, z, s), 1)
        push(piece(z, s), (o, y, z, s), 2)
    for s in range(PARTS):
        pltpu.make_async_copy(piece(z, s), tile(o, y, z, s), local.at[0]).start()

    for n in range(4):
        load(n).start()
    raw_local.start()
    raw_c.start()
    ones = jnp.ones((16, block), sides.dtype)

    def rows_of(s):
        return pl.ds(s * group, group)

    def gram_group(s, known):
        here = rows_of(s)
        sums = lax.dot_general(ones, sides[here, :], across, preferred_element_type=jnp.float32)
        rays[0:8, here] = sums[0:8]
        for i in known + [s]:
            there = rows_of(i)
            product = lax.dot_general(
                sides[there, :], sides[here, :], across, preferred_element_type=jnp.float32
            )
            product = product * (1.0 / tokens)
            low[there, here] = product.astype(low.dtype)
            if i != s:
                low[here, there] = jnp.transpose(product).astype(low.dtype)

    def straight(j, s):
        return j == 3 and s == PARTS - 1

    def finish(s):
        over_core(oc, s, 0).wait_recv()
        over_core(oxc, s, 1).wait_recv()
        gram_group(s, known)
        known.append(s)

    known = []
    placed = []
    waiting = []
    for kind, j, s in PLAN:
        if kind == "z":
            where = (o, y, near[j], s)
            ref = arrived(0, *where)
            push(ref, where, 1)
            push(ref, where, 2)
            if straight(j, s):
                push(ref, where, CORNER)
        elif kind == "y":
            where = (o, 1 - y, near[j], s)
            ref = arrived(1, *where)
            if (j + s) % 2 == 0 and not straight(j, s):
                relay(ref, where, CORNER, x_peer)
        elif kind == "x":
            where = (ox, y, near[j], s)
            ref = arrived(2, *where)
            if (j + s) % 2 == 1 and not straight(j, s):
                relay(ref, where, CORNER, y_peer)
        elif kind == "c":
            if not placed:
                pltpu.make_async_copy(pieces.at[0], pieces.at[0], local.at[0]).wait()
                placed.append(s)
            over_core(o, s, 0).start()
        else:
            corner = pl.multiple_of((s * 2 + 1 - y) * 4 * rows, rows)
            ref = sides.at[pl.ds(corner, 4 * rows), columns(ox)]
            remote(ref, ref, send.at[0], d_recv.at[s], c_peer).wait_recv()
            over_core(ox, s, 1).start()
            if waiting:
                finish(waiting.pop())
            waiting.append(s)
    raw_x.start()
    finish(waiting.pop())

    def pair(a, b):
        return jnp.sum(a * b, axis=1, keepdims=True)

    def advance(ray):
        high = ray.astype(low.dtype)
        rest = ray - high.astype(jnp.float32)
        middle = rest.astype(low.dtype)
        least = (rest - middle.astype(jnp.float32)).astype(low.dtype)
        zero = jnp.zeros((13, tokens), low.dtype)
        stack = jnp.concatenate([high, middle, least, zero], axis=0)
        image = jnp.dot(stack, low[...], preferred_element_type=jnp.float32)
        return image[0:1] + image[1:2] + image[2:3] + DAMPING * ray

    ray_0 = rays[0:1, :]
    ray_1 = advance(ray_0)
    ray_2 = advance(ray_1)
    dots = [
        pair(ray_0, ray_0),
        pair(ray_0, ray_1),
        pair(ray_1, ray_1),
        pair(ray_1, ray_2),
        pair(ray_2, ray_2),
    ]

    def moment(power):
        total = jnp.full((1, 1), DAMPING**power * block, jnp.float32)
        for i in range(power):
            total = total + DAMPING ** (power - 1 - i) * dots[i] / tokens
        return total

    scale = moment(2 * POWER - 1) / moment(2 * POWER - 2)
    inverse = 1.0 / scale
    root = 1.0 / jnp.sqrt(scale)
    act_start = 2 * (lax.rem(o, 2) * 2 + y) + o // 2
    is_grad = (z // 3) + (3 - z) // 3
    start = (is_grad * (2 * o + y) + (1 - is_grad) * act_start) * part
    cols = pl.ds(pl.multiple_of(start, part), part)
    tall = min(512, tokens)
    steps = tokens // tall

    def span(i):
        return pl.ds(pl.multiple_of(i * tall, tall), tall)

    def apply(i, source, value):
        image = jnp.dot(low[span(i), :], source[...], preferred_element_type=jnp.float32)
        return (image + DAMPING * value) * inverse

    left[...] = sides[:, cols]

    @pl.loop(0, steps, unroll=True)
    def _(i):
        value = left[span(i), :].astype(jnp.float32)
        value = 1.5 * value - 0.5 * apply(i, left, value)
        head[span(i), :] = value
        right[span(i), :] = value.astype(right.dtype)

    @pl.loop(0, steps, unroll=True)
    def _(i):
        value = apply(i, right, head[span(i), :])
        tail[span(i), :] = value
        left[span(i), :] = value.astype(left.dtype)

    @pl.loop(0, steps, unroll=True)
    def _(i):
        value = tail[span(i), :]
        value = 1.5 * value - 0.5 * apply(i, left, value)
        tail[span(i), :] = value
        right[span(i), :] = value.astype(right.dtype)

    @pl.loop(0, steps, unroll=True)
    def _(i):
        value = tail[span(i), :]
        value = 1.5 * value - 0.5 * apply(i, right, value)
        left[span(i), :] = ((1.5 * head[span(i), :] - 0.5 * value) * root).astype(left.dtype)

    span_rows = tokens // CHUNKS
    is_end = is_grad == 1
    is_middle = is_grad == 0
    mine = z // 3
    h = o // 2
    goal_z = (z // 2) * 2 + lax.rem(o, 2)
    stays = goal_z == z
    goal = {"tok": goal_z, "out": o, "grp": y}
    first, second = z // 2, 1 - z // 2
    is_hub = lax.rem(o, 2) == lax.rem(z, 2)
    here = is_middle & stays
    plain = [c for c in range(CHUNKS - TURNED)]
    turned = [c for c in range(CHUNKS - TURNED, CHUNKS)]

    def rung(c):
        return pl.ds(c * span_rows, span_rows)

    def piece_of(c):
        return left.at[rung(c), :]

    def half(i):
        return pl.ds(pl.multiple_of(i * part, part), part)

    def g_tile(b, yi, c):
        return grads.at[b, rung(c), half(yi)]

    def a_tile(i, c):
        return acts.at[rung(c), half(i)]

    def own_grad():
        return pltpu.make_async_copy(left, grads.at[mine, :, half(y)], put.at[0])

    def own_act():
        return pltpu.make_async_copy(left, acts.at[:, half(h)], put.at[0])

    def onward(b):
        return {"tok": lax.rem(z + 5 - 2 * b, 4), "out": o, "grp": y}

    def to_plane(src, b, c):
        n = b * CHUNKS + c
        return remote(src, g_tile(b, y, c), g_send.at[b], g_recv.at[n], onward(b))

    def lands(b, c):
        if c in turned:
            return t_recv.at[b * TURNED + turned.index(c)]
        return y_recv.at[b]

    def other_to_plane(b, c):
        ref = g_tile(b, 1 - y, c)
        return remote(ref, ref, t_send.at[b], lands(b, c), onward(b))

    def y_copy(src, b, c):
        return remote(src, g_tile(b, y, c), y_send.at[b], lands(b, c), y_peer)

    def to_hub(c):
        return remote(piece_of(c), a_tile(h, c), a_send.at[0], a_recv.at[c], goal)

    def over_x(c, i):
        return remote(a_tile(i, c), a_tile(i, c), h_send.at[0], h_recv.at[c], x_peer)

    def act_core(c, i):
        return remote(a_tile(i, c), a_tile(i, c), k_send.at[0], k_recv.at[0], c_peer)

    for b in range(2):

        @pl.when(z == 3 * b)
        def _():
            for c in turned + plain:
                y_copy(piece_of(c), b, c).start()
            for c in plain + turned:
                to_plane(piece_of(c), b, c).start()

    @pl.when(is_end)
    def _():
        own_grad().start()

    @pl.when(here)
    def _():
        own_act().start()

    @pl.when(is_middle & jnp.logical_not(stays))
    def _():
        for c in range(CHUNKS):
            to_hub(c).start()

    def strip_product(n):
        b, i = strips[n]
        load(n).wait()
        total = jnp.zeros((raw.shape[1], strip), jnp.float32)
        for k in range(2):
            total += lax.dot_general(
                raw[k],
                held_weight[b, pl.ds(i * strip, strip), pl.ds(k * block, block)],
                (((1,), (1,)), ((), ())),
                preferred_element_type=jnp.float32,
            )
        return total

    def multiply(i):
        pair_of = jnp.stack([strip_product(i), strip_product(2 + i)], axis=1)
        product[:, :, pl.ds(i * strip, strip)] = pair_of.astype(product.dtype)

    def hub_step(c):
        if c == 0:

            @pl.when(here)
            def _():
                own_act().wait()

        @pl.when(is_hub & jnp.logical_not(here))
        def _():
            ref = a_tile(h, c)
            remote(ref, ref, a_send.at[0], a_recv.at[c], c_peer).wait_recv()

        @pl.when(is_hub)
        def _():
            over_x(c, h).start()
            act_core(c, h).start()

    def cross_step(c):
        @pl.when(is_hub)
        def _():
            over_x(c, 1 - h).wait_recv()
            act_core(c, 1 - h).start()

    def g_wait(b, c):
        ref = g_tile(b, y, c)
        remote(ref, ref, g_send.at[0], g_recv.at[b * CHUNKS + c], c_peer).wait_recv()
        return ref

    def y_wait(b, c):
        ref = g_tile(b, 1 - y, c)
        remote(ref, ref, y_send.at[0], lands(b, c), c_peer).wait_recv()

    def take(b, kind, c):
        if kind == "own":
            ref = g_wait(b, c)

            @pl.when(is_middle)
            def _():
                to_plane(ref, b, c).start()

            if c not in turned:
                y_copy(ref, b, c).start()
        else:
            y_wait(b, c)

            @pl.when(is_middle)
            def _():
                other_to_plane(b, c).start()

    raw_x.wait_recv()
    raw_xc.start()
    raw_local.wait()
    raw_c.wait_recv()

    def multiply_all():
        raw_xc.wait_recv()
        for i in range(2):
            multiply(i)

    @pl.when(is_end)
    def _():
        for c in turned:
            y_wait(mine, c)
            other_to_plane(mine, c).start()

    pl.when(is_end)(multiply_all)
    flow = [("own", c) for c in plain + turned] + [("other", c) for c in turned]
    for step in range(len(flow) + LAG):
        if step < len(flow):

            @pl.when(is_middle)
            def _():
                take(first, *flow[step])

        if step < CHUNKS:
            hub_step(step)
        if step >= LAG:
            take(second, *flow[step - LAG])
    for c in range(CHUNKS):
        cross_step(c)
    pl.when(is_middle)(multiply_all)
    straight_rows = pl.ds(0, span_rows * len(plain))
    turned_rows = pl.ds(span_rows * len(plain), span_rows * TURNED)

    def settle(ref, sem):
        remote(ref, ref, sem, sem, c_peer).wait_send()

    for b in range(2):
        ref = grads.at[b, straight_rows, half(1 - y)]
        remote(ref, ref, y_send.at[0], y_recv.at[b], c_peer).wait_recv()

        @pl.when(z == 3 * b)
        def _():
            settle(left, y_send.at[b])

        @pl.when(z != 3 * b)
        def _():
            settle(grads.at[b, straight_rows, half(y)], y_send.at[b])

        @pl.when(z != 3 - 3 * b)
        def _():
            settle(left, g_send.at[b])
            settle(grads.at[b, turned_rows, half(1 - y)], t_send.at[b])

    @pl.when(is_end)
    def _():
        own_grad().wait()

    @pl.when(is_middle & jnp.logical_not(stays))
    def _():
        settle(left, a_send.at[0])

    @pl.when(is_hub)
    def _():
        settle(acts, k_send.at[0])
        settle(acts.at[:, half(h)], h_send.at[0])

    @pl.when(jnp.logical_not(is_hub))
    def _():
        remote(acts, acts, k_send.at[0], k_recv.at[0], c_peer).wait_recv()

    raw_x.wait_send()
    raw_c.wait_send()
    raw_xc.wait_send()
    settle(pieces.at[0:3], z_send.at[0])
    settle(sides.at[pl.ds(0, len(sent) * rows * width // block), :], send.at[0])
    settle(sides.at[pl.ds(0, tokens // 2), :], c_send.at[0])


def fused(activations, out_grads, weight, part):
    rows, _, width = activations.shape
    tokens, block = rows * 8, width * 4
    dma = pltpu.SemaphoreType.DMA
    vmem = pl.BlockSpec(memory_space=pltpu.VMEM)
    low = activations.dtype
    return pl.pallas_call(
        fused_kernel,
        out_shape=(
            jax.ShapeDtypeStruct((2, tokens, 2 * part), low),
            jax.ShapeDtypeStruct((tokens, 2 * part), low),
            jax.ShapeDtypeStruct((rows, 2, width), low),
        ),
        in_specs=[pl.BlockSpec(memory_space=pltpu.HBM)] * 3,
        out_specs=(vmem, vmem, vmem),
        scratch_shapes=[
            pltpu.VMEM((2, rows, 2, width), low),
            dma((2,)),
            pltpu.VMEM((4, rows, width), low),
            pltpu.VMEM((tokens, block), low),
            pltpu.VMEM((tokens, tokens), low),
            pltpu.VMEM((tokens, part), jnp.float32),
            pltpu.VMEM((tokens, part), low),
            pltpu.VMEM((tokens, part), low),
            pltpu.VMEM((tokens, part), jnp.float32),
            pltpu.VMEM((8, tokens), jnp.float32),
            pltpu.VMEM((2, rows, block), low),
            pltpu.VMEM(weight.shape, weight.dtype),
            dma((1,)),
            dma((1,)),
            dma((12 * PARTS,)),
            dma((PARTS,)),
            dma((1,)),
            dma((2 * PARTS,)),
            dma((1,)),
            dma((4,)),
            dma((4,)),
            dma((3,)),
            dma((2,)),
            dma((2,)),
            dma((2,)),
            dma((2 * CHUNKS,)),
            dma((2,)),
            dma((2 * TURNED,)),
            dma((1,)),
            dma((CHUNKS,)),
            dma((1,)),
            dma((CHUNKS,)),
            dma((1,)),
            dma((1,)),
            dma((1,)),
        ],
        compiler_params=pltpu.CompilerParams(collective_id=0, has_side_effects=True, vmem_limit_bytes=ROOM),
        name="fused",
    )(
        pltpu.with_memory_space_constraint(activations, pltpu.HBM),
        pltpu.with_memory_space_constraint(out_grads, pltpu.HBM),
        weight,
    )


def update_kernel(grads, acts, product, update, input_grad, sem):
    i = pl.program_id(0)
    tokens = acts.shape[0]
    tall = update.shape[0]
    copy = pltpu.make_async_copy(product, input_grad, sem)

    @pl.when(i == 0)
    def _():
        copy.start()

    left = acts[:, pl.ds(pl.multiple_of(i * tall, tall), tall)]
    down = (((0,), (0,)), ((), ()))
    both = [
        lax.dot_general(left, grads[b], down, preferred_element_type=jnp.float32)
        * (1.0 / math.sqrt(tokens))
        for b in range(2)
    ]
    update[...] = jnp.stack([u.astype(update.dtype) for u in both], axis=1)

    @pl.when(i == pl.num_programs(0) - 1)
    def _():
        copy.wait()


def update_product(grads, acts, product):
    count, tokens, width = grads.shape
    height = acts.shape[1]
    tall = height // STEPS
    vmem = pl.BlockSpec(memory_space=pltpu.VMEM)
    return pl.pallas_call(
        update_kernel,
        grid=(STEPS,),
        out_shape=(
            jax.ShapeDtypeStruct((height, count, width), grads.dtype),
            jax.ShapeDtypeStruct(product.shape, product.dtype),
        ),
        in_specs=[vmem, vmem, vmem],
        out_specs=(
            pl.BlockSpec((tall, count, width), lambda i: (i, 0, 0)),
            pl.BlockSpec(memory_space=pl.ANY),
        ),
        scratch_shapes=[pltpu.SemaphoreType.DMA],
        compiler_params=pltpu.CompilerParams(vmem_limit_bytes=ROOM),
        name="update",
    )(grads, acts, product)


def planes(activations, out_grads, weight):
    tok_dev, _, width = activations.shape
    part = width // lax.axis_size("grp")
    token_count = tok_dev * lax.axis_size(("tok", "grp"))
    grads_low, acts_low, product = fused(activations, out_grads, weight, part)
    return update_product(grads_low, acts_low, product)


def solution(mesh):
    in_specs = (
        P(("tok", "grp"), None, "out"),
        P(("tok", "grp"), None, "out"),
        P(None, "out", None),
    )
    out_specs = (P(("tok", "grp"), None, "out"), P(("tok", "grp"), None, "out"))

    def body(activations, out_grads, weight):
        blocks = activations.shape[1]
        tok, grp, out = (mesh.shape[name] for name in ("tok", "grp", "out"))
        fits = (blocks, tok, grp, out) == (2, 4, 2, 4)
        return (planes if fits else local)(activations, out_grads, weight)

    return jax.shard_map(body, mesh=mesh, in_specs=in_specs, out_specs=out_specs, check_vma=False)
```
